32 devices in a mesh: dp: 1 (over z), tp: 4 (over y), ep: 8 (over x, core).
Axes of the slice: x: 4, y: 4, z: 1, core: 2. Of those that a mesh axis runs over, the one named last changes fastest.
The devices are a block of a 4x4x8 slice.
Arguments:
- resid_in: bfloat16 [2048, 4096], P(('dp', 'ep'))
- norm_scale: bfloat16 [4096], replicated
- w_router: bfloat16 [4096, 16], replicated
- w_gate: bfloat16 [16, 4096, 3072], P('ep', None, 'tp')
- w_up: bfloat16 [16, 4096, 3072], P('ep', None, 'tp')
- w_down: bfloat16 [16, 3072, 4096], P('ep', 'tp')
- choice: int32 [2048, 2], P(('dp', 'ep'))
Outputs:
- output: bfloat16 [2048, 4096], P(('dp', 'ep'))
All inputs are finite; a program needn't handle non-finite values.
Results may differ from the reference program's by a relative error of at most 0.00643143.
Values are sent between devices in bfloat16 or wider.
A program may use at most 768 MiB of HBM per device.

```python
import jax
import jax.numpy as jnp
from jax import lax

D_MODEL = 4096
EXPERTS = 16
TOP_K = 2
TOK_DEV = 256
FF_SHARD = 768
EP_GROUPS = 8
TP_SHARDS = 4

TOKENS = EP_GROUPS * TOK_DEV
FF_WIDTH = TP_SHARDS * FF_SHARD
CAPACITY = (2 * TOK_DEV * TOP_K + EXPERTS - 1) // EXPERTS
NUM_SLOTS = EXPERTS * EP_GROUPS * CAPACITY
NORM_EPS = 1e-5


def draw_choice(choice_key):
    base_key, bias_key = jax.random.split(choice_key)
    base_score = jax.random.randint(base_key, (TOKENS, EXPERTS), 0, 65536, dtype=jnp.int32)
    expert_bias = jax.random.randint(bias_key, (EXPERTS,), 0, 16384, dtype=jnp.int32)
    scores = (base_score + expert_bias[None, :]) * EXPERTS + jnp.arange(EXPERTS, dtype=jnp.int32)[None, :]
    return lax.top_k(scores, TOP_K)[1].astype(jnp.int32)


def setup_inputs(seed: int = 0, part: int = 0) -> dict:
    root_key = jax.random.key(seed)
    sub_keys = jax.random.split(root_key, 7)
    resid_in = jax.random.normal(jax.random.fold_in(sub_keys[0], part), (TOKENS, D_MODEL), jnp.float32)
    norm_scale = 1.0 + 0.3 * jax.random.normal(sub_keys[1], (D_MODEL,), jnp.float32)
    w_router = jax.random.normal(sub_keys[2], (D_MODEL, EXPERTS), jnp.float32) * D_MODEL ** -0.5
    w_gate = jax.random.normal(sub_keys[3], (EXPERTS, D_MODEL, FF_WIDTH), jnp.float32) * D_MODEL ** -0.5
    w_up = jax.random.normal(sub_keys[4], (EXPERTS, D_MODEL, FF_WIDTH), jnp.float32) * D_MODEL ** -0.5
    w_down = jax.random.normal(sub_keys[5], (EXPERTS, FF_WIDTH, D_MODEL), jnp.float32) * (2.0 * FF_WIDTH ** -0.5)
    choice = draw_choice(jax.random.fold_in(sub_keys[6], part))
    return {'resid_in': resid_in.astype(jnp.bfloat16), 'norm_scale': norm_scale.astype(jnp.bfloat16), 'w_router': w_router.astype(jnp.bfloat16), 'w_gate': w_gate.astype(jnp.bfloat16), 'w_up': w_up.astype(jnp.bfloat16), 'w_down': w_down.astype(jnp.bfloat16), 'choice': choice}


def norm_route(resid_rows, norm_scale, w_router, choice_rows):
    rows_f32 = resid_rows.astype(jnp.float32)
    centered = rows_f32 - jnp.mean(rows_f32, axis=-1, keepdims=True)
    variance = jnp.mean(centered * centered, axis=-1, keepdims=True)
    normed = (centered * lax.rsqrt(variance + NORM_EPS) * norm_scale.astype(jnp.float32)).astype(jnp.bfloat16)
    logits = jnp.dot(normed, w_router, preferred_element_type=jnp.float32)
    router_probs = jax.nn.softmax(logits, axis=-1)
    expert_ids = jnp.arange(w_router.shape[1], dtype=jnp.int32)
    picked = jnp.sum(jnp.where(choice_rows[:, :, None] == expert_ids[None, None, :], router_probs[:, None, :], 0.0), axis=-1)
    gate_vals = picked / jnp.sum(picked, axis=-1, keepdims=True)
    return normed, gate_vals


def expert_glu(rows_in, w_gate_e, w_up_e, w_down_e):
    gate_act = jnp.dot(rows_in, w_gate_e, preferred_element_type=jnp.float32)
    up_act = jnp.dot(rows_in, w_up_e, preferred_element_type=jnp.float32)
    hidden = (jax.nn.silu(gate_act) * up_act).astype(jnp.bfloat16)
    hidden_split = hidden.reshape(rows_in.shape[0], TP_SHARDS, FF_SHARD).astype(jnp.float32)
    down_split = w_down_e.reshape(TP_SHARDS, FF_SHARD, D_MODEL).astype(jnp.float32)
    partial_out = jnp.einsum('stf,tfd->tsd', hidden_split, down_split).astype(jnp.bfloat16)
    return jnp.sum(partial_out.astype(jnp.float32), axis=0)


def reference(resid_in, norm_scale, w_router, w_gate, w_up, w_down, choice):
    normed, gate_vals = norm_route(resid_in, norm_scale, w_router, choice)
    group_choice = choice.reshape(EP_GROUPS, TOK_DEV * TOP_K)
    onehot = (group_choice[:, :, None] == jnp.arange(EXPERTS, dtype=jnp.int32)[None, None, :]).astype(jnp.int32)
    earlier = jnp.cumsum(onehot, axis=1) - onehot
    position = jnp.sum(earlier * onehot, axis=2)
    is_kept = (position < CAPACITY).reshape(-1)
    group_ids = jnp.arange(EP_GROUPS, dtype=jnp.int32)[:, None]
    slot_ids = (group_choice * (EP_GROUPS * CAPACITY) + group_ids * CAPACITY + position).reshape(-1)
    target = jnp.where(is_kept, slot_ids, NUM_SLOTS)
    token_rows = (group_ids * TOK_DEV + jnp.arange(TOK_DEV * TOP_K, dtype=jnp.int32)[None, :] // TOP_K).reshape(-1)
    source_row = jnp.zeros((NUM_SLOTS + 1,), jnp.int32).at[target].set(token_rows)[:NUM_SLOTS]
    kept_gate = jnp.where(is_kept, gate_vals.reshape(-1), 0.0)
    slot_gate = jnp.zeros((NUM_SLOTS + 1,), jnp.float32).at[target].set(kept_gate)[:NUM_SLOTS]

    def expert_step(mixed_sum, expert_in):
        rows_idx, gate_col, w_gate_e, w_up_e, w_down_e = expert_in
        y_rows = expert_glu(normed[rows_idx], w_gate_e, w_up_e, w_down_e)
        return mixed_sum.at[rows_idx].add(gate_col[:, None] * y_rows), None

    mixed_sum, unused = lax.scan(expert_step, jnp.zeros((TOKENS, D_MODEL), jnp.float32), (source_row.reshape(EXPERTS, EP_GROUPS * CAPACITY), slot_gate.reshape(EXPERTS, EP_GROUPS * CAPACITY), w_gate, w_up, w_down))
    return (resid_in.astype(jnp.float32) + mixed_sum).astype(jnp.bfloat16)
```

```python
import functools

import jax
import jax.numpy as jnp
from jax import lax
from jax.experimental import pallas as pl
from jax.experimental.pallas import tpu as pltpu
from jax.sharding import PartitionSpec as P

NORM_EPS = 1e-5
MESH = pl.DeviceIdType.MESH
BF16 = jnp.bfloat16
F32 = jnp.float32
SUBS = 4


def norm_route(resid_rows, norm_scale, w_router, choice_rows):
    rows_f32 = resid_rows.astype(F32)
    centered = rows_f32 - jnp.mean(rows_f32, axis=-1, keepdims=True)
    variance = jnp.mean(centered * centered, axis=-1, keepdims=True)
    normed = (centered * lax.rsqrt(variance + NORM_EPS) * norm_scale.astype(F32)).astype(BF16)
    logits = jnp.dot(normed, w_router, preferred_element_type=F32)
    router_probs = jax.nn.softmax(logits, axis=-1)
    expert_ids = jnp.arange(w_router.shape[1], dtype=jnp.int32)
    chosen = choice_rows[:, :, None] == expert_ids[None, None, :]
    picked = jnp.sum(jnp.where(chosen, router_probs[:, None, :], 0.0), axis=-1)
    gate_vals = picked / jnp.sum(picked, axis=-1, keepdims=True)
    gate_by_expert = jnp.sum(jnp.where(chosen, gate_vals[:, :, None], 0.0), axis=1)
    return normed, gate_by_expert, jnp.any(chosen, axis=1)


def slot_meta(gate_by_expert, is_chosen, capacity):
    rows = is_chosen.shape[0]
    earlier = jnp.arange(rows)[:, None] > jnp.arange(rows)[None, :]
    position = jnp.dot(earlier.astype(BF16), is_chosen.astype(BF16), preferred_element_type=F32)
    kept = is_chosen & (position < capacity)
    return jnp.concatenate([jnp.where(kept, position, -1.0).T, jnp.where(kept, gate_by_expert, 0.0).T], axis=0)


def moe_kernel(experts, capacity, ny, nx, u_in, resid, meta_in, w_gate, w_up, w_down, out, ug,
               w1, v1, w2, xg, hid, hpart, sums, rfar, rplus, rminus, yown, yfar, yplus, yminus, fin, xres, utile, gsplit, meta,
               load_sem, tile_sem, send_sem, recv_sem):
    rows, d_model = resid.shape
    half = d_model // 2
    quarter = half // ny
    width = w_gate.shape[2]
    chunk = rows // 8
    sub = rows // SUBS
    tile = utile.shape[2]
    y = lax.axis_index('tp')
    ep = lax.axis_index('ep')
    core = lax.rem(ep, 2)
    x = ep // 2

    def ep_at(dx, other=False):
        return lax.rem(x + dx + nx, nx) * 2 + ((1 - core) if other else core)

    def dev_x(dx, other=False):
        return {'ep': ep_at(dx, other)}

    def dev_y(dy, other=False):
        return {'tp': lax.rem(y + dy + ny, ny), 'ep': ep_at(0, other)}

    partner = dev_x(0, True)

    barrier = pltpu.get_barrier_semaphore()
    peers = [dev_x(dx, o) for dx in range(nx) for o in (False, True) if (dx, o) != (0, False)]
    peers += [dev_y(dy, o) for dy in (1, -1) for o in (False, True)]
    for peer in peers:
        pl.semaphore_signal(barrier, inc=1, device_id=peer, device_id_type=MESH)
    pl.semaphore_wait(barrier, len(peers))

    copies = []

    def remote(src, dst, device):
        at = len(copies)
        copy = pltpu.make_async_remote_copy(src_ref=src, dst_ref=dst, send_sem=send_sem.at[at], recv_sem=recv_sem.at[at], device_id=device, device_id_type=MESH)
        copies.append(copy)
        copy.start()
        return copy

    sent = []

    def finish_send(copy):
        copy.wait_send()
        sent.append(copy)

    locals_ = []

    def local(src, dst):
        copy = pltpu.make_async_copy(src, dst, load_sem.at[len(locals_)])
        locals_.append(copy)
        copy.start()
        return copy

    my_half = pl.multiple_of(core * half, half)
    other_half = pl.multiple_of((1 - core) * half, half)
    my_quarter = pl.multiple_of(my_half + y * quarter, quarter)
    other_quarter = pl.multiple_of(other_half + y * quarter, quarter)

    parity = lax.rem(y, 2)

    def piece(q, mine=True):
        side = parity if mine else 1 - parity
        return pl.ds(pl.multiple_of(side * (rows // 2) + q * chunk, chunk), chunk)

    ax = {}
    for q in range(4):
        ax[1, q] = remote(u_in.at[piece(q)], ug.at[1, 0, piece(q)], dev_x(1))
        ax[2, q] = remote(u_in.at[piece(q)], ug.at[2, 0, piece(q)], dev_x(-1))
    own_pair = remote(u_in, ug.at[0, 1], partner)
    meta_copies = []
    for slot, dx in ((0, 0), (1, 1), (2, -1), (3, 2)):
        for lane in range(2):
            if (slot, lane) == (0, 0):
                meta_copies.append(local(meta_in, meta.at[0]))
            else:
                meta_copies.append(remote(meta_in, meta.at[slot * 2 + lane], dev_x(dx, lane == 1)))
    loads = {}
    for e in range(2):
        loads[e] = (local(w_gate.at[e], w1.at[e]), local(w_up.at[e], v1.at[e]))
    w2_copies = [local(w_down.at[e, :, pl.ds(my_half, half)], w2.at[e]) for e in range(2)]
    w2_copies += [remote(w_down.at[e, :, pl.ds(other_half, half)], w2.at[2 + e], partner) for e in range(2)]
    res_copies = [local(resid.at[:, pl.ds(my_quarter, quarter)], xres.at[0]),
                  remote(resid.at[:, pl.ds(other_quarter, quarter)], xres.at[1], partner)]

    ay, pushed = {}, {1: [], 2: [], 3: []}

    def push(slot, q, mine):
        at = piece(q, mine)
        pushed[slot].append(remote(ug.at[slot, 0, at], ug.at[slot, 1, at], partner))

    def y_forward(slot, q):
        up = (q % 2 == 0) == (slot != 2)
        ay[slot, q] = remote(ug.at[slot, 0, piece(q)], ug.at[slot, 0, piece(q)], dev_y(1 if up else -1))

    def on_near(q):
        for slot in (1, 2):
            ax[slot, q].wait_recv()
            if (q % 2 == 0) == (slot == 1):
                ax[3, q] = remote(ug.at[slot, 0, piece(q)], ug.at[3, 0, piece(q)], dev_x(1 if slot == 1 else -1))
            y_forward(slot, q)
        for slot in (1, 2):
            push(slot, q, True)

    def on_far(q):
        ax[3, q].wait_recv()
        y_forward(3, q)
        push(3, q, True)

    def on_side(slot, q):
        ay[slot, q].wait_recv()
        push(slot, q, False)

    def slot_onehot(pos_row):
        return lax.broadcasted_iota(jnp.int32, (capacity, rows), 0).astype(F32) == pos_row

    def gather(slot):
        picks = []
        for lane in range(2):
            parts = []
            for e in range(2):
                pos_row = meta[slot * 2 + lane, pl.ds(2 * ep + e, 1), :]
                parts.append(slot_onehot(pos_row).astype(F32).astype(BF16))
            picks.append(jnp.concatenate(parts, axis=0))
            gates = []
            for e in range(4):
                row = 2 * (ep if e < 2 else ep_at(0, True)) + e % 2
                pos_row = meta[slot * 2 + lane, pl.ds(row, 1), :]
                gate_row = meta[slot * 2 + lane, pl.ds(experts + row, 1), :]
                gates.append(jnp.where(slot_onehot(pos_row), gate_row, 0.0))
            gate_mat = jnp.concatenate(gates, axis=0).T
            for term in range(3):
                part = gate_mat.astype(BF16)
                gsplit[lane, term] = part
                gate_mat = gate_mat - part.astype(F32)

        tiles = d_model // tile

        def fetch(t, lane):
            cols = pl.ds(pl.multiple_of(t * tile, tile), tile)
            src = u_in.at[:, cols] if (slot, lane) == (0, 0) else ug.at[slot, lane, :, cols]
            at = lax.rem(t, 2) * 2 + lane
            return pltpu.make_async_copy(src, utile.at[at], tile_sem.at[at])

        for lane in range(2):
            fetch(0, lane).start()

        def body(t, carry):
            @pl.when(t + 1 < tiles)
            def _():
                for lane in range(2):
                    fetch(t + 1, lane).start()
            cols = pl.ds(pl.multiple_of(t * tile, tile), tile)
            for lane in range(2):
                fetch(t, lane).wait()
                got = jnp.dot(picks[lane], utile[lax.rem(t, 2) * 2 + lane], preferred_element_type=F32).astype(BF16)
                for e in range(2):
                    xg[e, lane * capacity:(lane + 1) * capacity, cols] = got[e * capacity:(e + 1) * capacity]
            return carry

        lax.fori_loop(0, tiles, body, 0)

    ftile = min(256, width)

    def gate_up(e):
        def body(t, carry):
            cols = pl.ds(pl.multiple_of(t * ftile, ftile), ftile)
            gate_act = jnp.dot(xg[e], w1[e, :, cols], preferred_element_type=F32)
            up_act = jnp.dot(xg[e], v1[e, :, cols], preferred_element_type=F32)
            hid[e, :, cols] = (jax.nn.silu(gate_act) * up_act).astype(BF16)
            return carry

        lax.fori_loop(0, width // ftile, body, 0)

    dtile = min(512, half)

    def share_hidden(slot):
        return remote(hid, hpart.at[slot], partner)

    def down(slot):
        def body(t, carry):
            cols = pl.ds(pl.multiple_of(t * dtile, dtile), dtile)
            outs = []
            for e in range(4):
                lhs = hid[e] if e < 2 else hpart[slot, e - 2]
                outs.append(jnp.dot(lhs, w2[e, :, cols], preferred_element_type=F32).astype(BF16))
            for lane in range(2):
                stack = []
                for e in range(4):
                    at = lane if e < 2 else 1 - lane
                    stack.append(outs[e][at * capacity:(at + 1) * capacity])
                stacked = jnp.concatenate(stack, axis=0)
                total = jnp.dot(gsplit[lane, 0], stacked, preferred_element_type=F32)
                for term in (1, 2):
                    total += jnp.dot(gsplit[lane, term], stacked, preferred_element_type=F32)
                sums[slot, lane, :, cols] = total.astype(BF16)
            return carry

        lax.fori_loop(0, half // dtile, body, 0)

    for copy in meta_copies:
        copy.wait_recv() if copy.is_remote else copy.wait()
    own_pair.wait_recv()
    gather(0)
    for copy in loads[0]:
        copy.wait()
    gate_up(0)
    on_near(0)
    for copy in loads[1]:
        copy.wait()
    gate_up(1)
    hs = share_hidden(0)
    on_near(1)
    for copy in w2_copies:
        copy.wait_recv() if copy.is_remote else copy.wait()
    hs.wait_recv()
    down(0)
    finish_send(hs)
    on_near(2)
    for q in (0, 1):
        on_side(1, q)
        on_side(2, q)
    on_near(3)
    for q in (2,):
        on_side(1, q)
        on_side(2, q)
    on_far(0)
    on_far(1)
    for q in (3,):
        on_side(1, q)
        on_side(2, q)

    def chip_pair(slot, between):
        for copy in pushed[slot]:
            copy.wait_recv()
        gather(slot)
        gate_up(0)
        between(0)
        gate_up(1)
        between(1)
        hs = share_hidden(slot)
        between(2)
        hs.wait_recv()
        down(slot)
        finish_send(hs)

    def sub_rows(j):
        return pl.ds(j * sub, sub)

    sx = {}

    def send_sum(name, slot, lane, j, landing, dx):
        sx[name, j] = remote(sums.at[slot, lane, sub_rows(j)], landing.at[lane, sub_rows(j)], dev_x(dx))

    def during_left(step):
        if step < 2:
            on_far(2 + step)

    def during_right(step):
        for q in ((0, 1), (2,), (3,))[step]:
            on_side(3, q)

    chip_pair(1, during_left)
    for j in range(SUBS):
        send_sum('m0', 1, 0, j, rminus, -1)
    chip_pair(2, during_right)
    for j in range(SUBS):
        send_sum('p1', 2, 1, j, rplus, 1)
    chip_pair(3, lambda step: None)

    def send_far(j):
        send_sum('f0', 3, 0, j, rfar, 1)
        send_sum('f1', 3, 1, j, rfar, -1)

    def q_cols(dy):
        return pl.ds(pl.multiple_of(lax.rem(y + dy + ny, ny) * quarter, quarter), quarter)

    def stage_far(j):
        sx['f0', j].wait_recv()
        sx['f1', j].wait_recv()
        at = sub_rows(j)
        sums[2, 0, at, :] = (sums[2, 0, at, :].astype(F32) + rfar[0, at, :].astype(F32)).astype(BF16)
        send_sum('p0', 2, 0, j, rplus, 1)
        sums[1, 1, at, :] = (sums[1, 1, at, :].astype(F32) + rfar[1, at, :].astype(F32)).astype(BF16)
        send_sum('m1', 1, 1, j, rminus, -1)
        if j + 2 < SUBS:
            send_far(j + 2)

    def send_y(name, lane, j, dcol, landing, dy):
        sx[name, j] = remote(sums.at[0, lane, sub_rows(j), q_cols(dcol)], landing.at[lane, sub_rows(j)], dev_y(dy))

    def stage_own(j):
        for name in ('m0', 'p1', 'p0', 'm1'):
            sx[name, j].wait_recv()
        at = sub_rows(j)
        for lane in range(2):
            cols = q_cols(0)
            yown[lane, at, :] = sums[0, lane, at, cols].astype(F32) + rplus[lane, at, cols].astype(F32) + rminus[lane, at, cols].astype(F32)
        for lane in range(2):
            sums[0, lane, at, :] = (sums[0, lane, at, :].astype(F32) + rplus[lane, at, :].astype(F32) + rminus[lane, at, :].astype(F32)).astype(BF16)
        send_y('yf0', 0, j, 2, yfar, 1)
        send_y('yf1', 1, j, 2, yfar, -1)
        send_y('yp1', 1, j, 1, yplus, 1)
        send_y('ym0', 0, j, -1, yminus, -1)

    def stage_yfar(j):
        sx['yf0', j].wait_recv()
        sx['yf1', j].wait_recv()
        at = sub_rows(j)
        cols = q_cols(1)
        sums[0, 0, at, cols] = (sums[0, 0, at, cols].astype(F32) + yfar[0, at, :].astype(F32)).astype(BF16)
        send_y('yp0', 0, j, 1, yplus, 1)
        cols = q_cols(-1)
        sums[0, 1, at, cols] = (sums[0, 1, at, cols].astype(F32) + yfar[1, at, :].astype(F32)).astype(BF16)
        send_y('ym1', 1, j, -1, yminus, -1)

    done = {}

    def stage_final(j):
        for name in ('ym0', 'yp1', 'yp0', 'ym1'):
            sx[name, j].wait_recv()
        at = sub_rows(j)
        for lane in range(2):
            total = yown[lane, at, :] + yplus[lane, at, :].astype(F32) + yminus[lane, at, :].astype(F32)
            fin[lane, at, :] = (xres[lane, at, :].astype(F32) + total).astype(BF16)
        place = out.at[at, pl.ds(my_quarter, quarter)]
        for lane in range(2):
            done['up', lane, j] = remote(fin.at[lane, at], place, dev_y(1, lane == 1))
            done['down', lane, j] = remote(fin.at[lane, at], place, dev_y(-1, lane == 1))
        done['own', j] = local(fin.at[0, at], place)
        done['pair', j] = remote(fin.at[1, at], place, partner)

    def stage_relay(j):
        at = sub_rows(j)
        done['up', 0, j].wait_recv()
        cols = pl.ds(pl.multiple_of(my_half + lax.rem(y - 1 + ny, ny) * quarter, quarter), quarter)
        done['up2', j] = remote(out.at[at, cols], out.at[at, cols], dev_y(1))
        done['down', 1, j].wait_recv()
        cols = pl.ds(pl.multiple_of(other_half + lax.rem(y + 1, ny) * quarter, quarter), quarter)
        done['down2', j] = remote(out.at[at, cols], out.at[at, cols], dev_y(-1))

    for copy in res_copies:
        copy.wait_recv() if copy.is_remote else copy.wait()
    send_far(0)
    send_far(1)
    stages = (stage_far, stage_own, stage_yfar, stage_final, stage_relay)
    for step in range(SUBS + len(stages) - 1):
        for lag, stage in enumerate(stages):
            if 0 <= step - lag < SUBS:
                stage(step - lag)
    for j in range(SUBS):
        done['up', 1, j].wait_recv()
        done['down', 0, j].wait_recv()
        done['pair', j].wait_recv()
        done['up2', j].wait_recv()
        done['down2', j].wait_recv()
        done['own', j].wait()
    for copy in copies:
        if not any(copy is other for other in sent):
            copy.wait_send()


def solution(mesh):
    row_spec = P(('dp', 'ep'), None)
    ny, nx = mesh.shape['tp'], mesh.shape['ep'] // 2

    def device_step(resid_in, norm_scale, w_router, w_gate, w_up, w_down, choice):
        rows, d_model = resid_in.shape
        experts = w_router.shape[1]
        width = w_gate.shape[2]
        capacity = (2 * rows * choice.shape[1] + experts - 1) // experts
        normed, gate_by_expert, is_chosen = norm_route(resid_in, norm_scale, w_router, choice)
        meta = slot_meta(gate_by_expert, is_chosen, capacity)
        half, slots = d_model // 2, 2 * capacity
        quarter = half // ny
        tile = min(512, d_model)

        hbm = pl.BlockSpec(memory_space=pl.ANY)
        out, _ = pl.pallas_call(
            functools.partial(moe_kernel, experts, capacity, ny, nx),
            out_shape=(jax.ShapeDtypeStruct((rows, d_model), BF16), jax.ShapeDtypeStruct((4, 2, rows, d_model), BF16)),
            in_specs=[hbm] * 6,
            out_specs=(hbm, hbm),
            scratch_shapes=[
                pltpu.VMEM((2, d_model, width), BF16),
                pltpu.VMEM((2, d_model, width), BF16),
                pltpu.VMEM((4, width, half), BF16),
                pltpu.VMEM((2, slots, d_model), BF16),
                pltpu.VMEM((2, slots, width), BF16),
                pltpu.VMEM((4, 2, slots, width), BF16),
                pltpu.VMEM((4, 2, rows, half), BF16),
                pltpu.VMEM((2, rows, half), BF16),
                pltpu.VMEM((2, rows, half), BF16),
                pltpu.VMEM((2, rows, half), BF16),
                pltpu.VMEM((2, rows, quarter), F32),
                pltpu.VMEM((2, rows, quarter), BF16),
                pltpu.VMEM((2, rows, quarter), BF16),
                pltpu.VMEM((2, rows, quarter), BF16),
                pltpu.VMEM((2, rows, quarter), BF16),
                pltpu.VMEM((2, rows, quarter), BF16),
                pltpu.VMEM((4, rows, tile), BF16),
                pltpu.VMEM((2, 3, rows, 4 * capacity), BF16),
                pltpu.VMEM((8, 2 * experts, rows), F32),
                pltpu.SemaphoreType.DMA((16,)),
                pltpu.SemaphoreType.DMA((4,)),
                pltpu.SemaphoreType.DMA((192,)),
                pltpu.SemaphoreType.DMA((192,)),
            ],
            compiler_params=pltpu.CompilerParams(collective_id=0, has_side_effects=True, vmem_limit_bytes=67043328),
            name='moe_ring',
        )(normed, resid_in, meta, w_gate, w_up, w_down)
        return out

    return jax.shard_map(device_step, mesh=mesh, in_specs=(row_spec, P(None), P(None, None), P('ep', None, 'tp'), P('ep', None, 'tp'), P('ep', 'tp', None), row_spec), out_specs=row_spec, check_vma=False)
```

```python
import functools

import jax
import jax.numpy as jnp
from jax import lax
from jax.experimental import pallas as pl
from jax.experimental.pallas import tpu as pltpu
from jax.sharding import PartitionSpec as P

NORM_EPS = 1e-5
MESH = pl.DeviceIdType.MESH
BF16 = jnp.bfloat16
F32 = jnp.float32
SUBS = 4


def norm_route(resid_rows, norm_scale, w_router, choice_rows):
    rows_f32 = resid_rows.astype(F32)
    centered = rows_f32 - jnp.mean(rows_f32, axis=-1, keepdims=True)
    variance = jnp.mean(centered * centered, axis=-1, keepdims=True)
    normed = (centered * lax.rsqrt(variance + NORM_EPS) * norm_scale.astype(F32)).astype(BF16)
    logits = jnp.dot(normed, w_router, preferred_element_type=F32)
    router_probs = jax.nn.softmax(logits, axis=-1)
    expert_ids = jnp.arange(w_router.shape[1], dtype=jnp.int32)
    chosen = choice_rows[:, :, None] == expert_ids[None, None, :]
    picked = jnp.sum(jnp.where(chosen, router_probs[:, None, :], 0.0), axis=-1)
    gate_vals = picked / jnp.sum(picked, axis=-1, keepdims=True)
    gate_by_expert = jnp.sum(jnp.where(chosen, gate_vals[:, :, None], 0.0), axis=1)
    return normed, gate_by_expert, jnp.any(chosen, axis=1)


def slot_meta(gate_by_expert, is_chosen, capacity):
    rows = is_chosen.shape[0]
    earlier = jnp.arange(rows)[:, None] > jnp.arange(rows)[None, :]
    position = jnp.dot(earlier.astype(BF16), is_chosen.astype(BF16), preferred_element_type=F32)
    kept = is_chosen & (position < capacity)
    return jnp.concatenate([jnp.where(kept, position, -1.0).T, jnp.where(kept, gate_by_expert, 0.0).T], axis=0)


def moe_kernel(experts, capacity, ny, nx, u_in, resid, meta_in, w_gate, w_up, w_down, out, ug,
               w1, v1, w2, xg, hid, hpart, sums, rfar, rplus, rminus, yown, yfar, yplus, yminus, ycon, vfar, vplus, vminus, wsum, wown, wfar, wplus, wminus, fin, xres, utile, gsplit, meta,
               load_sem, tile_sem, send_sem, recv_sem):
    rows, d_model = resid.shape
    half = d_model // 2
    quarter = half // ny
    width = w_gate.shape[2]
    chunk = rows // 8
    sub = rows // SUBS
    tile = utile.shape[2]
    y = lax.axis_index('tp')
    ep = lax.axis_index('ep')
    core = lax.rem(ep, 2)
    x = ep // 2

    def ep_at(dx, other=False):
        return lax.rem(x + dx + nx, nx) * 2 + ((1 - core) if other else core)

    def dev_x(dx, other=False):
        return {'ep': ep_at(dx, other)}

    def dev_y(dy, other=False):
        return {'tp': lax.rem(y + dy + ny, ny), 'ep': ep_at(0, other)}

    partner = dev_x(0, True)

    barrier = pltpu.get_barrier_semaphore()
    peers = [dev_x(dx, o) for dx in range(nx) for o in (False, True) if (dx, o) != (0, False)]
    peers += [dev_y(dy, o) for dy in (1, -1) for o in (False, True)]
    for peer in peers:
        pl.semaphore_signal(barrier, inc=1, device_id=peer, device_id_type=MESH)
    pl.semaphore_wait(barrier, len(peers))

    copies = []

    def remote(src, dst, device):
        at = len(copies)
        copy = pltpu.make_async_remote_copy(src_ref=src, dst_ref=dst, send_sem=send_sem.at[at], recv_sem=recv_sem.at[at], device_id=device, device_id_type=MESH)
        copies.append(copy)
        copy.start()
        return copy

    sent = []

    def finish_send(copy):
        copy.wait_send()
        sent.append(copy)

    locals_ = []

    def local(src, dst):
        copy = pltpu.make_async_copy(src, dst, load_sem.at[len(locals_)])
        locals_.append(copy)
        copy.start()
        return copy

    my_half = pl.multiple_of(core * half, half)
    other_half = pl.multiple_of((1 - core) * half, half)
    my_quarter = pl.multiple_of(my_half + y * quarter, quarter)
    other_quarter = pl.multiple_of(other_half + y * quarter, quarter)

    parity = lax.rem(y, 2)

    def piece(q, mine=True):
        side = parity if mine else 1 - parity
        return pl.ds(pl.multiple_of(side * (rows // 2) + q * chunk, chunk), chunk)

    meta_copies = {}
    for slot, dx in ((0, 0), (1, 1), (2, -1), (3, 2)):
        for lane in range(2):
            if (slot, lane) == (0, 0):
                meta_copies[slot, lane] = local(meta_in, meta.at[0])
            else:
                meta_copies[slot, lane] = remote(meta_in, meta.at[slot * 2 + lane], dev_x(dx, lane == 1))
    ax = {}
    for q in range(4):
        ax[1, q] = remote(u_in.at[piece(q)], ug.at[1, 0, piece(q)], dev_x(1))
        ax[2, q] = remote(u_in.at[piece(q)], ug.at[2, 0, piece(q)], dev_x(-1))
    own_pair = remote(u_in, ug.at[0, 1], partner)
    loads = {}
    for e in range(2):
        loads[e] = (local(w_gate.at[e], w1.at[e]), local(w_up.at[e], v1.at[e]))
    w2_copies = [local(w_down.at[e, :, pl.ds(my_half, half)], w2.at[e]) for e in range(2)]
    w2_copies += [remote(w_down.at[e, :, pl.ds(other_half, half)], w2.at[2 + e], partner) for e in range(2)]
    res_copies = [local(resid.at[:, pl.ds(my_quarter, quarter)], xres.at[0]),
                  remote(resid.at[:, pl.ds(other_quarter, quarter)], xres.at[1], partner)]

    ay, pushed = {}, {1: [], 2: [], 3: []}

    def push(slot, q, mine):
        at = piece(q, mine)
        pushed[slot].append(remote(ug.at[slot, 0, at], ug.at[slot, 1, at], partner))

    def y_forward(slot, q):
        up = (q % 2 == 0) == (slot != 2)
        ay[slot, q] = remote(ug.at[slot, 0, piece(q)], ug.at[slot, 0, piece(q)], dev_y(1 if up else -1))

    def on_near(q):
        for slot in (1, 2):
            ax[slot, q].wait_recv()
            if (q % 2 == 0) == (slot == 1):
                ax[3, q] = remote(ug.at[slot, 0, piece(q)], ug.at[3, 0, piece(q)], dev_x(1 if slot == 1 else -1))
            y_forward(slot, q)
        for slot in (1, 2):
            push(slot, q, True)

    def on_far(q):
        ax[3, q].wait_recv()
        y_forward(3, q)
        push(3, q, True)

    def on_side(slot, q):
        ay[slot, q].wait_recv()
        push(slot, q, False)

    def slot_onehot(pos_row):
        return lax.broadcasted_iota(jnp.int32, (capacity, rows), 0).astype(F32) == pos_row

    def gather(slot):
        for lane in range(2):
            copy = meta_copies[slot, lane]
            copy.wait_recv() if copy.is_remote else copy.wait()
        picks = []
        for lane in range(2):
            parts = []
            for e in range(2):
                pos_row = meta[slot * 2 + lane, pl.ds(2 * ep + e, 1), :]
                parts.append(slot_onehot(pos_row).astype(F32).astype(BF16))
            picks.append(jnp.concatenate(parts, axis=0))
            gates = []
            for e in range(4):
                row = 2 * (ep if e < 2 else ep_at(0, True)) + e % 2
                pos_row = meta[slot * 2 + lane, pl.ds(row, 1), :]
                gate_row = meta[slot * 2 + lane, pl.ds(experts + row, 1), :]
                gates.append(jnp.where(slot_onehot(pos_row), gate_row, 0.0))
            gate_mat = jnp.concatenate(gates, axis=0).T
            for term in range(3):
                part = gate_mat.astype(BF16)
                gsplit[lane, term] = part
                gate_mat = gate_mat - part.astype(F32)

        tiles = d_model // tile

        def fetch(t, lane):
            cols = pl.ds(pl.multiple_of(t * tile, tile), tile)
            src = u_in.at[:, cols] if (slot, lane) == (0, 0) else ug.at[slot, lane, :, cols]
            at = lax.rem(t, 2) * 2 + lane
            return pltpu.make_async_copy(src, utile.at[at], tile_sem.at[at])

        for lane in range(2):
            fetch(0, lane).start()

        def body(t, carry):
            @pl.when(t + 1 < tiles)
            def _():
                for lane in range(2):
                    fetch(t + 1, lane).start()
            cols = pl.ds(pl.multiple_of(t * tile, tile), tile)
            for lane in range(2):
                fetch(t, lane).wait()
                got = jnp.dot(picks[lane], utile[lax.rem(t, 2) * 2 + lane], preferred_element_type=F32).astype(BF16)
                for e in range(2):
                    xg[e, lane * capacity:(lane + 1) * capacity, cols] = got[e * capacity:(e + 1) * capacity]
            return carry

        lax.fori_loop(0, tiles, body, 0)

    ftile = min(256, width)

    def gate_up(e):
        def body(t, carry):
            cols = pl.ds(pl.multiple_of(t * ftile, ftile), ftile)
            gate_act = jnp.dot(xg[e], w1[e, :, cols], preferred_element_type=F32)
            up_act = jnp.dot(xg[e], v1[e, :, cols], preferred_element_type=F32)
            hid[e, :, cols] = (jax.nn.silu(gate_act) * up_act).astype(BF16)
            return carry

        lax.fori_loop(0, width // ftile, body, 0)

    xcols = yfar.shape[2]
    ycols = quarter - xcols

    def share_hidden(slot):
        return remote(hid, hpart.at[slot], partner)

    def down(slot):
        def body(t, carry):
            cols = pl.ds(pl.multiple_of(t * quarter, quarter), quarter)
            outs = []
            for e in range(4):
                lhs = hid[e] if e < 2 else hpart[slot, e - 2]
                outs.append(jnp.dot(lhs, w2[e, :, cols], preferred_element_type=F32).astype(BF16))
            for lane in range(2):
                stack = []
                for e in range(4):
                    at = lane if e < 2 else 1 - lane
                    stack.append(outs[e][at * capacity:(at + 1) * capacity])
                stacked = jnp.concatenate(stack, axis=0)
                total = jnp.dot(gsplit[lane, 0], stacked, preferred_element_type=F32)
                for term in (1, 2):
                    total += jnp.dot(gsplit[lane, term], stacked, preferred_element_type=F32)
                total = total.astype(BF16)
                sums[slot, lane, :, pl.ds(pl.multiple_of(t * xcols, 128), xcols)] = total[:, :xcols]
                ycon[slot, lane, :, pl.ds(pl.multiple_of(t * ycols, 128), ycols)] = total[:, xcols:]
            return carry

        lax.fori_loop(0, ny, body, 0)

    rs = {}

    def add_into(ref, other):
        ref[...] = (ref[...].astype(F32) + other[...].astype(F32)).astype(BF16)

    def rs_start(tag, src, landing, dev):
        far, plus, minus = landing
        rs[tag] = {'f0': remote(src(2, 0), far.at[0], dev(1)), 'f1': remote(src(2, 1), far.at[1], dev(-1)),
                   'p1': remote(src(1, 1), plus.at[1], dev(1)), 'm0': remote(src(-1, 0), minus.at[0], dev(-1))}

    def rs_mid(tag, src, landing, dev):
        far, plus, minus = landing
        rs[tag]['f0'].wait_recv()
        add_into(src(1, 0), far.at[0])
        rs[tag]['p0'] = remote(src(1, 0), plus.at[0], dev(1))
        rs[tag]['f1'].wait_recv()
        add_into(src(-1, 1), far.at[1])
        rs[tag]['m1'] = remote(src(-1, 1), minus.at[1], dev(-1))

    def rs_end(tag):
        for name in ('m0', 'p1', 'p0', 'm1'):
            rs[tag][name].wait_recv()

    def y_args(slot):
        def src(dy, lane):
            return ycon.at[slot, lane, :, pl.ds(pl.multiple_of(lax.rem(y + dy + ny, ny) * ycols, 128), ycols)]
        return src, (vfar.at[slot], vplus.at[slot], vminus.at[slot]), dev_y

    def y_start(slot):
        rs_start(slot, *y_args(slot))

    def y_mid(slot):
        rs_mid(slot, *y_args(slot))

    def y_end(slot):
        rs_end(slot)
        src = y_args(slot)[0]
        for lane in range(2):
            total = src(0, lane)[...].astype(F32) + vplus[slot, lane].astype(F32) + vminus[slot, lane].astype(F32)
            if slot == 0:
                wown[lane] = total
            else:
                wsum[slot - 1, lane] = total.astype(BF16)

    def w_src(dx, lane):
        return wsum.at[{-1: 0, 1: 1, 2: 2}[dx], lane]

    w_args = (w_src, (wfar, wplus, wminus), dev_x)

    def w_end():
        rs_end('w')
        for lane in range(2):
            wown[lane] += wplus[lane].astype(F32) + wminus[lane].astype(F32)

    own_pair.wait_recv()
    gather(0)
    for copy in loads[0]:
        copy.wait()
    gate_up(0)
    on_near(0)
    for copy in loads[1]:
        copy.wait()
    gate_up(1)
    hs = share_hidden(0)
    on_near(1)
    for copy in w2_copies:
        copy.wait_recv() if copy.is_remote else copy.wait()
    hs.wait_recv()
    down(0)
    finish_send(hs)
    on_near(2)
    for q in (0, 1):
        on_side(1, q)
        on_side(2, q)
    on_near(3)
    for q in (2,):
        on_side(1, q)
        on_side(2, q)
    on_far(0)
    on_far(1)
    for q in (3,):
        on_side(1, q)
        on_side(2, q)

    def chip_pair(slot, between):
        for copy in pushed[slot]:
            copy.wait_recv()
        gather(slot)
        gate_up(0)
        between(0)
        gate_up(1)
        between(1)
        hs = share_hidden(slot)
        between(2)
        hs.wait_recv()
        down(slot)
        finish_send(hs)

    def sub_rows(j):
        return pl.ds(j * sub, sub)

    sx = {}

    def send_sum(name, slot, lane, j, landing, dx):
        sx[name, j] = remote(sums.at[slot, lane, sub_rows(j)], landing.at[lane, sub_rows(j)], dev_x(dx))

    def during_left(step):
        if step < 2:
            on_far(2 + step)
        else:
            y_start(0)

    def during_right(step):
        for q in ((0, 1), (2,), (3,))[step]:
            on_side(3, q)
        if step == 1:
            y_mid(0)
            y_mid(1)

    def during_far(step):
        if step == 0:
            y_end(0)
            y_end(1)
        if step == 1:
            y_mid(2)
        if step == 2:
            y_end(2)

    chip_pair(1, during_left)
    for j in range(SUBS):
        send_sum('m0', 1, 0, j, rminus, -1)
    y_start(1)
    chip_pair(2, during_right)
    for j in range(SUBS):
        send_sum('p1', 2, 1, j, rplus, 1)
    y_start(2)
    chip_pair(3, during_far)

    def send_far(j):
        send_sum('f0', 3, 0, j, rfar, 1)
        send_sum('f1', 3, 1, j, rfar, -1)

    def q_cols(dy):
        return pl.ds(pl.multiple_of(lax.rem(y + dy + ny, ny) * xcols, 128), xcols)

    def stage_far(j):
        sx['f0', j].wait_recv()
        sx['f1', j].wait_recv()
        at = sub_rows(j)
        sums[2, 0, at, :] = (sums[2, 0, at, :].astype(F32) + rfar[0, at, :].astype(F32)).astype(BF16)
        send_sum('p0', 2, 0, j, rplus, 1)
        sums[1, 1, at, :] = (sums[1, 1, at, :].astype(F32) + rfar[1, at, :].astype(F32)).astype(BF16)
        send_sum('m1', 1, 1, j, rminus, -1)
        if j + 2 < SUBS:
            send_far(j + 2)

    def send_y(name, lane, j, dcol, landing, dy):
        sx[name, j] = remote(sums.at[0, lane, sub_rows(j), q_cols(dcol)], landing.at[lane, sub_rows(j)], dev_y(dy))

    def stage_own(j):
        for name in ('m0', 'p1', 'p0', 'm1'):
            sx[name, j].wait_recv()
        at = sub_rows(j)
        for lane in range(2):
            cols = q_cols(0)
            yown[lane, at, :] = sums[0, lane, at, cols].astype(F32) + rplus[lane, at, cols].astype(F32) + rminus[lane, at, cols].astype(F32)
        for lane in range(2):
            sums[0, lane, at, :] = (sums[0, lane, at, :].astype(F32) + rplus[lane, at, :].astype(F32) + rminus[lane, at, :].astype(F32)).astype(BF16)
        send_y('yf0', 0, j, 2, yfar, 1)
        send_y('yf1', 1, j, 2, yfar, -1)
        send_y('yp1', 1, j, 1, yplus, 1)
        send_y('ym0', 0, j, -1, yminus, -1)

    def stage_yfar(j):
        sx['yf0', j].wait_recv()
        sx['yf1', j].wait_recv()
        at = sub_rows(j)
        cols = q_cols(1)
        sums[0, 0, at, cols] = (sums[0, 0, at, cols].astype(F32) + yfar[0, at, :].astype(F32)).astype(BF16)
        send_y('yp0', 0, j, 1, yplus, 1)
        cols = q_cols(-1)
        sums[0, 1, at, cols] = (sums[0, 1, at, cols].astype(F32) + yfar[1, at, :].astype(F32)).astype(BF16)
        send_y('ym1', 1, j, -1, yminus, -1)

    done = {}

    def stage_final(j):
        for name in ('ym0', 'yp1', 'yp0', 'ym1'):
            sx[name, j].wait_recv()
        at = sub_rows(j)
        for lane in range(2):
            total = yown[lane, at, :] + yplus[lane, at, :].astype(F32) + yminus[lane, at, :].astype(F32)
            fin[lane, at, :xcols] = (xres[lane, at, :xcols].astype(F32) + total).astype(BF16)
            fin[lane, at, xcols:] = (xres[lane, at, xcols:].astype(F32) + wown[lane, at, :]).astype(BF16)
        place = out.at[at, pl.ds(my_quarter, quarter)]
        for lane in range(2):
            done['up', lane, j] = remote(fin.at[lane, at], place, dev_y(1, lane == 1))
            done['down', lane, j] = remote(fin.at[lane, at], place, dev_y(-1, lane == 1))
        done['own', j] = local(fin.at[0, at], place)
        done['pair', j] = remote(fin.at[1, at], place, partner)

    def stage_relay(j):
        at = sub_rows(j)
        done['up', 0, j].wait_recv()
        cols = pl.ds(pl.multiple_of(my_half + lax.rem(y - 1 + ny, ny) * quarter, quarter), quarter)
        done['up2', j] = remote(out.at[at, cols], out.at[at, cols], dev_y(1))
        done['down', 1, j].wait_recv()
        cols = pl.ds(pl.multiple_of(other_half + lax.rem(y + 1, ny) * quarter, quarter), quarter)
        done['down2', j] = remote(out.at[at, cols], out.at[at, cols], dev_y(-1))

    for copy in res_copies:
        copy.wait_recv() if copy.is_remote else copy.wait()
    send_far(0)
    send_far(1)
    y_start(3)
    stages = (stage_far, stage_own, stage_yfar, stage_final, stage_relay)
    for step in range(SUBS + len(stages) - 1):
        if step == 3:
            w_end()
        for lag, stage in enumerate(stages):
            if 0 <= step - lag < SUBS:
                stage(step - lag)
        if step == 0:
            y_mid(3)
        if step == 1:
            y_end(3)
            rs_start('w', *w_args)
        if step == 2:
            rs_mid('w', *w_args)
    for j in range(SUBS):
        done['up', 1, j].wait_recv()
        done['down', 0, j].wait_recv()
        done['pair', j].wait_recv()
        done['up2', j].wait_recv()
        done['down2', j].wait_recv()
        done['own', j].wait()
    for copy in copies:
        if not any(copy is other for other in sent):
            copy.wait_send()


def solution(mesh):
    row_spec = P(('dp', 'ep'), None)
    ny, nx = mesh.shape['tp'], mesh.shape['ep'] // 2

    def device_step(resid_in, norm_scale, w_router, w_gate, w_up, w_down, choice):
        rows, d_model = resid_in.shape
        experts = w_router.shape[1]
        width = w_gate.shape[2]
        capacity = (2 * rows * choice.shape[1] + experts - 1) // experts
        normed, gate_by_expert, is_chosen = norm_route(resid_in, norm_scale, w_router, choice)
        meta = slot_meta(gate_by_expert, is_chosen, capacity)
        half, slots = d_model // 2, 2 * capacity
        quarter = half // ny
        tile = min(512, d_model)
        ycols = 128
        xcols = quarter - ycols

        hbm = pl.BlockSpec(memory_space=pl.ANY)
        out, _ = pl.pallas_call(
            functools.partial(moe_kernel, experts, capacity, ny, nx),
            out_shape=(jax.ShapeDtypeStruct((rows, d_model), BF16), jax.ShapeDtypeStruct((4, 2, rows, d_model), BF16)),
            in_specs=[hbm] * 6,
            out_specs=(hbm, hbm),
            scratch_shapes=[
                pltpu.VMEM((2, d_model, width), BF16),
                pltpu.VMEM((2, d_model, width), BF16),
                pltpu.VMEM((4, width, half), BF16),
                pltpu.VMEM((2, slots, d_model), BF16),
                pltpu.VMEM((2, slots, width), BF16),
                pltpu.VMEM((4, 2, slots, width), BF16),
                pltpu.VMEM((4, 2, rows, ny * xcols), BF16),
                pltpu.VMEM((2, rows, ny * xcols), BF16),
                pltpu.VMEM((2, rows, ny * xcols), BF16),
                pltpu.VMEM((2, rows, ny * xcols), BF16),
                pltpu.VMEM((2, rows, xcols), F32),
                pltpu.VMEM((2, rows, xcols), BF16),
                pltpu.VMEM((2, rows, xcols), BF16),
                pltpu.VMEM((2, rows, xcols), BF16),
                pltpu.VMEM((4, 2, rows, ny * ycols), BF16),
                pltpu.VMEM((4, 2, rows, ycols), BF16),
                pltpu.VMEM((4, 2, rows, ycols), BF16),
                pltpu.VMEM((4, 2, rows, ycols), BF16),
                pltpu.VMEM((3, 2, rows, ycols), BF16),
                pltpu.VMEM((2, rows, ycols), F32),
                pltpu.VMEM((2, rows, ycols), BF16),
                pltpu.VMEM((2, rows, ycols), BF16),
                pltpu.VMEM((2, rows, ycols), BF16),
                pltpu.VMEM((2, rows, quarter), BF16),
                pltpu.VMEM((2, rows, quarter), BF16),
                pltpu.VMEM((4, rows, tile), BF16),
                pltpu.VMEM((2, 3, rows, 4 * capacity), BF16),
                pltpu.VMEM((8, 2 * experts, rows), F32),
                pltpu.SemaphoreType.DMA((16,)),
                pltpu.SemaphoreType.DMA((4,)),
                pltpu.SemaphoreType.DMA((256,)),
                pltpu.SemaphoreType.DMA((256,)),
            ],
            compiler_params=pltpu.CompilerParams(collective_id=0, has_side_effects=True, vmem_limit_bytes=67043328),
            name='moe_ring',
        )(normed, resid_in, meta, w_gate, w_up, w_down)
        return out

    return jax.shard_map(device_step, mesh=mesh, in_specs=(row_spec, P(None), P(None, None), P('ep', None, 'tp'), P('ep', None, 'tp'), P('ep', 'tp', None), row_spec), out_specs=row_spec, check_vma=False)
```

```python
import functools

import jax
import jax.numpy as jnp
from jax import lax
from jax.experimental import pallas as pl
from jax.experimental.pallas import tpu as pltpu
from jax.sharding import PartitionSpec as P

NORM_EPS = 1e-5
MESH = pl.DeviceIdType.MESH
BF16 = jnp.bfloat16
F32 = jnp.float32
SUBS = 4


def norm_route(resid_rows, norm_scale, w_router, choice_rows):
    rows_f32 = resid_rows.astype(F32)
    centered = rows_f32 - jnp.mean(rows_f32, axis=-1, keepdims=True)
    variance = jnp.mean(centered * centered, axis=-1, keepdims=True)
    normed = (centered * lax.rsqrt(variance + NORM_EPS) * norm_scale.astype(F32)).astype(BF16)
    logits = jnp.dot(normed, w_router, preferred_element_type=F32)
    router_probs = jax.nn.softmax(logits, axis=-1)
    expert_ids = jnp.arange(w_router.shape[1], dtype=jnp.int32)
    chosen = choice_rows[:, :, None] == expert_ids[None, None, :]
    picked = jnp.sum(jnp.where(chosen, router_probs[:, None, :], 0.0), axis=-1)
    gate_vals = picked / jnp.sum(picked, axis=-1, keepdims=True)
    gate_by_expert = jnp.sum(jnp.where(chosen, gate_vals[:, :, None], 0.0), axis=1)
    return normed, gate_by_expert, jnp.any(chosen, axis=1)


def slot_meta(gate_by_expert, is_chosen, capacity):
    rows = is_chosen.shape[0]
    earlier = jnp.arange(rows)[:, None] > jnp.arange(rows)[None, :]
    position = jnp.dot(earlier.astype(BF16), is_chosen.astype(BF16), preferred_element_type=F32)
    kept = is_chosen & (position < capacity)
    return jnp.concatenate([jnp.where(kept, position, -1.0).T, jnp.where(kept, gate_by_expert, 0.0).T], axis=0)


def moe_kernel(experts, capacity, ny, nx, u_in, resid, meta_in, w_gate, w_up, w_down, out, ug,
               w1, v1, w2, xg, hid, hpart, sums, rfar, rplus, rminus, yown, yfar, yplus, yminus, ycon, vfar, vplus, vminus, wsum, wown, wfar, wplus, wminus, fin, xres, utile, gsplit, meta,
               load_sem, tile_sem, send_sem, recv_sem):
    rows, d_model = resid.shape
    half = d_model // 2
    quarter = half // ny
    width = w_gate.shape[2]
    chunk = rows // 8
    sub = rows // SUBS
    y = lax.axis_index('tp')
    ep = lax.axis_index('ep')
    core = lax.rem(ep, 2)
    x = ep // 2

    def ep_at(dx, other=False):
        return lax.rem(x + dx + nx, nx) * 2 + ((1 - core) if other else core)

    def dev_x(dx, other=False):
        return {'ep': ep_at(dx, other)}

    def dev_y(dy, other=False):
        return {'tp': lax.rem(y + dy + ny, ny), 'ep': ep_at(0, other)}

    partner = dev_x(0, True)

    barrier = pltpu.get_barrier_semaphore()
    peers = [dev_x(dx, o) for dx in range(nx) for o in (False, True) if (dx, o) != (0, False)]
    peers += [dev_y(dy, o) for dy in (1, -1) for o in (False, True)]
    for peer in peers:
        pl.semaphore_signal(barrier, inc=1, device_id=peer, device_id_type=MESH)
    pl.semaphore_wait(barrier, len(peers))

    copies = []

    def remote(src, dst, device):
        at = len(copies)
        copy = pltpu.make_async_remote_copy(src_ref=src, dst_ref=dst, send_sem=send_sem.at[at], recv_sem=recv_sem.at[at], device_id=device, device_id_type=MESH)
        copies.append(copy)
        copy.start()
        return copy

    sent = []

    def finish_send(copy):
        copy.wait_send()
        sent.append(copy)

    locals_ = []

    def local(src, dst):
        copy = pltpu.make_async_copy(src, dst, load_sem.at[len(locals_)])
        locals_.append(copy)
        copy.start()
        return copy

    my_half = pl.multiple_of(core * half, half)
    other_half = pl.multiple_of((1 - core) * half, half)
    my_quarter = pl.multiple_of(my_half + y * quarter, quarter)
    other_quarter = pl.multiple_of(other_half + y * quarter, quarter)

    parity = lax.rem(y, 2)

    def piece(q, mine=True):
        side = parity if mine else 1 - parity
        return pl.ds(pl.multiple_of(side * (rows // 2) + q * chunk, chunk), chunk)

    meta_copies = {}
    for slot, dx in ((0, 0), (1, 1), (2, -1), (3, 2)):
        for lane in range(2):
            if (slot, lane) == (0, 0):
                meta_copies[slot, lane] = local(meta_in, meta.at[0])
            else:
                meta_copies[slot, lane] = remote(meta_in, meta.at[slot * 2 + lane], dev_x(dx, lane == 1))
    ax = {}
    for q in range(4):
        ax[1, q] = remote(u_in.at[piece(q)], ug.at[1, 0, piece(q)], dev_x(1))
        ax[2, q] = remote(u_in.at[piece(q)], ug.at[2, 0, piece(q)], dev_x(-1))
    own_pair = remote(u_in, ug.at[0, 1], partner)
    loads = {}
    for e in range(2):
        loads[e] = (local(w_gate.at[e], w1.at[e]), local(w_up.at[e], v1.at[e]))
    w2_copies = [local(w_down.at[e, :, pl.ds(my_half, half)], w2.at[e]) for e in range(2)]
    w2_copies += [remote(w_down.at[e, :, pl.ds(other_half, half)], w2.at[2 + e], partner) for e in range(2)]
    res_copies = [local(resid.at[:, pl.ds(my_quarter, quarter)], xres.at[0]),
                  remote(resid.at[:, pl.ds(other_quarter, quarter)], xres.at[1], partner)]

    ay, pushed = {}, {1: [], 2: [], 3: []}

    def push(slot, q, mine):
        at = piece(q, mine)
        pushed[slot].append(remote(ug.at[slot, 0, at], ug.at[slot, 1, at], partner))

    def y_forward(slot, q):
        up = (q % 2 == 0) == (slot != 2)
        ay[slot, q] = remote(ug.at[slot, 0, piece(q)], ug.at[slot, 0, piece(q)], dev_y(1 if up else -1))

    def on_near(q):
        for slot in (1, 2):
            ax[slot, q].wait_recv()
            if (q % 2 == 0) == (slot == 1):
                ax[3, q] = remote(ug.at[slot, 0, piece(q)], ug.at[3, 0, piece(q)], dev_x(1 if slot == 1 else -1))
            y_forward(slot, q)
        for slot in (1, 2):
            push(slot, q, True)

    def on_far(q):
        ax[3, q].wait_recv()
        y_forward(3, q)
        push(3, q, True)

    def on_side(slot, q):
        ay[slot, q].wait_recv()
        push(slot, q, False)

    def slot_onehot(pos_row):
        return lax.broadcasted_iota(jnp.int32, (capacity, rows), 0).astype(F32) == pos_row

    tile = min(512, d_model)
    tiles = d_model // tile

    def fetch(slot, t, lane):
        cols = pl.ds(t * tile, tile) if isinstance(t, int) else pl.ds(pl.multiple_of(t * tile, tile), tile)
        src = u_in.at[:, cols] if (slot, lane) == (0, 0) else ug.at[slot, lane, :, cols]
        return pltpu.make_async_copy(src, utile.at[lane, :, cols], tile_sem.at[lane * tiles + t])

    def prefetch(slot):
        for copy in pushed.get(slot, ()):
            copy.wait_recv()
        for t in range(tiles):
            for lane in range(2):
                fetch(slot, t, lane).start()

    def gather(slot):
        for lane in range(2):
            copy = meta_copies[slot, lane]
            copy.wait_recv() if copy.is_remote else copy.wait()
        picks = []
        for lane in range(2):
            parts = []
            for e in range(2):
                pos_row = meta[slot * 2 + lane, pl.ds(2 * ep + e, 1), :]
                parts.append(slot_onehot(pos_row).astype(F32).astype(BF16))
            picks.append(jnp.concatenate(parts, axis=0))
            gates = []
            for e in range(4):
                row = 2 * (ep if e < 2 else ep_at(0, True)) + e % 2
                pos_row = meta[slot * 2 + lane, pl.ds(row, 1), :]
                gate_row = meta[slot * 2 + lane, pl.ds(experts + row, 1), :]
                gates.append(jnp.where(slot_onehot(pos_row), gate_row, 0.0))
            gate_mat = jnp.concatenate(gates, axis=0).T
            for term in range(3):
                part = gate_mat.astype(BF16)
                gsplit[lane, term] = part
                gate_mat = gate_mat - part.astype(F32)

        def body(t, carry):
            cols = pl.ds(pl.multiple_of(t * tile, tile), tile)
            for lane in range(2):
                fetch(slot, t, lane).wait()
                got = jnp.dot(picks[lane], utile[lane, :, cols], preferred_element_type=F32).astype(BF16)
                for e in range(2):
                    xg[e, lane * capacity:(lane + 1) * capacity, cols] = got[e * capacity:(e + 1) * capacity]
            return carry

        lax.fori_loop(0, tiles, body, 0)

    ftile = min(256, width)

    def gate_up(e):
        def body(t, carry):
            cols = pl.ds(pl.multiple_of(t * ftile, ftile), ftile)
            gate_act = jnp.dot(xg[e], w1[e, :, cols], preferred_element_type=F32)
            up_act = jnp.dot(xg[e], v1[e, :, cols], preferred_element_type=F32)
            hid[e, :, cols] = (jax.nn.silu(gate_act) * up_act).astype(BF16)
            return carry

        lax.fori_loop(0, width // ftile, body, 0)

    xcols = yfar.shape[2]
    ycols = quarter - xcols

    def share_hidden(slot):
        return remote(hid, hpart.at[slot], partner)

    def down(slot):
        def body(t, carry):
            cols = pl.ds(pl.multiple_of(t * quarter, quarter), quarter)
            outs = []
            for e in range(4):
                lhs = hid[e] if e < 2 else hpart[slot, e - 2]
                outs.append(jnp.dot(lhs, w2[e, :, cols], preferred_element_type=F32).astype(BF16))
            for lane in range(2):
                stack = []
                for e in range(4):
                    at = lane if e < 2 else 1 - lane
                    stack.append(outs[e][at * capacity:(at + 1) * capacity])
                stacked = jnp.concatenate(stack, axis=0)
                total = jnp.dot(gsplit[lane, 0], stacked, preferred_element_type=F32)
                for term in (1, 2):
                    total += jnp.dot(gsplit[lane, term], stacked, preferred_element_type=F32)
                total = total.astype(BF16)
                sums[slot, lane, :, pl.ds(pl.multiple_of(t * xcols, 128), xcols)] = total[:, :xcols]
                ycon[slot, lane, :, pl.ds(pl.multiple_of(t * ycols, 128), ycols)] = total[:, xcols:]
            return carry

        lax.fori_loop(0, ny, body, 0)

    rs = {}

    def add_into(ref, other):
        ref[...] = (ref[...].astype(F32) + other[...].astype(F32)).astype(BF16)

    def rs_start(tag, src, landing, dev):
        far, plus, minus = landing
        rs[tag] = {'f0': remote(src(2, 0), far.at[0], dev(1)), 'f1': remote(src(2, 1), far.at[1], dev(-1)),
                   'p1': remote(src(1, 1), plus.at[1], dev(1)), 'm0': remote(src(-1, 0), minus.at[0], dev(-1))}

    def rs_mid(tag, src, landing, dev):
        far, plus, minus = landing
        rs[tag]['f0'].wait_recv()
        add_into(src(1, 0), far.at[0])
        rs[tag]['p0'] = remote(src(1, 0), plus.at[0], dev(1))
        rs[tag]['f1'].wait_recv()
        add_into(src(-1, 1), far.at[1])
        rs[tag]['m1'] = remote(src(-1, 1), minus.at[1], dev(-1))

    def rs_end(tag):
        for name in ('m0', 'p1', 'p0', 'm1'):
            rs[tag][name].wait_recv()

    def y_args(slot):
        def src(dy, lane):
            return ycon.at[slot, lane, :, pl.ds(pl.multiple_of(lax.rem(y + dy + ny, ny) * ycols, 128), ycols)]
        return src, (vfar.at[slot], vplus.at[slot], vminus.at[slot]), dev_y

    def y_start(slot):
        rs_start(slot, *y_args(slot))

    def y_mid(slot):
        rs_mid(slot, *y_args(slot))

    def y_end(slot):
        rs_end(slot)
        src = y_args(slot)[0]
        for lane in range(2):
            total = src(0, lane)[...].astype(F32) + vplus[slot, lane].astype(F32) + vminus[slot, lane].astype(F32)
            if slot == 0:
                wown[lane] = total
            else:
                wsum[slot - 1, lane] = total.astype(BF16)

    def w_src(dx, lane):
        return wsum.at[{-1: 0, 1: 1, 2: 2}[dx], lane]

    w_args = (w_src, (wfar, wplus, wminus), dev_x)

    def w_end():
        rs_end('w')
        for lane in range(2):
            wown[lane] += wplus[lane].astype(F32) + wminus[lane].astype(F32)

    own_pair.wait_recv()
    prefetch(0)
    gather(0)
    for copy in loads[0]:
        copy.wait()
    gate_up(0)
    on_near(0)
    for copy in loads[1]:
        copy.wait()
    gate_up(1)
    hs = share_hidden(0)
    on_near(1)
    for copy in w2_copies:
        copy.wait_recv() if copy.is_remote else copy.wait()
    hs.wait_recv()
    down(0)
    finish_send(hs)
    on_near(2)
    for q in (0, 1):
        on_side(1, q)
        on_side(2, q)
    on_near(3)
    for q in (2,):
        on_side(1, q)
        on_side(2, q)
    on_far(0)
    on_far(1)
    for q in (3,):
        on_side(1, q)
        on_side(2, q)

    def chip_pair(slot, between):
        gather(slot)
        if slot == 1:
            prefetch(2)
        gate_up(0)
        between(0)
        gate_up(1)
        between(1)
        hs = share_hidden(slot)
        between(2)
        hs.wait_recv()
        down(slot)
        finish_send(hs)

    def sub_rows(j):
        return pl.ds(j * sub, sub)

    sx = {}

    def send_sum(name, slot, lane, j, landing, dx):
        sx[name, j] = remote(sums.at[slot, lane, sub_rows(j)], landing.at[lane, sub_rows(j)], dev_x(dx))

    def during_left(step):
        if step < 2:
            on_far(2 + step)
        else:
            y_start(0)

    def during_right(step):
        for q in ((0, 1), (2,), (3,))[step]:
            on_side(3, q)
        if step == 1:
            y_mid(0)
            y_mid(1)
        if step == 2:
            prefetch(3)

    def during_far(step):
        if step == 0:
            y_end(0)
            y_end(1)
        if step == 1:
            y_mid(2)
        if step == 2:
            y_end(2)

    prefetch(1)
    chip_pair(1, during_left)
    for j in range(SUBS):
        send_sum('m0', 1, 0, j, rminus, -1)
    y_start(1)
    chip_pair(2, during_right)
    for j in range(SUBS):
        send_sum('p1', 2, 1, j, rplus, 1)
    y_start(2)
    chip_pair(3, during_far)

    def send_far(j):
        send_sum('f0', 3, 0, j, rfar, 1)
        send_sum('f1', 3, 1, j, rfar, -1)

    def q_cols(dy):
        return pl.ds(pl.multiple_of(lax.rem(y + dy + ny, ny) * xcols, 128), xcols)

    def stage_far(j):
        sx['f0', j].wait_recv()
        sx['f1', j].wait_recv()
        at = sub_rows(j)
        sums[2, 0, at, :] = (sums[2, 0, at, :].astype(F32) + rfar[0, at, :].astype(F32)).astype(BF16)
        send_sum('p0', 2, 0, j, rplus, 1)
        sums[1, 1, at, :] = (sums[1, 1, at, :].astype(F32) + rfar[1, at, :].astype(F32)).astype(BF16)
        send_sum('m1', 1, 1, j, rminus, -1)
        if j + 2 < SUBS:
            send_far(j + 2)

    def send_y(name, lane, j, dcol, landing, dy):
        sx[name, j] = remote(sums.at[0, lane, sub_rows(j), q_cols(dcol)], landing.at[lane, sub_rows(j)], dev_y(dy))

    def stage_own(j):
        for name in ('m0', 'p1', 'p0', 'm1'):
            sx[name, j].wait_recv()
        at = sub_rows(j)
        for lane in range(2):
            cols = q_cols(0)
            yown[lane, at, :] = sums[0, lane, at, cols].astype(F32) + rplus[lane, at, cols].astype(F32) + rminus[lane, at, cols].astype(F32)
        for lane in range(2):
            sums[0, lane, at, :] = (sums[0, lane, at, :].astype(F32) + rplus[lane, at, :].astype(F32) + rminus[lane, at, :].astype(F32)).astype(BF16)
        send_y('yf0', 0, j, 2, yfar, 1)
        send_y('yf1', 1, j, 2, yfar, -1)
        send_y('yp1', 1, j, 1, yplus, 1)
        send_y('ym0', 0, j, -1, yminus, -1)

    def stage_yfar(j):
        sx['yf0', j].wait_recv()
        sx['yf1', j].wait_recv()
        at = sub_rows(j)
        cols = q_cols(1)
        sums[0, 0, at, cols] = (sums[0, 0, at, cols].astype(F32) + yfar[0, at, :].astype(F32)).astype(BF16)
        send_y('yp0', 0, j, 1, yplus, 1)
        cols = q_cols(-1)
        sums[0, 1, at, cols] = (sums[0, 1, at, cols].astype(F32) + yfar[1, at, :].astype(F32)).astype(BF16)
        send_y('ym1', 1, j, -1, yminus, -1)

    done = {}

    def stage_final(j):
        for name in ('ym0', 'yp1', 'yp0', 'ym1'):
            sx[name, j].wait_recv()
        at = sub_rows(j)
        for lane in range(2):
            total = yown[lane, at, :] + yplus[lane, at, :].astype(F32) + yminus[lane, at, :].astype(F32)
            fin[lane, at, :xcols] = (xres[lane, at, :xcols].astype(F32) + total).astype(BF16)
            fin[lane, at, xcols:] = (xres[lane, at, xcols:].astype(F32) + wown[lane, at, :]).astype(BF16)
        place = out.at[at, pl.ds(my_quarter, quarter)]
        for lane in range(2):
            done['up', lane, j] = remote(fin.at[lane, at], place, dev_y(1, lane == 1))
            done['down', lane, j] = remote(fin.at[lane, at], place, dev_y(-1, lane == 1))
        done['own', j] = local(fin.at[0, at], place)
        done['pair', j] = remote(fin.at[1, at], place, partner)

    def stage_relay(j):
        at = sub_rows(j)
        done['up', 0, j].wait_recv()
        cols = pl.ds(pl.multiple_of(my_half + lax.rem(y - 1 + ny, ny) * quarter, quarter), quarter)
        done['up2', j] = remote(out.at[at, cols], out.at[at, cols], dev_y(1))
        done['down', 1, j].wait_recv()
        cols = pl.ds(pl.multiple_of(other_half + lax.rem(y + 1, ny) * quarter, quarter), quarter)
        done['down2', j] = remote(out.at[at, cols], out.at[at, cols], dev_y(-1))

    for copy in res_copies:
        copy.wait_recv() if copy.is_remote else copy.wait()
    send_far(0)
    send_far(1)
    y_start(3)
    stages = (stage_far, stage_own, stage_yfar, stage_final, stage_relay)
    for step in range(SUBS + len(stages) - 1):
        if step == 3:
            w_end()
        for lag, stage in enumerate(stages):
            if 0 <= step - lag < SUBS:
                stage(step - lag)
        if step == 0:
            y_mid(3)
        if step == 1:
            y_end(3)
            rs_start('w', *w_args)
        if step == 2:
            rs_mid('w', *w_args)
    for j in range(SUBS):
        done['up', 1, j].wait_recv()
        done['down', 0, j].wait_recv()
        done['pair', j].wait_recv()
        done['up2', j].wait_recv()
        done['down2', j].wait_recv()
        done['own', j].wait()
    for copy in copies:
        if not any(copy is other for other in sent):
            copy.wait_send()


def solution(mesh):
    row_spec = P(('dp', 'ep'), None)
    ny, nx = mesh.shape['tp'], mesh.shape['ep'] // 2

    def device_step(resid_in, norm_scale, w_router, w_gate, w_up, w_down, choice):
        rows, d_model = resid_in.shape
        experts = w_router.shape[1]
        width = w_gate.shape[2]
        capacity = (2 * rows * choice.shape[1] + experts - 1) // experts
        normed, gate_by_expert, is_chosen = norm_route(resid_in, norm_scale, w_router, choice)
        meta = slot_meta(gate_by_expert, is_chosen, capacity)
        half, slots = d_model // 2, 2 * capacity
        quarter = half // ny
        ycols = 128
        xcols = quarter - ycols

        hbm = pl.BlockSpec(memory_space=pl.ANY)
        out, _ = pl.pallas_call(
            functools.partial(moe_kernel, experts, capacity, ny, nx),
            out_shape=(jax.ShapeDtypeStruct((rows, d_model), BF16), jax.ShapeDtypeStruct((4, 2, rows, d_model), BF16)),
            in_specs=[hbm] * 6,
            out_specs=(hbm, hbm),
            scratch_shapes=[
                pltpu.VMEM((2, d_model, width), BF16),
                pltpu.VMEM((2, d_model, width), BF16),
                pltpu.VMEM((4, width, half), BF16),
                pltpu.VMEM((2, slots, d_model), BF16),
                pltpu.VMEM((2, slots, width), BF16),
                pltpu.VMEM((4, 2, slots, width), BF16),
                pltpu.VMEM((4, 2, rows, ny * xcols), BF16),
                pltpu.VMEM((2, rows, ny * xcols), BF16),
                pltpu.VMEM((2, rows, ny * xcols), BF16),
                pltpu.VMEM((2, rows, ny * xcols), BF16),
                pltpu.VMEM((2, rows, xcols), F32),
                pltpu.VMEM((2, rows, xcols), BF16),
                pltpu.VMEM((2, rows, xcols), BF16),
                pltpu.VMEM((2, rows, xcols), BF16),
                pltpu.VMEM((4, 2, rows, ny * ycols), BF16),
                pltpu.VMEM((4, 2, rows, ycols), BF16),
                pltpu.VMEM((4, 2, rows, ycols), BF16),
                pltpu.VMEM((4, 2, rows, ycols), BF16),
                pltpu.VMEM((3, 2, rows, ycols), BF16),
                pltpu.VMEM((2, rows, ycols), F32),
                pltpu.VMEM((2, rows, ycols), BF16),
                pltpu.VMEM((2, rows, ycols), BF16),
                pltpu.VMEM((2, rows, ycols), BF16),
                pltpu.VMEM((2, rows, quarter), BF16),
                pltpu.VMEM((2, rows, quarter), BF16),
                pltpu.VMEM((2, rows, d_model), BF16),
                pltpu.VMEM((2, 3, rows, 4 * capacity), BF16),
                pltpu.VMEM((8, 2 * experts, rows), F32),
                pltpu.SemaphoreType.DMA((16,)),
                pltpu.SemaphoreType.DMA((2 * (d_model // min(512, d_model)),)),
                pltpu.SemaphoreType.DMA((256,)),
                pltpu.SemaphoreType.DMA((256,)),
            ],
            compiler_params=pltpu.CompilerParams(collective_id=0, has_side_effects=True, vmem_limit_bytes=67043328),
            name='moe_ring',
        )(normed, resid_in, meta, w_gate, w_up, w_down)
        return out

    return jax.shard_map(device_step, mesh=mesh, in_specs=(row_spec, P(None), P(None, None), P('ep', None, 'tp'), P('ep', None, 'tp'), P('ep', 'tp', None), row_spec), out_specs=row_spec, check_vma=False)
```

```python
import functools

import jax
import jax.numpy as jnp
from jax import lax
from jax.experimental import pallas as pl
from jax.experimental.pallas import tpu as pltpu
from jax.sharding import PartitionSpec as P

NORM_EPS = 1e-5
MESH = pl.DeviceIdType.MESH
BF16 = jnp.bfloat16
F32 = jnp.float32
SUBS = 4
PIECES = 4
LATE_X_SHARE = 2
ORDER = (
    ('ns', 2, 1), ('ns', 1, 0), ('ns', 2, 3), ('ns', 1, 2), ('G', 0), ('A', 2, 1), ('A', 1, 0), ('T', 0), ('A', 1, 2),
    ('ns', 1, 1), ('A', 2, 3), ('ns', 1, 3), ('ns', 2, 2), ('ns', 2, 0), ('U0', 0), ('U1', 0), ('A', 3, 0), ('H', 0),
    ('A', 3, 1), ('A', 3, 2), ('S', 1, 0), ('A', 3, 3), ('D', 0), ('S', 1, 2), ('S', 3, 0), ('S', 3, 1), ('A', 1, 1),
    ('A', 2, 2), ('meta',), ('S', 3, 2), ('S', 3, 3), ('S', 2, 3), ('PF', 3), ('A', 2, 0), ('A', 1, 3), ('G', 3),
    ('YS', 0), ('U0', 3), ('S', 1, 1), ('U1', 3), ('H', 3), ('T', 3), ('S', 1, 3), ('S', 2, 2), ('PF', 1), ('S', 2, 1),
    ('D', 3), ('S', 2, 0), ('YS', 3), ('f1', 3), ('f1', 1), ('G', 1), ('PF', 2), ('U0', 1), ('T', 1), ('f0', 3),
    ('U1', 1), ('H', 1), ('f0', 1), ('G', 2), ('f0', 2), ('f1', 0), ('D', 1), ('m0', 0), ('m0', 3), ('YS', 1),
    ('U0', 2), ('U1', 2), ('H', 2), ('f0', 0), ('m1', 1), ('YM', 3), ('m0', 1), ('T', 2), ('f1', 2), ('D', 2),
    ('YS', 2), ('p1', 0), ('p0', 0), ('YE', 3), ('m1', 3), ('YM', 1), ('p1', 1), ('YM', 2), ('p0', 1), ('YM', 0),
    ('m1', 0), ('p0', 3), ('p1', 3), ('wf',), ('m0', 2), ('O', 1), ('O', 0), ('p1', 2), ('YE', 1), ('wm1',), ('m1', 2),
    ('p0', 2), ('V', 1), ('V', 0), ('O', 3), ('N', 1), ('V', 3), ('YE', 2), ('wm0',), ('YE', 0), ('wp1',), ('N', 0),
    ('R', 1), ('wp0',), ('N', 3), ('O', 2), ('R', 0), ('R', 3), ('V', 2), ('WS',), ('N', 2), ('WR',), ('R', 2),
)


def norm_route(resid_rows, norm_scale, w_router, choice_rows):
    rows_f32 = resid_rows.astype(F32)
    centered = rows_f32 - jnp.mean(rows_f32, axis=-1, keepdims=True)
    variance = jnp.mean(centered * centered, axis=-1, keepdims=True)
    normed = (centered * lax.rsqrt(variance + NORM_EPS) * norm_scale.astype(F32)).astype(BF16)
    logits = jnp.dot(normed, w_router, preferred_element_type=F32)
    router_probs = jax.nn.softmax(logits, axis=-1)
    expert_ids = jnp.arange(w_router.shape[1], dtype=jnp.int32)
    chosen = choice_rows[:, :, None] == expert_ids[None, None, :]
    picked = jnp.sum(jnp.where(chosen, router_probs[:, None, :], 0.0), axis=-1)
    gate_vals = picked / jnp.sum(picked, axis=-1, keepdims=True)
    gate_by_expert = jnp.sum(jnp.where(chosen, gate_vals[:, :, None], 0.0), axis=1)
    return normed, gate_by_expert, jnp.any(chosen, axis=1)


def slot_meta(gate_by_expert, is_chosen, capacity, chips):
    rows = is_chosen.shape[0]
    earlier = jnp.arange(rows)[:, None] > jnp.arange(rows)[None, :]
    position = jnp.dot(earlier.astype(BF16), is_chosen.astype(BF16), preferred_element_type=F32)
    kept = is_chosen & (position < capacity)
    slots = jnp.where(kept, position, -1.0).T.reshape(chips, -1, rows)
    gates = jnp.where(kept, gate_by_expert, 0.0).T.reshape(chips, -1, rows)
    return jnp.concatenate([slots, gates], axis=1)


def moe_kernel(capacity, ny, nx, u_in, resid, meta_in, w_gate, w_up, w_down, out, ug,
               w1, v1, w2, xg, hid, hpart, sums, rfar, rplus, rminus, yown, yfar, yplus, yminus, ycon, vfar, vplus, vminus, wsum, wown, wfar, wplus, wminus, fin, xres, utile, gsplit, meta,
               load_sem, tile_sem, send_sem, recv_sem):
    rows, d_model = resid.shape
    half = d_model // 2
    quarter = half // ny
    width = w_gate.shape[2]
    chunk = rows // (2 * PIECES)
    sub = rows // SUBS
    y = lax.axis_index('tp')
    ep = lax.axis_index('ep')
    core = lax.rem(ep, 2)
    x = ep // 2

    def ep_at(dx, other=False):
        return lax.rem(x + dx + nx, nx) * 2 + ((1 - core) if other else core)

    def dev_x(dx, other=False):
        return {'ep': ep_at(dx, other)}

    def dev_y(dy, other=False):
        return {'tp': lax.rem(y + dy + ny, ny), 'ep': ep_at(0, other)}

    partner = dev_x(0, True)

    barrier = pltpu.get_barrier_semaphore()
    peers = [dev_x(dx, o) for dx in range(nx) for o in (False, True) if (dx, o) != (0, False)]
    peers += [dev_y(dy, o) for dy in (1, -1) for o in (False, True)]
    for peer in peers:
        pl.semaphore_signal(barrier, inc=1, device_id=peer, device_id_type=MESH)
    pl.semaphore_wait(barrier, len(peers))

    copies = []

    def remote(src, dst, device):
        at = len(copies)
        copy = pltpu.make_async_remote_copy(src_ref=src, dst_ref=dst, send_sem=send_sem.at[at], recv_sem=recv_sem.at[at], device_id=device, device_id_type=MESH)
        copies.append(copy)
        copy.start()
        return copy

    sent = []

    def finish_send(copy):
        copy.wait_send()
        sent.append(copy)

    locals_ = []

    def local(src, dst):
        copy = pltpu.make_async_copy(src, dst, load_sem.at[len(locals_)])
        locals_.append(copy)
        copy.start()
        return copy

    my_half = pl.multiple_of(core * half, half)
    other_half = pl.multiple_of((1 - core) * half, half)
    my_quarter = pl.multiple_of(my_half + y * quarter, quarter)
    other_quarter = pl.multiple_of(other_half + y * quarter, quarter)

    parity = lax.rem(y, 2)

    def piece(q, mine=True):
        side = parity if mine else 1 - parity
        return pl.ds(pl.multiple_of(side * (rows // 2) + q * chunk, chunk), chunk)

    def meta_for(dx):
        return meta_in.at[lax.rem(x + dx + nx, nx)]

    ax = {}

    def near_send(slot, q):
        ax[slot, q] = remote(u_in.at[piece(q)], ug.at[slot, 0, piece(q)], dev_x(1 if slot == 1 else -1))

    own_rows = (local(u_in, utile.at[0]), remote(u_in, utile.at[1], partner))
    meta_copies = {(0, 0): local(meta_for(0), meta.at[0]), (0, 1): remote(meta_for(0), meta.at[1], partner)}

    def send_meta():
        for slot, dx in ((1, 1), (2, -1), (3, 2)):
            for lane in range(2):
                meta_copies[slot, lane] = remote(meta_for(dx), meta.at[slot * 2 + lane], dev_x(dx, lane == 1))

    loads = {}
    for e in range(2):
        loads[e] = (local(w_gate.at[e], w1.at[e]), local(w_up.at[e], v1.at[e]))
    w2_copies = [local(w_down.at[e, :, pl.ds(my_half, half)], w2.at[e]) for e in range(2)]
    w2_copies += [remote(w_down.at[e, :, pl.ds(other_half, half)], w2.at[2 + e], partner) for e in range(2)]
    res_copies = [local(resid.at[:, pl.ds(my_quarter, quarter)], xres.at[0]),
                  remote(resid.at[:, pl.ds(other_quarter, quarter)], xres.at[1], partner)]

    ay, pushed = {}, {1: [], 2: [], 3: []}

    def push(slot, q, mine):
        at = piece(q, mine)
        pushed[slot].append(remote(ug.at[slot, 0, at], ug.at[slot, 1, at], partner))

    def y_forward(slot, q):
        up = slot == 1 or (slot == 3 and q % 2 == 0)
        ay[slot, q] = remote(ug.at[slot, 0, piece(q)], ug.at[slot, 0, piece(q)], dev_y(1 if up else -1))

    def on_piece(slot, q):
        ax[slot, q].wait_recv()
        if slot == 2 - (q + 1) % 2:
            ax[3, q] = remote(ug.at[slot, 0, piece(q)], ug.at[3, 0, piece(q)], dev_x(1 if slot == 1 else -1))
        y_forward(slot, q)
        push(slot, q, True)

    def on_side(slot, q):
        ay[slot, q].wait_recv()
        push(slot, q, False)

    def slot_onehot(pos_row):
        return lax.broadcasted_iota(jnp.int32, (capacity, rows), 0).astype(F32) == pos_row

    tile = min(1024, d_model)
    tiles = d_model // tile

    def fetch(slot, t, lane):
        cols = pl.ds(t * tile, tile) if isinstance(t, int) else pl.ds(pl.multiple_of(t * tile, tile), tile)
        return pltpu.make_async_copy(ug.at[slot, lane, :, cols], utile.at[lane, :, cols], tile_sem.at[lane * tiles + t])

    def prefetch(slot):
        for copy in pushed[slot]:
            copy.wait_recv()
        for t in range(tiles):
            for lane in range(2):
                fetch(slot, t, lane).start()

    def meta_rows(slot, lane, e):
        row = 2 * core + e if e < 2 else 2 * (1 - core) + e - 2
        return meta[slot * 2 + lane, pl.ds(row, 1), :], meta[slot * 2 + lane, pl.ds(4 + row, 1), :]

    def gates(slot):
        for lane in range(2):
            parts = []
            for e in range(4):
                pos_row, gate_row = meta_rows(slot, lane, e)
                parts.append(jnp.where(slot_onehot(pos_row), gate_row, 0.0))
            gate_mat = jnp.concatenate(parts, axis=0).T
            for term in range(3):
                part = gate_mat.astype(BF16)
                gsplit[lane, term] = part
                gate_mat = gate_mat - part.astype(F32)

    def gather(slot):
        picks = []
        for lane in range(2):
            copy = meta_copies[slot, lane]
            copy.wait_recv() if copy.is_remote else copy.wait()
            parts = [slot_onehot(meta_rows(slot, lane, e)[0]).astype(F32).astype(BF16) for e in range(2)]
            picks.append(jnp.concatenate(parts, axis=0))
        if slot == 0:
            own_rows[0].wait()
            own_rows[1].wait_recv()

        def body(t, carry):
            cols = pl.ds(pl.multiple_of(t * tile, tile), tile)
            for lane in range(2):
                if slot:
                    fetch(slot, t, lane).wait()
                got = jnp.dot(picks[lane], utile[lane, :, cols], preferred_element_type=F32).astype(BF16)
                for e in range(2):
                    xg[e, lane * capacity:(lane + 1) * capacity, cols] = got[e * capacity:(e + 1) * capacity]
            return carry

        lax.fori_loop(0, tiles, body, 0)

    ftile = min(256, width)

    def gate_up(e, slot):
        if slot == 0:
            for copy in loads[e]:
                copy.wait()

        def body(t, carry):
            cols = pl.ds(pl.multiple_of(t * ftile, ftile), ftile)
            gate_act = jnp.dot(xg[e], w1[e, :, cols], preferred_element_type=F32)
            up_act = jnp.dot(xg[e], v1[e, :, cols], preferred_element_type=F32)
            hid[e, :, cols] = (jax.nn.silu(gate_act) * up_act).astype(BF16)
            return carry

        lax.fori_loop(0, width // ftile, body, 0)

    xcols = yfar.shape[2]
    ycols = quarter - xcols

    shared = {}

    def share_hidden(slot):
        shared[slot] = remote(hid, hpart.at[slot], partner)

    def down(slot):
        if slot == 0:
            for copy in w2_copies:
                copy.wait_recv() if copy.is_remote else copy.wait()
        shared[slot].wait_recv()

        def body(t, carry):
            cols = pl.ds(pl.multiple_of(t * quarter, quarter), quarter)
            outs = []
            for e in range(4):
                lhs = hid[e] if e < 2 else hpart[slot, e - 2]
                outs.append(jnp.dot(lhs, w2[e, :, cols], preferred_element_type=F32).astype(BF16))
            for lane in range(2):
                stack = []
                for e in range(4):
                    at = lane if e < 2 else 1 - lane
                    stack.append(outs[e][at * capacity:(at + 1) * capacity])
                stacked = jnp.concatenate(stack, axis=0)
                total = jnp.dot(gsplit[lane, 0], stacked, preferred_element_type=F32)
                for term in (1, 2):
                    total += jnp.dot(gsplit[lane, term], stacked, preferred_element_type=F32)
                total = total.astype(BF16)
                sums[slot, lane, :, pl.ds(pl.multiple_of(t * xcols, 128), xcols)] = total[:, :xcols]
                ycon[slot, lane, :, pl.ds(pl.multiple_of(t * ycols, 128), ycols)] = total[:, xcols:]
            return carry

        lax.fori_loop(0, ny, body, 0)
        finish_send(shared[slot])

    rs = {}

    def add_into(ref, other):
        ref[...] = (ref[...].astype(F32) + other[...].astype(F32)).astype(BF16)

    def rs_start(tag, src, landing, dev):
        far, plus, minus = landing
        rs[tag] = {'f0': remote(src(2, 0), far.at[0], dev(1)), 'f1': remote(src(2, 1), far.at[1], dev(-1)),
                   'p1': remote(src(1, 1), plus.at[1], dev(1)), 'm0': remote(src(-1, 0), minus.at[0], dev(-1))}

    def rs_mid(tag, src, landing, dev):
        far, plus, minus = landing
        rs[tag]['f0'].wait_recv()
        add_into(src(1, 0), far.at[0])
        rs[tag]['p0'] = remote(src(1, 0), plus.at[0], dev(1))
        rs[tag]['f1'].wait_recv()
        add_into(src(-1, 1), far.at[1])
        rs[tag]['m1'] = remote(src(-1, 1), minus.at[1], dev(-1))

    def rs_end(tag):
        for name in ('m0', 'p1', 'p0', 'm1'):
            rs[tag][name].wait_recv()

    def y_args(slot):
        def src(dy, lane):
            return ycon.at[slot, lane, :, pl.ds(pl.multiple_of(lax.rem(y + dy + ny, ny) * ycols, 128), ycols)]
        return src, (vfar.at[slot], vplus.at[slot], vminus.at[slot]), dev_y

    def y_start(slot):
        rs_start(slot, *y_args(slot))

    def y_mid(slot):
        rs_mid(slot, *y_args(slot))

    def y_end(slot):
        rs_end(slot)
        src = y_args(slot)[0]
        for lane in range(2):
            total = src(0, lane)[...].astype(F32) + vplus[slot, lane].astype(F32) + vminus[slot, lane].astype(F32)
            if slot == 0:
                wown[lane] = total
            else:
                wsum[slot - 1, lane] = total.astype(BF16)

    def w_src(dx, lane):
        return wsum.at[{-1: 0, 1: 1, 2: 2}[dx], lane]

    def w_far():
        rs['w'] = {'f0': remote(w_src(2, 0), wfar.at[0], dev_x(1)), 'f1': remote(w_src(2, 1), wfar.at[1], dev_x(-1))}

    wx = {}

    def w_send(name):
        lane = int(name[1])
        dx = 1 if name[0] == 'p' else -1
        if name in ('p0', 'm1'):
            rs['w']['f%d' % lane].wait_recv()
            add_into(w_src(dx, lane), wfar.at[lane])
        landing = wplus if dx == 1 else wminus
        wx[name] = remote(w_src(dx, lane), landing.at[lane], dev_x(dx))

    def sub_rows(j):
        return pl.ds(j * sub, sub)

    sx = {}

    def send_sum(name, slot, lane, j, landing, dx):
        sx[name, j] = remote(sums.at[slot, lane, sub_rows(j)], landing.at[lane, sub_rows(j)], dev_x(dx))

    def x_send(name, j):
        lane = int(name[1])
        if name[0] == 'f':
            send_sum(name, 3, lane, j, rfar, 1 if lane == 0 else -1)
            return
        slot, landing, dx = (2, rplus, 1) if name[0] == 'p' else (1, rminus, -1)
        if name in ('p0', 'm1'):
            sx['f%d' % lane, j].wait_recv()
            add_into(sums.at[slot, lane, sub_rows(j)], rfar.at[lane, sub_rows(j)])
        send_sum(name, slot, lane, j, landing, dx)

    def q_cols(dy):
        return pl.ds(pl.multiple_of(lax.rem(y + dy + ny, ny) * xcols, 128), xcols)

    def send_y(name, lane, j, dcol, landing, dy):
        sx[name, j] = remote(sums.at[0, lane, sub_rows(j), q_cols(dcol)], landing.at[lane, sub_rows(j)], dev_y(dy))

    def stage_own(j):
        for name in ('m0', 'p1', 'p0', 'm1'):
            sx[name, j].wait_recv()
        at = sub_rows(j)
        for lane in range(2):
            cols = q_cols(0)
            yown[lane, at, :] = sums[0, lane, at, cols].astype(F32) + rplus[lane, at, cols].astype(F32) + rminus[lane, at, cols].astype(F32)
        for lane in range(2):
            sums[0, lane, at, :] = (sums[0, lane, at, :].astype(F32) + rplus[lane, at, :].astype(F32) + rminus[lane, at, :].astype(F32)).astype(BF16)
        send_y('yf0', 0, j, 2, yfar, 1)
        send_y('yf1', 1, j, 2, yfar, -1)
        send_y('yp1', 1, j, 1, yplus, 1)
        send_y('ym0', 0, j, -1, yminus, -1)

    def stage_yfar(j):
        sx['yf0', j].wait_recv()
        sx['yf1', j].wait_recv()
        at = sub_rows(j)
        cols = q_cols(1)
        sums[0, 0, at, cols] = (sums[0, 0, at, cols].astype(F32) + yfar[0, at, :].astype(F32)).astype(BF16)
        send_y('yp0', 0, j, 1, yplus, 1)
        cols = q_cols(-1)
        sums[0, 1, at, cols] = (sums[0, 1, at, cols].astype(F32) + yfar[1, at, :].astype(F32)).astype(BF16)
        send_y('ym1', 1, j, -1, yminus, -1)

    done = {}
    pending = [res_copies]

    def residual_ready():
        for copy in pending.pop() if pending else ():
            copy.wait_recv() if copy.is_remote else copy.wait()

    def share_rows(key, at, first, cols):
        def place(start):
            return out.at[at, pl.ds(pl.multiple_of(start + first, 128), cols)]

        src = fin.at[:, at, pl.ds(first, cols)]
        for lane in range(2):
            done['up', lane, key] = remote(src.at[lane], place(my_quarter), dev_y(1, lane == 1))
            done['down', lane, key] = remote(src.at[lane], place(my_quarter), dev_y(-1, lane == 1))
        done['own', key] = local(src.at[0], place(my_quarter))
        done['pair', key] = remote(src.at[1], place(my_quarter), partner)

    def relay_rows(key, at, first, cols):
        def place(start):
            return out.at[at, pl.ds(pl.multiple_of(start + first, 128), cols)]

        done['up', 0, key].wait_recv()
        start = my_half + lax.rem(y - 1 + ny, ny) * quarter
        done['up2', key] = remote(place(start), place(start), dev_y(1))
        done['down', 1, key].wait_recv()
        start = other_half + lax.rem(y + 1, ny) * quarter
        done['down2', key] = remote(place(start), place(start), dev_y(-1))

    def stage_final(j):
        for name in ('ym0', 'yp1', 'yp0', 'ym1'):
            sx[name, j].wait_recv()
        residual_ready()
        at = sub_rows(j)
        for lane in range(2):
            total = yown[lane, at, :] + yplus[lane, at, :].astype(F32) + yminus[lane, at, :].astype(F32)
            fin[lane, at, :xcols] = (xres[lane, at, :xcols].astype(F32) + total).astype(BF16)
        share_rows(j, at, 0, xcols)

    def stage_relay(j):
        relay_rows(j, sub_rows(j), 0, xcols)

    def w_share():
        for name in ('m0', 'p1', 'p0', 'm1'):
            wx[name].wait_recv()
        residual_ready()
        for lane in range(2):
            total = wown[lane] + wplus[lane].astype(F32) + wminus[lane].astype(F32)
            fin[lane, :, xcols:] = (xres[lane, :, xcols:].astype(F32) + total).astype(BF16)
        share_rows('w', pl.ds(0, rows), xcols, ycols)

    def w_relay():
        relay_rows('w', pl.ds(0, rows), xcols, ycols)

    actions = {'ns': near_send, 'meta': send_meta, 'A': on_piece, 'S': on_side, 'PF': prefetch, 'G': gather,
               'U0': functools.partial(gate_up, 0), 'U1': functools.partial(gate_up, 1), 'H': share_hidden, 'T': gates, 'D': down,
               'YS': y_start, 'YM': y_mid, 'YE': y_end, 'wf': w_far, 'WS': w_share, 'WR': w_relay,
               'O': stage_own, 'V': stage_yfar, 'N': stage_final, 'R': stage_relay}
    for name in ('f0', 'f1', 'm0', 'm1', 'p0', 'p1'):
        actions[name] = functools.partial(x_send, name)
        actions['w' + name] = functools.partial(w_send, name)
    for name, *args in ORDER:
        actions[name](*args)
    for key in (*range(SUBS), 'w'):
        done['up', 1, key].wait_recv()
        done['down', 0, key].wait_recv()
        done['pair', key].wait_recv()
        done['up2', key].wait_recv()
        done['down2', key].wait_recv()
        done['own', key].wait()
    for copy in copies:
        if not any(copy is other for other in sent):
            copy.wait_send()


def solution(mesh):
    row_spec = P(('dp', 'ep'), None)
    ny, nx = mesh.shape['tp'], mesh.shape['ep'] // 2

    def device_step(resid_in, norm_scale, w_router, w_gate, w_up, w_down, choice):
        rows, d_model = resid_in.shape
        experts = w_router.shape[1]
        width = w_gate.shape[2]
        capacity = (2 * rows * choice.shape[1] + experts - 1) // experts
        normed, gate_by_expert, is_chosen = norm_route(resid_in, norm_scale, w_router, choice)
        meta = slot_meta(gate_by_expert, is_chosen, capacity, nx)
        half, slots = d_model // 2, 2 * capacity
        quarter = half // ny
        ycols = quarter // LATE_X_SHARE
        xcols = quarter - ycols

        hbm = pl.BlockSpec(memory_space=pl.ANY)
        out, _ = pl.pallas_call(
            functools.partial(moe_kernel, capacity, ny, nx),
            out_shape=(jax.ShapeDtypeStruct((rows, d_model), BF16), jax.ShapeDtypeStruct((4, 2, rows, d_model), BF16)),
            in_specs=[hbm] * 6,
            out_specs=(hbm, hbm),
            scratch_shapes=[
                pltpu.VMEM((2, d_model, width), BF16),
                pltpu.VMEM((2, d_model, width), BF16),
                pltpu.VMEM((4, width, half), BF16),
                pltpu.VMEM((2, slots, d_model), BF16),
                pltpu.VMEM((2, slots, width), BF16),
                pltpu.VMEM((4, 2, slots, width), BF16),
                pltpu.VMEM((4, 2, rows, ny * xcols), BF16),
                pltpu.VMEM((2, rows, ny * xcols), BF16),
                pltpu.VMEM((2, rows, ny * xcols), BF16),
                pltpu.VMEM((2, rows, ny * xcols), BF16),
                pltpu.VMEM((2, rows, xcols), F32),
                pltpu.VMEM((2, rows, xcols), BF16),
                pltpu.VMEM((2, rows, xcols), BF16),
                pltpu.VMEM((2, rows, xcols), BF16),
                pltpu.VMEM((4, 2, rows, ny * ycols), BF16),
                pltpu.VMEM((4, 2, rows, ycols), BF16),
                pltpu.VMEM((4, 2, rows, ycols), BF16),
                pltpu.VMEM((4, 2, rows, ycols), BF16),
                pltpu.VMEM((3, 2, rows, ycols), BF16),
                pltpu.VMEM((2, rows, ycols), F32),
                pltpu.VMEM((2, rows, ycols), BF16),
                pltpu.VMEM((2, rows, ycols), BF16),
                pltpu.VMEM((2, rows, ycols), BF16),
                pltpu.VMEM((2, rows, quarter), BF16),
                pltpu.VMEM((2, rows, quarter), BF16),
                pltpu.VMEM((2, rows, d_model), BF16),
                pltpu.VMEM((2, 3, rows, 4 * capacity), BF16),
                pltpu.VMEM((2 * nx, meta.shape[1], rows), F32),
                pltpu.SemaphoreType.DMA((16,)),
                pltpu.SemaphoreType.DMA((2 * (d_model // min(1024, d_model)),)),
                pltpu.SemaphoreType.DMA((256,)),
                pltpu.SemaphoreType.DMA((256,)),
            ],
            compiler_params=pltpu.CompilerParams(collective_id=0, has_side_effects=True, vmem_limit_bytes=67043328),
            name='moe_ring',
        )(normed, resid_in, meta, w_gate, w_up, w_down)
        return out

    return jax.shard_map(device_step, mesh=mesh, in_specs=(row_spec, P(None), P(None, None), P('ep', None, 'tp'), P('ep', None, 'tp'), P('ep', 'tp', None), row_spec), out_specs=row_spec, check_vma=False)
```

```python
import functools

import jax
import jax.numpy as jnp
from jax import lax
from jax.experimental import pallas as pl
from jax.experimental.pallas import tpu as pltpu
from jax.sharding import PartitionSpec as P

NORM_EPS = 1e-5
MESH = pl.DeviceIdType.MESH
BF16 = jnp.bfloat16
F32 = jnp.float32
SUBS = 4
PIECES = 4
LATE_X_SHARE = 2
ORDER = (
    ('ns', 1, 0), ('ns', 1, 2), ('ns', 2, 3), ('E2',), ('ns', 2, 1), ('G', 0), ('T', 0), ('A', 2, 3), ('A', 1, 0),
    ('U0', 0), ('A', 1, 2), ('A', 2, 1), ('ns', 2, 2), ('U1', 0), ('H', 0), ('S', 1, 0), ('A', 3, 3), ('ns', 1, 1),
    ('A', 3, 0), ('A', 3, 1), ('A', 3, 2), ('ns', 1, 3), ('D', 0), ('ns', 2, 0), ('S', 3, 3), ('A', 2, 2), ('S', 3, 0),
    ('A', 1, 1), ('S', 3, 2), ('S', 3, 1), ('PF', 3), ('meta',), ('A', 2, 0), ('A', 1, 3), ('YS', 0), ('S', 2, 1),
    ('G', 3), ('U0', 3), ('S', 1, 2), ('S', 1, 1), ('U1', 3), ('H', 3), ('T', 3), ('S', 1, 3), ('PF', 1), ('S', 2, 2),
    ('S', 2, 0), ('D', 3), ('f1', 2), ('YS', 3), ('f0', 2), ('S', 2, 3), ('f0', 3), ('f1', 1), ('G', 1), ('U0', 1),
    ('PF', 2), ('T', 1), ('U1', 1), ('H', 1), ('YM', 3), ('f0', 1), ('f1', 0), ('f1', 3), ('G', 2), ('D', 1), ('YS', 1),
    ('m0', 0), ('f0', 0), ('U0', 2), ('U1', 2), ('H', 2), ('YM', 0), ('T', 2), ('YE', 3), ('m0', 1), ('wf',), ('D', 2),
    ('p1', 0), ('m1', 0), ('YS', 2), ('p0', 0), ('p1', 1), ('m1', 2), ('p0', 1), ('YM', 2), ('O', 0), ('m1', 1),
    ('p1', 2), ('p0', 2), ('YM', 1), ('m0', 2), ('m1', 3), ('V', 0), ('O', 1), ('p0', 3), ('N', 0), ('YE', 2), ('V', 1),
    ('YE', 1), ('p1', 3), ('O', 2), ('wp0',), ('m0', 3), ('wp1',), ('N', 1), ('wm0',), ('R', 0), ('wm1',), ('V', 2),
    ('O', 3), ('R', 1), ('N', 2), ('V', 3), ('YE', 0), ('WS',), ('R', 2), ('N', 3), ('WR',), ('R', 3),
)


def route(normed, router_t, choice_t, capacity):
    logits = lax.dot_general(router_t, normed, (((1,), (1,)), ((), ())), preferred_element_type=F32)
    weights = jnp.exp(logits - jnp.max(logits, axis=0, keepdims=True))
    probs = weights / jnp.sum(weights, axis=0, keepdims=True)
    expert_ids = lax.broadcasted_iota(jnp.int32, logits.shape, 0)
    chosen = [expert_ids == choice_t[k:k + 1] for k in range(2)]
    picked = [jnp.sum(jnp.where(hit, probs, 0.0), axis=0, keepdims=True) for hit in chosen]
    total = picked[0] + picked[1]
    gate = jnp.where(chosen[0], picked[0] / total, jnp.where(chosen[1], picked[1] / total, 0.0))
    any_chosen = jnp.where(chosen[0], 1.0, jnp.where(chosen[1], 1.0, 0.0))
    rows = normed.shape[0]
    earlier = lax.broadcasted_iota(jnp.int32, (rows, rows), 0) < lax.broadcasted_iota(jnp.int32, (rows, rows), 1)
    earlier = jnp.where(earlier, 1.0, 0.0).astype(BF16)
    position = jnp.dot(any_chosen.astype(BF16), earlier, preferred_element_type=F32)
    kept = (any_chosen > 0.0) & (position < capacity)
    return jnp.where(kept, position, -1.0), jnp.where(kept, gate, 0.0)


def moe_kernel(capacity, ny, nx, resid, scale, router_t, choice_t, w_gate, w_up, w_down, out, ug,
               w1, v1, w2, xg, hid, hpart, sums, rfar, rplus, rminus, yown, yfar, yplus, yminus, ycon, vfar, vplus, vminus, wsum, wown, wfar, wplus, wminus, fin, xres, utile, gsplit, meta, meta_src,
               load_sem, tile_sem, send_sem, recv_sem):
    rows, d_model = resid.shape
    half = d_model // 2
    quarter = half // ny
    width = w_gate.shape[2]
    chunk = rows // (2 * PIECES)
    sub = rows // SUBS
    y = lax.axis_index('tp')
    ep = lax.axis_index('ep')
    core = lax.rem(ep, 2)
    x = ep // 2

    def ep_at(dx, other=False):
        return lax.rem(x + dx + nx, nx) * 2 + ((1 - core) if other else core)

    def dev_x(dx, other=False):
        return {'ep': ep_at(dx, other)}

    def dev_y(dy, other=False):
        return {'tp': lax.rem(y + dy + ny, ny), 'ep': ep_at(0, other)}

    partner = dev_x(0, True)

    first_load = pltpu.make_async_copy(resid, utile.at[0], load_sem.at[15])
    first_load.start()
    barrier = pltpu.get_barrier_semaphore()
    peers = [dev_x(dx, o) for dx in range(nx) for o in (False, True) if (dx, o) != (0, False)]
    peers += [dev_y(dy, o) for dy in (1, -1) for o in (False, True)]
    for peer in peers:
        pl.semaphore_signal(barrier, inc=1, device_id=peer, device_id_type=MESH)
    pl.semaphore_wait(barrier, len(peers))

    copies = []

    def remote(src, dst, device):
        at = len(copies)
        copy = pltpu.make_async_remote_copy(src_ref=src, dst_ref=dst, send_sem=send_sem.at[at], recv_sem=recv_sem.at[at], device_id=device, device_id_type=MESH)
        copies.append(copy)
        copy.start()
        return copy

    sent = []

    def finish_send(copy):
        copy.wait_send()
        sent.append(copy)

    locals_ = []

    def local(src, dst):
        copy = pltpu.make_async_copy(src, dst, load_sem.at[len(locals_)])
        locals_.append(copy)
        copy.start()
        return copy

    my_half = pl.multiple_of(core * half, half)
    other_half = pl.multiple_of((1 - core) * half, half)
    my_quarter = pl.multiple_of(my_half + y * quarter, quarter)
    other_quarter = pl.multiple_of(other_half + y * quarter, quarter)

    parity = lax.rem(y, 2)

    def piece(q, mine=True):
        side = parity if mine else 1 - parity
        return pl.ds(pl.multiple_of(side * (rows // 2) + q * chunk, chunk), chunk)

    loads = {}
    for e in range(2):
        loads[e] = (local(w_gate.at[e], w1.at[e]), local(w_up.at[e], v1.at[e]))
    first_load.wait()

    def normalize(i, carry):
        at = pl.ds(pl.multiple_of(i * 16, 16), 16)
        values = utile[0, at, :].astype(F32)
        centered = values - jnp.mean(values, axis=-1, keepdims=True)
        variance = jnp.mean(centered * centered, axis=-1, keepdims=True)
        utile[0, at, :] = (centered * lax.rsqrt(variance + NORM_EPS) * scale[...].astype(F32)).astype(BF16)
        return carry

    lax.fori_loop(0, rows // 16, normalize, 0)

    def meta_for(dx):
        return meta_src.at[lax.rem(x + dx + nx, nx)]

    ax = {}

    def near_send(slot, q):
        ax[slot, q] = remote(utile.at[0, piece(q)], ug.at[slot, 0, piece(q)], dev_x(1 if slot == 1 else -1))

    meta_copies, entry = {}, {}

    def own_routes():
        entry['own'] = remote(utile.at[0], utile.at[1], partner)
        positions, gate_rows = route(utile[0], router_t[...], choice_t[...], capacity)
        per_chip = positions.shape[0] // nx
        for k in range(nx):
            meta_src[k, :per_chip] = positions[k * per_chip:(k + 1) * per_chip]
            meta_src[k, per_chip:] = gate_rows[k * per_chip:(k + 1) * per_chip]
        meta[0] = meta_src[x]
        meta_copies[0, 1] = remote(meta_for(0), meta.at[1], partner)

    def send_meta():
        for slot, dx in ((1, 1), (2, -1), (3, 2)):
            for lane in range(2):
                meta_copies[slot, lane] = remote(meta_for(dx), meta.at[slot * 2 + lane], dev_x(dx, lane == 1))

    w2_copies = [local(w_down.at[e, :, pl.ds(my_half, half)], w2.at[e]) for e in range(2)]
    w2_copies += [remote(w_down.at[e, :, pl.ds(other_half, half)], w2.at[2 + e], partner) for e in range(2)]
    res_copies = [local(resid.at[:, pl.ds(my_quarter, quarter)], xres.at[0]),
                  remote(resid.at[:, pl.ds(other_quarter, quarter)], xres.at[1], partner)]

    ay, pushed = {}, {1: [], 2: [], 3: []}

    def push(slot, q, mine):
        at = piece(q, mine)
        pushed[slot].append(remote(ug.at[slot, 0, at], ug.at[slot, 1, at], partner))

    def y_forward(slot, q):
        up = slot == 1 or (slot == 3 and q % 2 == 0)
        ay[slot, q] = remote(ug.at[slot, 0, piece(q)], ug.at[slot, 0, piece(q)], dev_y(1 if up else -1))

    def on_piece(slot, q):
        ax[slot, q].wait_recv()
        if slot == 2 - (q + 1) % 2:
            ax[3, q] = remote(ug.at[slot, 0, piece(q)], ug.at[3, 0, piece(q)], dev_x(1 if slot == 1 else -1))
        y_forward(slot, q)
        push(slot, q, True)

    def on_side(slot, q):
        ay[slot, q].wait_recv()
        push(slot, q, False)

    def slot_onehot(pos_row):
        return lax.broadcasted_iota(jnp.int32, (capacity, rows), 0).astype(F32) == pos_row

    tile = min(1024, d_model)
    tiles = d_model // tile

    def fetch(slot, t, lane):
        cols = pl.ds(t * tile, tile) if isinstance(t, int) else pl.ds(pl.multiple_of(t * tile, tile), tile)
        return pltpu.make_async_copy(ug.at[slot, lane, :, cols], utile.at[lane, :, cols], tile_sem.at[lane * tiles + t])

    def prefetch(slot):
        if 'own' in entry:
            finish_send(entry.pop('own'))
            for q in range(PIECES):
                finish_send(ax[1, q])
                finish_send(ax[2, q])
        for copy in pushed[slot]:
            copy.wait_recv()
        for t in range(tiles):
            for lane in range(2):
                fetch(slot, t, lane).start()

    def meta_rows(slot, lane, e):
        row = 2 * core + e if e < 2 else 2 * (1 - core) + e - 2
        return meta[slot * 2 + lane, pl.ds(row, 1), :], meta[slot * 2 + lane, pl.ds(4 + row, 1), :]

    def gates(slot):
        for lane in range(2):
            parts = []
            for e in range(4):
                pos_row, gate_row = meta_rows(slot, lane, e)
                parts.append(jnp.where(slot_onehot(pos_row), gate_row, 0.0))
            gate_mat = jnp.concatenate(parts, axis=0).T
            for term in range(3):
                part = gate_mat.astype(BF16)
                gsplit[lane, term] = part
                gate_mat = gate_mat - part.astype(F32)

    def gather(slot):
        picks = []
        for lane in range(2):
            if (slot, lane) != (0, 0):
                meta_copies[slot, lane].wait_recv()
            parts = [slot_onehot(meta_rows(slot, lane, e)[0]).astype(F32).astype(BF16) for e in range(2)]
            picks.append(jnp.concatenate(parts, axis=0))
        if slot == 0:
            entry['own'].wait_recv()

        def body(t, carry):
            cols = pl.ds(pl.multiple_of(t * tile, tile), tile)
            for lane in range(2):
                if slot:
                    fetch(slot, t, lane).wait()
                got = jnp.dot(picks[lane], utile[lane, :, cols], preferred_element_type=F32).astype(BF16)
                for e in range(2):
                    xg[e, lane * capacity:(lane + 1) * capacity, cols] = got[e * capacity:(e + 1) * capacity]
            return carry

        lax.fori_loop(0, tiles, body, 0)

    ftile = min(256, width)

    def gate_up(e, slot):
        if slot == 0:
            for copy in loads[e]:
                copy.wait()

        def body(t, carry):
            cols = pl.ds(pl.multiple_of(t * ftile, ftile), ftile)
            gate_act = jnp.dot(xg[e], w1[e, :, cols], preferred_element_type=F32)
            up_act = jnp.dot(xg[e], v1[e, :, cols], preferred_element_type=F32)
            hid[e, :, cols] = (jax.nn.silu(gate_act) * up_act).astype(BF16)
            return carry

        lax.fori_loop(0, width // ftile, body, 0)

    xcols = yfar.shape[2]
    ycols = quarter - xcols

    shared = {}

    def share_hidden(slot):
        shared[slot] = remote(hid, hpart.at[slot], partner)

    def down(slot):
        if slot == 0:
            for copy in w2_copies:
                copy.wait_recv() if copy.is_remote else copy.wait()
        shared[slot].wait_recv()

        def body(t, carry):
            cols = pl.ds(pl.multiple_of(t * quarter, quarter), quarter)
            outs = []
            for e in range(4):
                lhs = hid[e] if e < 2 else hpart[slot, e - 2]
                outs.append(jnp.dot(lhs, w2[e, :, cols], preferred_element_type=F32).astype(BF16))
            for lane in range(2):
                stack = []
                for e in range(4):
                    at = lane if e < 2 else 1 - lane
                    stack.append(outs[e][at * capacity:(at + 1) * capacity])
                stacked = jnp.concatenate(stack, axis=0)
                total = jnp.dot(gsplit[lane, 0], stacked, preferred_element_type=F32)
                for term in (1, 2):
                    total += jnp.dot(gsplit[lane, term], stacked, preferred_element_type=F32)
                total = total.astype(BF16)
                sums[slot, lane, :, pl.ds(pl.multiple_of(t * xcols, 128), xcols)] = total[:, :xcols]
                ycon[slot, lane, :, pl.ds(pl.multiple_of(t * ycols, 128), ycols)] = total[:, xcols:]
            return carry

        lax.fori_loop(0, ny, body, 0)
        finish_send(shared[slot])

    rs = {}

    def add_into(ref, other):
        ref[...] = (ref[...].astype(F32) + other[...].astype(F32)).astype(BF16)

    def rs_start(tag, src, landing, dev):
        far, plus, minus = landing
        rs[tag] = {'f0': remote(src(2, 0), far.at[0], dev(1)), 'f1': remote(src(2, 1), far.at[1], dev(-1)),
                   'p1': remote(src(1, 1), plus.at[1], dev(1)), 'm0': remote(src(-1, 0), minus.at[0], dev(-1))}

    def rs_mid(tag, src, landing, dev):
        far, plus, minus = landing
        rs[tag]['f0'].wait_recv()
        add_into(src(1, 0), far.at[0])
        rs[tag]['p0'] = remote(src(1, 0), plus.at[0], dev(1))
        rs[tag]['f1'].wait_recv()
        add_into(src(-1, 1), far.at[1])
        rs[tag]['m1'] = remote(src(-1, 1), minus.at[1], dev(-1))

    def rs_end(tag):
        for name in ('m0', 'p1', 'p0', 'm1'):
            rs[tag][name].wait_recv()

    def y_args(slot):
        def src(dy, lane):
            return ycon.at[slot, lane, :, pl.ds(pl.multiple_of(lax.rem(y + dy + ny, ny) * ycols, 128), ycols)]
        return src, (vfar.at[slot], vplus.at[slot], vminus.at[slot]), dev_y

    def y_start(slot):
        rs_start(slot, *y_args(slot))

    def y_mid(slot):
        rs_mid(slot, *y_args(slot))

    def y_end(slot):
        rs_end(slot)
        src = y_args(slot)[0]
        for lane in range(2):
            total = src(0, lane)[...].astype(F32) + vplus[slot, lane].astype(F32) + vminus[slot, lane].astype(F32)
            if slot == 0:
                wown[lane] = total
            else:
                wsum[slot - 1, lane] = total.astype(BF16)

    def w_src(dx, lane):
        return wsum.at[{-1: 0, 1: 1, 2: 2}[dx], lane]

    def w_far():
        rs['w'] = {'f0': remote(w_src(2, 0), wfar.at[0], dev_x(1)), 'f1': remote(w_src(2, 1), wfar.at[1], dev_x(-1))}

    wx = {}

    def w_send(name):
        lane = int(name[1])
        dx = 1 if name[0] == 'p' else -1
        if name in ('p0', 'm1'):
            rs['w']['f%d' % lane].wait_recv()
            add_into(w_src(dx, lane), wfar.at[lane])
        landing = wplus if dx == 1 else wminus
        wx[name] = remote(w_src(dx, lane), landing.at[lane], dev_x(dx))

    def sub_rows(j):
        return pl.ds(j * sub, sub)

    sx = {}

    def send_sum(name, slot, lane, j, landing, dx):
        sx[name, j] = remote(sums.at[slot, lane, sub_rows(j)], landing.at[lane, sub_rows(j)], dev_x(dx))

    def x_send(name, j):
        lane = int(name[1])
        if name[0] == 'f':
            send_sum(name, 3, lane, j, rfar, 1 if lane == 0 else -1)
            return
        slot, landing, dx = (2, rplus, 1) if name[0] == 'p' else (1, rminus, -1)
        if name in ('p0', 'm1'):
            sx['f%d' % lane, j].wait_recv()
            add_into(sums.at[slot, lane, sub_rows(j)], rfar.at[lane, sub_rows(j)])
        send_sum(name, slot, lane, j, landing, dx)

    def q_cols(dy):
        return pl.ds(pl.multiple_of(lax.rem(y + dy + ny, ny) * xcols, 128), xcols)

    def send_y(name, lane, j, dcol, landing, dy):
        sx[name, j] = remote(sums.at[0, lane, sub_rows(j), q_cols(dcol)], landing.at[lane, sub_rows(j)], dev_y(dy))

    def stage_own(j):
        for name in ('m0', 'p1', 'p0', 'm1'):
            sx[name, j].wait_recv()
        at = sub_rows(j)
        for lane in range(2):
            cols = q_cols(0)
            yown[lane, at, :] = sums[0, lane, at, cols].astype(F32) + rplus[lane, at, cols].astype(F32) + rminus[lane, at, cols].astype(F32)
        for lane in range(2):
            sums[0, lane, at, :] = (sums[0, lane, at, :].astype(F32) + rplus[lane, at, :].astype(F32) + rminus[lane, at, :].astype(F32)).astype(BF16)
        send_y('yf0', 0, j, 2, yfar, 1)
        send_y('yf1', 1, j, 2, yfar, -1)
        send_y('yp1', 1, j, 1, yplus, 1)
        send_y('ym0', 0, j, -1, yminus, -1)

    def stage_yfar(j):
        sx['yf0', j].wait_recv()
        sx['yf1', j].wait_recv()
        at = sub_rows(j)
        cols = q_cols(1)
        sums[0, 0, at, cols] = (sums[0, 0, at, cols].astype(F32) + yfar[0, at, :].astype(F32)).astype(BF16)
        send_y('yp0', 0, j, 1, yplus, 1)
        cols = q_cols(-1)
        sums[0, 1, at, cols] = (sums[0, 1, at, cols].astype(F32) + yfar[1, at, :].astype(F32)).astype(BF16)
        send_y('ym1', 1, j, -1, yminus, -1)

    done = {}
    pending = [res_copies]

    def residual_ready():
        for copy in pending.pop() if pending else ():
            copy.wait_recv() if copy.is_remote else copy.wait()

    def share_rows(key, at, first, cols):
        def place(start):
            return out.at[at, pl.ds(pl.multiple_of(start + first, 128), cols)]

        src = fin.at[:, at, pl.ds(first, cols)]
        for lane in range(2):
            done['up', lane, key] = remote(src.at[lane], place(my_quarter), dev_y(1, lane == 1))
            done['down', lane, key] = remote(src.at[lane], place(my_quarter), dev_y(-1, lane == 1))
        done['own', key] = local(src.at[0], place(my_quarter))
        done['pair', key] = remote(src.at[1], place(my_quarter), partner)

    def relay_rows(key, at, first, cols):
        def place(start):
            return out.at[at, pl.ds(pl.multiple_of(start + first, 128), cols)]

        done['up', 0, key].wait_recv()
        start = my_half + lax.rem(y - 1 + ny, ny) * quarter
        done['up2', key] = remote(place(start), place(start), dev_y(1))
        done['down', 1, key].wait_recv()
        start = other_half + lax.rem(y + 1, ny) * quarter
        done['down2', key] = remote(place(start), place(start), dev_y(-1))

    def stage_final(j):
        for name in ('ym0', 'yp1', 'yp0', 'ym1'):
            sx[name, j].wait_recv()
        residual_ready()
        at = sub_rows(j)
        for lane in range(2):
            total = yown[lane, at, :] + yplus[lane, at, :].astype(F32) + yminus[lane, at, :].astype(F32)
            fin[lane, at, :xcols] = (xres[lane, at, :xcols].astype(F32) + total).astype(BF16)
        share_rows(j, at, 0, xcols)

    def stage_relay(j):
        relay_rows(j, sub_rows(j), 0, xcols)

    def w_share():
        for name in ('m0', 'p1', 'p0', 'm1'):
            wx[name].wait_recv()
        residual_ready()
        for lane in range(2):
            total = wown[lane] + wplus[lane].astype(F32) + wminus[lane].astype(F32)
            fin[lane, :, xcols:] = (xres[lane, :, xcols:].astype(F32) + total).astype(BF16)
        share_rows('w', pl.ds(0, rows), xcols, ycols)

    def w_relay():
        relay_rows('w', pl.ds(0, rows), xcols, ycols)

    actions = {'E2': own_routes, 'ns': near_send, 'meta': send_meta, 'A': on_piece, 'S': on_side, 'PF': prefetch, 'G': gather,
               'U0': functools.partial(gate_up, 0), 'U1': functools.partial(gate_up, 1), 'H': share_hidden, 'T': gates, 'D': down,
               'YS': y_start, 'YM': y_mid, 'YE': y_end, 'wf': w_far, 'WS': w_share, 'WR': w_relay,
               'O': stage_own, 'V': stage_yfar, 'N': stage_final, 'R': stage_relay}
    for name in ('f0', 'f1', 'm0', 'm1', 'p0', 'p1'):
        actions[name] = functools.partial(x_send, name)
        actions['w' + name] = functools.partial(w_send, name)
    for name, *args in ORDER:
        actions[name](*args)
    for key in (*range(SUBS), 'w'):
        done['up', 1, key].wait_recv()
        done['down', 0, key].wait_recv()
        done['pair', key].wait_recv()
        done['up2', key].wait_recv()
        done['down2', key].wait_recv()
        done['own', key].wait()
    for copy in copies:
        if not any(copy is other for other in sent):
            copy.wait_send()


def solution(mesh):
    row_spec = P(('dp', 'ep'), None)
    ny, nx = mesh.shape['tp'], mesh.shape['ep'] // 2

    def device_step(resid_in, norm_scale, w_router, w_gate, w_up, w_down, choice):
        rows, d_model = resid_in.shape
        experts = w_router.shape[1]
        width = w_gate.shape[2]
        capacity = (2 * rows * choice.shape[1] + experts - 1) // experts
        half, slots = d_model // 2, 2 * capacity
        quarter = half // ny
        ycols = quarter // LATE_X_SHARE
        xcols = quarter - ycols

        hbm, vmem = pl.BlockSpec(memory_space=pl.ANY), pl.BlockSpec(memory_space=pltpu.VMEM)
        out, _ = pl.pallas_call(
            functools.partial(moe_kernel, capacity, ny, nx),
            out_shape=(jax.ShapeDtypeStruct((rows, d_model), BF16), jax.ShapeDtypeStruct((4, 2, rows, d_model), BF16)),
            in_specs=[hbm, vmem, vmem, vmem, hbm, hbm, hbm],
            out_specs=(hbm, hbm),
            scratch_shapes=[
                pltpu.VMEM((2, d_model, width), BF16),
                pltpu.VMEM((2, d_model, width), BF16),
                pltpu.VMEM((4, width, half), BF16),
                pltpu.VMEM((2, slots, d_model), BF16),
                pltpu.VMEM((2, slots, width), BF16),
                pltpu.VMEM((4, 2, slots, width), BF16),
                pltpu.VMEM((4, 2, rows, ny * xcols), BF16),
                pltpu.VMEM((2, rows, ny * xcols), BF16),
                pltpu.VMEM((2, rows, ny * xcols), BF16),
                pltpu.VMEM((2, rows, ny * xcols), BF16),
                pltpu.VMEM((2, rows, xcols), F32),
                pltpu.VMEM((2, rows, xcols), BF16),
                pltpu.VMEM((2, rows, xcols), BF16),
                pltpu.VMEM((2, rows, xcols), BF16),
                pltpu.VMEM((4, 2, rows, ny * ycols), BF16),
                pltpu.VMEM((4, 2, rows, ycols), BF16),
                pltpu.VMEM((4, 2, rows, ycols), BF16),
                pltpu.VMEM((4, 2, rows, ycols), BF16),
                pltpu.VMEM((3, 2, rows, ycols), BF16),
                pltpu.VMEM((2, rows, ycols), F32),
                pltpu.VMEM((2, rows, ycols), BF16),
                pltpu.VMEM((2, rows, ycols), BF16),
                pltpu.VMEM((2, rows, ycols), BF16),
                pltpu.VMEM((2, rows, quarter), BF16),
                pltpu.VMEM((2, rows, quarter), BF16),
                pltpu.VMEM((2, rows, d_model), BF16),
                pltpu.VMEM((2, 3, rows, 4 * capacity), BF16),
                pltpu.VMEM((2 * nx, 2 * experts // nx, rows), F32),
                pltpu.VMEM((nx, 2 * experts // nx, rows), F32),
                pltpu.SemaphoreType.DMA((16,)),
                pltpu.SemaphoreType.DMA((2 * (d_model // min(1024, d_model)),)),
                pltpu.SemaphoreType.DMA((256,)),
                pltpu.SemaphoreType.DMA((256,)),
            ],
            compiler_params=pltpu.CompilerParams(collective_id=0, has_side_effects=True, vmem_limit_bytes=67043328),
            name='moe_ring',
        )(resid_in, norm_scale[None, :], w_router.T, choice.T, w_gate, w_up, w_down)
        return out

    return jax.shard_map(device_step, mesh=mesh, in_specs=(row_spec, P(None), P(None, None), P('ep', None, 'tp'), P('ep', None, 'tp'), P('ep', 'tp', None), row_spec), out_specs=row_spec, check_vma=False)
```

```python
import functools

import jax
import jax.numpy as jnp
from jax import lax
from jax.experimental import pallas as pl
from jax.experimental.pallas import tpu as pltpu
from jax.sharding import PartitionSpec as P

NORM_EPS = 1e-5
MESH = pl.DeviceIdType.MESH
BF16 = jnp.bfloat16
F32 = jnp.float32
SUBS = 4
PIECES = 4
LATE_X_SHARE = 2
ORDER = (
    ('ns', 2, 3), ('ns', 1, 0), ('ns', 2, 1), ('E2',), ('ns', 1, 2), ('G', 0), ('A', 1, 0), ('A', 2, 3), ('T', 0),
    ('U0', 0), ('U1', 0), ('A', 1, 2), ('A', 2, 1), ('S', 2, 3), ('A', 3, 3), ('H', 0), ('ns', 2, 0), ('A', 3, 0),
    ('ns', 1, 1), ('ns', 2, 2), ('D', 0), ('A', 3, 2), ('ns', 1, 3), ('meta',), ('A', 3, 1), ('S', 3, 0), ('A', 2, 0),
    ('S', 3, 3), ('A', 1, 1), ('S', 3, 2), ('S', 3, 1), ('S', 2, 1), ('PF', 3), ('A', 1, 3), ('A', 2, 2), ('G', 3),
    ('S', 2, 0), ('S', 1, 1), ('S', 1, 2), ('YS', 0), ('U0', 3), ('S', 1, 0), ('U1', 3), ('H', 3), ('T', 3),
    ('S', 1, 3), ('PF', 1), ('D', 3), ('f1', 2), ('f1', 0), ('YS', 3), ('f0', 3), ('S', 2, 2), ('G', 1), ('f0', 0),
    ('U0', 1), ('f1', 3), ('PF', 2), ('f0', 1), ('T', 1), ('U1', 1), ('H', 1), ('YM', 3), ('G', 2), ('f1', 1),
    ('f0', 2), ('D', 1), ('m0', 0), ('YS', 1), ('U0', 2), ('U1', 2), ('H', 2), ('YE', 3), ('wf',), ('YM', 0), ('m1', 2),
    ('T', 2), ('D', 2), ('p1', 0), ('YS', 2), ('m1', 0), ('p0', 1), ('p1', 1), ('m1', 1), ('m0', 1), ('m0', 2),
    ('p0', 0), ('YM', 2), ('YM', 1), ('p1', 3), ('O', 1), ('YE', 2), ('wp1',), ('O', 0), ('wp0',), ('YE', 1), ('wm1',),
    ('wm0',), ('V', 1), ('m1', 3), ('m0', 3), ('V', 0), ('p0', 3), ('N', 1), ('p0', 2), ('N', 0), ('YE', 0), ('WS',),
    ('p1', 2), ('O', 3), ('O', 2), ('V', 3), ('R', 0), ('V', 2), ('R', 1), ('N', 3), ('N', 2), ('WR',), ('R', 3),
    ('R', 2),
)


def route(normed, router_t, choice_t, capacity):
    logits = lax.dot_general(router_t, normed, (((1,), (1,)), ((), ())), preferred_element_type=F32)
    weights = jnp.exp(logits - jnp.max(logits, axis=0, keepdims=True))
    probs = weights / jnp.sum(weights, axis=0, keepdims=True)
    expert_ids = lax.broadcasted_iota(jnp.int32, logits.shape, 0)
    chosen = [expert_ids == choice_t[k:k + 1] for k in range(2)]
    picked = [jnp.sum(jnp.where(hit, probs, 0.0), axis=0, keepdims=True) for hit in chosen]
    total = picked[0] + picked[1]
    gate = jnp.where(chosen[0], picked[0] / total, jnp.where(chosen[1], picked[1] / total, 0.0))
    any_chosen = jnp.where(chosen[0], 1.0, jnp.where(chosen[1], 1.0, 0.0))
    rows = normed.shape[0]
    earlier = lax.broadcasted_iota(jnp.int32, (rows, rows), 0) < lax.broadcasted_iota(jnp.int32, (rows, rows), 1)
    earlier = jnp.where(earlier, 1.0, 0.0).astype(BF16)
    position = jnp.dot(any_chosen.astype(BF16), earlier, preferred_element_type=F32)
    kept = (any_chosen > 0.0) & (position < capacity)
    return jnp.where(kept, position, -1.0), jnp.where(kept, gate, 0.0)


def moe_kernel(capacity, ny, nx, resid, scale, router_t, choice_t, w_gate, w_up, w_down, out, ug,
               w1, v1, w2, xg, hid, hpart, sums, rfar, rplus, rminus, yown, yfar, yplus, yminus, ycon, vfar, vplus, vminus, wsum, wown, wfar, wplus, wminus, fin, xres, utile, gsplit, meta, meta_src,
               load_sem, tile_sem, send_sem, recv_sem):
    rows, d_model = resid.shape
    half = d_model // 2
    quarter = half // ny
    width = w_gate.shape[2]
    chunk = rows // (2 * PIECES)
    sub = rows // SUBS
    y = lax.axis_index('tp')
    ep = lax.axis_index('ep')
    core = lax.rem(ep, 2)
    x = ep // 2

    def ep_at(dx, other=False):
        return lax.rem(x + dx + nx, nx) * 2 + ((1 - core) if other else core)

    def dev_x(dx, other=False):
        return {'ep': ep_at(dx, other)}

    def dev_y(dy, other=False):
        return {'tp': lax.rem(y + dy + ny, ny), 'ep': ep_at(0, other)}

    partner = dev_x(0, True)

    first_load = pltpu.make_async_copy(resid, utile.at[0], load_sem.at[15])
    first_load.start()
    barrier = pltpu.get_barrier_semaphore()
    peers = [dev_x(dx, o) for dx in range(nx) for o in (False, True) if (dx, o) != (0, False)]
    peers += [dev_y(dy, o) for dy in (1, -1) for o in (False, True)]
    for peer in peers:
        pl.semaphore_signal(barrier, inc=1, device_id=peer, device_id_type=MESH)
    pl.semaphore_wait(barrier, len(peers))

    copies = []

    def remote(src, dst, device):
        at = len(copies)
        copy = pltpu.make_async_remote_copy(src_ref=src, dst_ref=dst, send_sem=send_sem.at[at], recv_sem=recv_sem.at[at], device_id=device, device_id_type=MESH)
        copies.append(copy)
        copy.start()
        return copy

    sent = []

    def finish_send(copy):
        copy.wait_send()
        sent.append(copy)

    locals_ = []

    def local(src, dst):
        copy = pltpu.make_async_copy(src, dst, load_sem.at[len(locals_)])
        locals_.append(copy)
        copy.start()
        return copy

    my_half = pl.multiple_of(core * half, half)
    other_half = pl.multiple_of((1 - core) * half, half)
    my_quarter = pl.multiple_of(my_half + y * quarter, quarter)
    other_quarter = pl.multiple_of(other_half + y * quarter, quarter)

    parity = lax.rem(y, 2)

    def piece(q, mine=True):
        side = parity if mine else 1 - parity
        return pl.ds(pl.multiple_of(side * (rows // 2) + q * chunk, chunk), chunk)

    first_load.wait()
    loads = {}
    for e in range(2):
        loads[e] = (local(w_gate.at[e], w1.at[e]), local(w_up.at[e], v1.at[e]))

    def normalize(i, carry):
        at = pl.ds(pl.multiple_of(i * 16, 16), 16)
        values = utile[0, at, :].astype(F32)
        centered = values - jnp.mean(values, axis=-1, keepdims=True)
        variance = jnp.mean(centered * centered, axis=-1, keepdims=True)
        utile[0, at, :] = (centered * lax.rsqrt(variance + NORM_EPS) * scale[...].astype(F32)).astype(BF16)
        return carry

    lax.fori_loop(0, rows // 16, normalize, 0)

    def meta_for(dx):
        return meta_src.at[lax.rem(x + dx + nx, nx)]

    ax = {}

    def near_send(slot, q):
        ax[slot, q] = remote(utile.at[0, piece(q)], ug.at[slot, 0, piece(q)], dev_x(1 if slot == 1 else -1))

    meta_copies, entry, w2_copies, res_copies = {}, {}, [], []

    def own_routes():
        entry['own'] = remote(utile.at[0], utile.at[1], partner)
        w2_copies.extend(local(w_down.at[e, :, pl.ds(my_half, half)], w2.at[e]) for e in range(2))
        positions, gate_rows = route(utile[0], router_t[...], choice_t[...], capacity)
        per_chip = positions.shape[0] // nx
        for k in range(nx):
            meta_src[k, :per_chip] = positions[k * per_chip:(k + 1) * per_chip]
            meta_src[k, per_chip:] = gate_rows[k * per_chip:(k + 1) * per_chip]
        meta[0] = meta_src[x]
        meta_copies[0, 1] = remote(meta_for(0), meta.at[1], partner)
        w2_copies.extend(remote(w_down.at[e, :, pl.ds(other_half, half)], w2.at[2 + e], partner) for e in range(2))
        res_copies.append(local(resid.at[:, pl.ds(my_quarter, quarter)], xres.at[0]))
        res_copies.append(remote(resid.at[:, pl.ds(other_quarter, quarter)], xres.at[1], partner))

    def send_meta():
        for slot, dx in ((1, 1), (2, -1), (3, 2)):
            for lane in range(2):
                meta_copies[slot, lane] = remote(meta_for(dx), meta.at[slot * 2 + lane], dev_x(dx, lane == 1))

    ay, pushed = {}, {1: [], 2: [], 3: []}

    def push(slot, q, mine):
        at = piece(q, mine)
        pushed[slot].append(remote(ug.at[slot, 0, at], ug.at[slot, 1, at], partner))

    def y_forward(slot, q):
        up = slot == 1 or (slot == 3 and q % 2 == 0)
        ay[slot, q] = remote(ug.at[slot, 0, piece(q)], ug.at[slot, 0, piece(q)], dev_y(1 if up else -1))

    def on_piece(slot, q):
        ax[slot, q].wait_recv()
        if slot == 2 - (q + 1) % 2:
            ax[3, q] = remote(ug.at[slot, 0, piece(q)], ug.at[3, 0, piece(q)], dev_x(1 if slot == 1 else -1))
        y_forward(slot, q)
        push(slot, q, True)

    def on_side(slot, q):
        ay[slot, q].wait_recv()
        push(slot, q, False)

    def slot_onehot(pos_row):
        return lax.broadcasted_iota(jnp.int32, (capacity, rows), 0).astype(F32) == pos_row

    tile = min(1024, d_model)
    tiles = d_model // tile

    def fetch(slot, t, lane):
        cols = pl.ds(t * tile, tile) if isinstance(t, int) else pl.ds(pl.multiple_of(t * tile, tile), tile)
        return pltpu.make_async_copy(ug.at[slot, lane, :, cols], utile.at[lane, :, cols], tile_sem.at[lane * tiles + t])

    def prefetch(slot):
        if 'own' in entry:
            finish_send(entry.pop('own'))
            for q in range(PIECES):
                finish_send(ax[1, q])
                finish_send(ax[2, q])
        for copy in pushed[slot]:
            copy.wait_recv()
        for t in range(tiles):
            for lane in range(2):
                fetch(slot, t, lane).start()

    def meta_rows(slot, lane, e):
        row = 2 * core + e if e < 2 else 2 * (1 - core) + e - 2
        return meta[slot * 2 + lane, pl.ds(row, 1), :], meta[slot * 2 + lane, pl.ds(4 + row, 1), :]

    def gates(slot):
        for lane in range(2):
            parts = []
            for e in range(4):
                pos_row, gate_row = meta_rows(slot, lane, e)
                parts.append(jnp.where(slot_onehot(pos_row), gate_row, 0.0))
            gate_mat = jnp.concatenate(parts, axis=0).T
            for term in range(3):
                part = gate_mat.astype(BF16)
                gsplit[lane, term] = part
                gate_mat = gate_mat - part.astype(F32)

    def gather(slot):
        picks = []
        for lane in range(2):
            if (slot, lane) != (0, 0):
                meta_copies[slot, lane].wait_recv()
            parts = [slot_onehot(meta_rows(slot, lane, e)[0]).astype(F32).astype(BF16) for e in range(2)]
            picks.append(jnp.concatenate(parts, axis=0))
        if slot == 0:
            entry['own'].wait_recv()

        def body(t, carry):
            cols = pl.ds(pl.multiple_of(t * tile, tile), tile)
            for lane in range(2):
                if slot:
                    fetch(slot, t, lane).wait()
                got = jnp.dot(picks[lane], utile[lane, :, cols], preferred_element_type=F32).astype(BF16)
                for e in range(2):
                    xg[e, lane * capacity:(lane + 1) * capacity, cols] = got[e * capacity:(e + 1) * capacity]
            return carry

        lax.fori_loop(0, tiles, body, 0)

    ftile = min(256, width)

    def gate_up(e, slot):
        if slot == 0:
            for copy in loads[e]:
                copy.wait()

        def body(t, carry):
            cols = pl.ds(pl.multiple_of(t * ftile, ftile), ftile)
            gate_act = jnp.dot(xg[e], w1[e, :, cols], preferred_element_type=F32)
            up_act = jnp.dot(xg[e], v1[e, :, cols], preferred_element_type=F32)
            hid[e, :, cols] = (jax.nn.silu(gate_act) * up_act).astype(BF16)
            return carry

        lax.fori_loop(0, width // ftile, body, 0)

    xcols = yfar.shape[2]
    ycols = quarter - xcols

    shared = {}

    def share_hidden(slot):
        shared[slot] = remote(hid, hpart.at[slot], partner)

    def down(slot):
        if slot == 0:
            for copy in w2_copies:
                copy.wait_recv() if copy.is_remote else copy.wait()
        shared[slot].wait_recv()

        def body(t, carry):
            cols = pl.ds(pl.multiple_of(t * quarter, quarter), quarter)
            outs = []
            for e in range(4):
                lhs = hid[e] if e < 2 else hpart[slot, e - 2]
                outs.append(jnp.dot(lhs, w2[e, :, cols], preferred_element_type=F32).astype(BF16))
            for lane in range(2):
                stack = []
                for e in range(4):
                    at = lane if e < 2 else 1 - lane
                    stack.append(outs[e][at * capacity:(at + 1) * capacity])
                stacked = jnp.concatenate(stack, axis=0)
                total = jnp.dot(gsplit[lane, 0], stacked, preferred_element_type=F32)
                for term in (1, 2):
                    total += jnp.dot(gsplit[lane, term], stacked, preferred_element_type=F32)
                total = total.astype(BF16)
                sums[slot, lane, :, pl.ds(pl.multiple_of(t * xcols, 128), xcols)] = total[:, :xcols]
                ycon[slot, lane, :, pl.ds(pl.multiple_of(t * ycols, 128), ycols)] = total[:, xcols:]
            return carry

        lax.fori_loop(0, ny, body, 0)
        finish_send(shared[slot])

    rs = {}

    def add_into(ref, other):
        ref[...] = (ref[...].astype(F32) + other[...].astype(F32)).astype(BF16)

    def rs_start(tag, src, landing, dev):
        far, plus, minus = landing
        rs[tag] = {'f0': remote(src(2, 0), far.at[0], dev(1)), 'f1': remote(src(2, 1), far.at[1], dev(-1)),
                   'p1': remote(src(1, 1), plus.at[1], dev(1)), 'm0': remote(src(-1, 0), minus.at[0], dev(-1))}

    def rs_mid(tag, src, landing, dev):
        far, plus, minus = landing
        rs[tag]['f0'].wait_recv()
        add_into(src(1, 0), far.at[0])
        rs[tag]['p0'] = remote(src(1, 0), plus.at[0], dev(1))
        rs[tag]['f1'].wait_recv()
        add_into(src(-1, 1), far.at[1])
        rs[tag]['m1'] = remote(src(-1, 1), minus.at[1], dev(-1))

    def rs_end(tag):
        for name in ('m0', 'p1', 'p0', 'm1'):
            rs[tag][name].wait_recv()

    def y_args(slot):
        def src(dy, lane):
            return ycon.at[slot, lane, :, pl.ds(pl.multiple_of(lax.rem(y + dy + ny, ny) * ycols, 128), ycols)]
        return src, (vfar.at[slot], vplus.at[slot], vminus.at[slot]), dev_y

    def y_start(slot):
        rs_start(slot, *y_args(slot))

    def y_mid(slot):
        rs_mid(slot, *y_args(slot))

    def y_end(slot):
        rs_end(slot)
        src = y_args(slot)[0]
        for lane in range(2):
            total = src(0, lane)[...].astype(F32) + vplus[slot, lane].astype(F32) + vminus[slot, lane].astype(F32)
            if slot == 0:
                wown[lane] = total
            else:
                wsum[slot - 1, lane] = total.astype(BF16)

    def w_src(dx, lane):
        return wsum.at[{-1: 0, 1: 1, 2: 2}[dx], lane]

    def w_far():
        rs['w'] = {'f0': remote(w_src(2, 0), wfar.at[0], dev_x(1)), 'f1': remote(w_src(2, 1), wfar.at[1], dev_x(-1))}

    wx = {}

    def w_send(name):
        lane = int(name[1])
        dx = 1 if name[0] == 'p' else -1
        if name in ('p0', 'm1'):
            rs['w']['f%d' % lane].wait_recv()
            add_into(w_src(dx, lane), wfar.at[lane])
        landing = wplus if dx == 1 else wminus
        wx[name] = remote(w_src(dx, lane), landing.at[lane], dev_x(dx))

    def sub_rows(j):
        return pl.ds(j * sub, sub)

    sx = {}

    def send_sum(name, slot, lane, j, landing, dx):
        sx[name, j] = remote(sums.at[slot, lane, sub_rows(j)], landing.at[lane, sub_rows(j)], dev_x(dx))

    def x_send(name, j):
        lane = int(name[1])
        if name[0] == 'f':
            send_sum(name, 3, lane, j, rfar, 1 if lane == 0 else -1)
            return
        slot, landing, dx = (2, rplus, 1) if name[0] == 'p' else (1, rminus, -1)
        if name in ('p0', 'm1'):
            sx['f%d' % lane, j].wait_recv()
            add_into(sums.at[slot, lane, sub_rows(j)], rfar.at[lane, sub_rows(j)])
        send_sum(name, slot, lane, j, landing, dx)

    def q_cols(dy):
        return pl.ds(pl.multiple_of(lax.rem(y + dy + ny, ny) * xcols, 128), xcols)

    def send_y(name, lane, j, dcol, landing, dy):
        sx[name, j] = remote(sums.at[0, lane, sub_rows(j), q_cols(dcol)], landing.at[lane, sub_rows(j)], dev_y(dy))

    def stage_own(j):
        for name in ('m0', 'p1', 'p0', 'm1'):
            sx[name, j].wait_recv()
        at = sub_rows(j)
        for lane in range(2):
            cols = q_cols(0)
            yown[lane, at, :] = sums[0, lane, at, cols].astype(F32) + rplus[lane, at, cols].astype(F32) + rminus[lane, at, cols].astype(F32)
        for lane in range(2):
            sums[0, lane, at, :] = (sums[0, lane, at, :].astype(F32) + rplus[lane, at, :].astype(F32) + rminus[lane, at, :].astype(F32)).astype(BF16)
        send_y('yf0', 0, j, 2, yfar, 1)
        send_y('yf1', 1, j, 2, yfar, -1)
        send_y('yp1', 1, j, 1, yplus, 1)
        send_y('ym0', 0, j, -1, yminus, -1)

    def stage_yfar(j):
        sx['yf0', j].wait_recv()
        sx['yf1', j].wait_recv()
        at = sub_rows(j)
        cols = q_cols(1)
        sums[0, 0, at, cols] = (sums[0, 0, at, cols].astype(F32) + yfar[0, at, :].astype(F32)).astype(BF16)
        send_y('yp0', 0, j, 1, yplus, 1)
        cols = q_cols(-1)
        sums[0, 1, at, cols] = (sums[0, 1, at, cols].astype(F32) + yfar[1, at, :].astype(F32)).astype(BF16)
        send_y('ym1', 1, j, -1, yminus, -1)

    done = {}
    pending = [res_copies]

    def residual_ready():
        for copy in pending.pop() if pending else ():
            copy.wait_recv() if copy.is_remote else copy.wait()

    def share_rows(key, at, first, cols):
        def place(start):
            return out.at[at, pl.ds(pl.multiple_of(start + first, 128), cols)]

        src = fin.at[:, at, pl.ds(first, cols)]
        for lane in range(2):
            done['up', lane, key] = remote(src.at[lane], place(my_quarter), dev_y(1, lane == 1))
            done['down', lane, key] = remote(src.at[lane], place(my_quarter), dev_y(-1, lane == 1))
        done['own', key] = local(src.at[0], place(my_quarter))
        done['pair', key] = remote(src.at[1], place(my_quarter), partner)

    def relay_rows(key, at, first, cols):
        def place(start):
            return out.at[at, pl.ds(pl.multiple_of(start + first, 128), cols)]

        done['up', 0, key].wait_recv()
        start = my_half + lax.rem(y - 1 + ny, ny) * quarter
        done['up2', key] = remote(place(start), place(start), dev_y(1))
        done['down', 1, key].wait_recv()
        start = other_half + lax.rem(y + 1, ny) * quarter
        done['down2', key] = remote(place(start), place(start), dev_y(-1))

    def stage_final(j):
        for name in ('ym0', 'yp1', 'yp0', 'ym1'):
            sx[name, j].wait_recv()
        residual_ready()
        at = sub_rows(j)
        for lane in range(2):
            total = yown[lane, at, :] + yplus[lane, at, :].astype(F32) + yminus[lane, at, :].astype(F32)
            fin[lane, at, :xcols] = (xres[lane, at, :xcols].astype(F32) + total).astype(BF16)
        share_rows(j, at, 0, xcols)

    def stage_relay(j):
        relay_rows(j, sub_rows(j), 0, xcols)

    def w_share():
        for name in ('m0', 'p1', 'p0', 'm1'):
            wx[name].wait_recv()
        residual_ready()
        for lane in range(2):
            total = wown[lane] + wplus[lane].astype(F32) + wminus[lane].astype(F32)
            fin[lane, :, xcols:] = (xres[lane, :, xcols:].astype(F32) + total).astype(BF16)
        share_rows('w', pl.ds(0, rows), xcols, ycols)

    def w_relay():
        relay_rows('w', pl.ds(0, rows), xcols, ycols)

    actions = {'E2': own_routes, 'ns': near_send, 'meta': send_meta, 'A': on_piece, 'S': on_side, 'PF': prefetch, 'G': gather,
               'U0': functools.partial(gate_up, 0), 'U1': functools.partial(gate_up, 1), 'H': share_hidden, 'T': gates, 'D': down,
               'YS': y_start, 'YM': y_mid, 'YE': y_end, 'wf': w_far, 'WS': w_share, 'WR': w_relay,
               'O': stage_own, 'V': stage_yfar, 'N': stage_final, 'R': stage_relay}
    for name in ('f0', 'f1', 'm0', 'm1', 'p0', 'p1'):
        actions[name] = functools.partial(x_send, name)
        actions['w' + name] = functools.partial(w_send, name)
    for name, *args in ORDER:
        actions[name](*args)
    for key in (*range(SUBS), 'w'):
        done['up', 1, key].wait_recv()
        done['down', 0, key].wait_recv()
        done['pair', key].wait_recv()
        done['up2', key].wait_recv()
        done['down2', key].wait_recv()
        done['own', key].wait()
    for copy in copies:
        if not any(copy is other for other in sent):
            copy.wait_send()


def solution(mesh):
    row_spec = P(('dp', 'ep'), None)
    ny, nx = mesh.shape['tp'], mesh.shape['ep'] // 2

    def device_step(resid_in, norm_scale, w_router, w_gate, w_up, w_down, choice):
        rows, d_model = resid_in.shape
        experts = w_router.shape[1]
        width = w_gate.shape[2]
        capacity = (2 * rows * choice.shape[1] + experts - 1) // experts
        half, slots = d_model // 2, 2 * capacity
        quarter = half // ny
        ycols = quarter // LATE_X_SHARE
        xcols = quarter - ycols

        hbm, vmem = pl.BlockSpec(memory_space=pl.ANY), pl.BlockSpec(memory_space=pltpu.VMEM)
        out, _ = pl.pallas_call(
            functools.partial(moe_kernel, capacity, ny, nx),
            out_shape=(jax.ShapeDtypeStruct((rows, d_model), BF16), jax.ShapeDtypeStruct((4, 2, rows, d_model), BF16)),
            in_specs=[hbm, vmem, vmem, vmem, hbm, hbm, hbm],
            out_specs=(hbm, hbm),
            scratch_shapes=[
                pltpu.VMEM((2, d_model, width), BF16),
                pltpu.VMEM((2, d_model, width), BF16),
                pltpu.VMEM((4, width, half), BF16),
                pltpu.VMEM((2, slots, d_model), BF16),
                pltpu.VMEM((2, slots, width), BF16),
                pltpu.VMEM((4, 2, slots, width), BF16),
                pltpu.VMEM((4, 2, rows, ny * xcols), BF16),
                pltpu.VMEM((2, rows, ny * xcols), BF16),
                pltpu.VMEM((2, rows, ny * xcols), BF16),
                pltpu.VMEM((2, rows, ny * xcols), BF16),
                pltpu.VMEM((2, rows, xcols), F32),
                pltpu.VMEM((2, rows, xcols), BF16),
                pltpu.VMEM((2, rows, xcols), BF16),
                pltpu.VMEM((2, rows, xcols), BF16),
                pltpu.VMEM((4, 2, rows, ny * ycols), BF16),
                pltpu.VMEM((4, 2, rows, ycols), BF16),
                pltpu.VMEM((4, 2, rows, ycols), BF16),
                pltpu.VMEM((4, 2, rows, ycols), BF16),
                pltpu.VMEM((3, 2, rows, ycols), BF16),
                pltpu.VMEM((2, rows, ycols), F32),
                pltpu.VMEM((2, rows, ycols), BF16),
                pltpu.VMEM((2, rows, ycols), BF16),
                pltpu.VMEM((2, rows, ycols), BF16),
                pltpu.VMEM((2, rows, quarter), BF16),
                pltpu.VMEM((2, rows, quarter), BF16),
                pltpu.VMEM((2, rows, d_model), BF16),
                pltpu.VMEM((2, 3, rows, 4 * capacity), BF16),
                pltpu.VMEM((2 * nx, 2 * experts // nx, rows), F32),
                pltpu.VMEM((nx, 2 * experts // nx, rows), F32),
                pltpu.SemaphoreType.DMA((16,)),
                pltpu.SemaphoreType.DMA((2 * (d_model // min(1024, d_model)),)),
                pltpu.SemaphoreType.DMA((256,)),
                pltpu.SemaphoreType.DMA((256,)),
            ],
            compiler_params=pltpu.CompilerParams(collective_id=0, has_side_effects=True, vmem_limit_bytes=67043328),
            name='moe_ring',
        )(resid_in, norm_scale[None, :], w_router.T, choice.T, w_gate, w_up, w_down)
        return out

    return jax.shard_map(device_step, mesh=mesh, in_specs=(row_spec, P(None), P(None, None), P('ep', None, 'tp'), P('ep', None, 'tp'), P('ep', 'tp', None), row_spec), out_specs=row_spec, check_vma=False)
```

```python
import functools

import jax
import jax.numpy as jnp
from jax import lax
from jax.experimental import pallas as pl
from jax.experimental.pallas import tpu as pltpu
from jax.sharding import PartitionSpec as P

NORM_EPS = 1e-5
MESH = pl.DeviceIdType.MESH
BF16 = jnp.bfloat16
F32 = jnp.float32
SUBS = 4
PIECES = 4
LATE_X_SHARE = 2
ORDER = (
    ('ns', 2, 3), ('ns', 1, 0), ('ns', 2, 1), ('E2',), ('ns', 1, 2), ('G', 0), ('A', 1, 0), ('A', 2, 3), ('T', 0),
    ('U0', 0), ('U1', 0), ('A', 1, 2), ('A', 2, 1), ('S', 2, 3), ('A', 3, 3), ('H', 0), ('ns', 2, 0), ('A', 3, 0),
    ('ns', 1, 1), ('ns', 2, 2), ('D', 0), ('A', 3, 2), ('ns', 1, 3), ('meta',), ('A', 3, 1), ('S', 3, 0), ('A', 2, 0),
    ('S', 3, 3), ('A', 1, 1), ('S', 3, 2), ('S', 3, 1), ('S', 2, 1), ('PF', 3), ('A', 1, 3), ('A', 2, 2), ('G', 3),
    ('S', 2, 0), ('S', 1, 1), ('S', 1, 2), ('YS', 0), ('U0', 3), ('S', 1, 0), ('U1', 3), ('H', 3), ('T', 3),
    ('S', 1, 3), ('PF', 1), ('D', 3), ('f1', 2), ('f1', 0), ('YS', 3), ('f0', 3), ('S', 2, 2), ('G', 1), ('f0', 0),
    ('U0', 1), ('f1', 3), ('PF', 2), ('f0', 1), ('T', 1), ('U1', 1), ('H', 1), ('YM', 3), ('G', 2), ('f1', 1),
    ('f0', 2), ('D', 1), ('m0', 0), ('YS', 1), ('U0', 2), ('U1', 2), ('H', 2), ('YE', 3), ('wf',), ('YM', 0), ('m1', 2),
    ('T', 2), ('D', 2), ('p1', 0), ('YS', 2), ('m1', 0), ('p0', 1), ('p1', 1), ('m1', 1), ('m0', 1), ('m0', 2),
    ('p0', 0), ('YM', 2), ('YM', 1), ('p1', 3), ('O', 1), ('YE', 2), ('wp1',), ('O', 0), ('wp0',), ('YE', 1), ('wm1',),
    ('wm0',), ('V', 1), ('m1', 3), ('m0', 3), ('V', 0), ('p0', 3), ('N', 1), ('p0', 2), ('N', 0), ('YE', 0), ('WS',),
    ('p1', 2), ('O', 3), ('O', 2), ('V', 3), ('R', 0), ('V', 2), ('R', 1), ('N', 3), ('N', 2), ('WR',), ('R', 3),
    ('R', 2),
)


def route(normed, router_t, choice_t, capacity):
    logits = lax.dot_general(router_t, normed, (((1,), (1,)), ((), ())), preferred_element_type=F32)
    weights = jnp.exp(logits - jnp.max(logits, axis=0, keepdims=True))
    probs = weights / jnp.sum(weights, axis=0, keepdims=True)
    expert_ids = lax.broadcasted_iota(jnp.int32, logits.shape, 0)
    chosen = [expert_ids == choice_t[k:k + 1] for k in range(2)]
    picked = [jnp.sum(jnp.where(hit, probs, 0.0), axis=0, keepdims=True) for hit in chosen]
    total = picked[0] + picked[1]
    gate = jnp.where(chosen[0], picked[0] / total, jnp.where(chosen[1], picked[1] / total, 0.0))
    any_chosen = jnp.where(chosen[0], 1.0, jnp.where(chosen[1], 1.0, 0.0))
    rows = normed.shape[0]
    earlier = lax.broadcasted_iota(jnp.int32, (rows, rows), 0) < lax.broadcasted_iota(jnp.int32, (rows, rows), 1)
    earlier = jnp.where(earlier, 1.0, 0.0).astype(BF16)
    position = jnp.dot(any_chosen.astype(BF16), earlier, preferred_element_type=F32)
    kept = (any_chosen > 0.0) & (position < capacity)
    return jnp.where(kept, position, -1.0), jnp.where(kept, gate, 0.0)


def moe_kernel(capacity, ny, nx, resid, scale, router_t, choice_t, w_gate, w_up, w_down, out, ug,
               w1, v1, w2, xg, hid, hpart, sums, rfar, rplus, rminus, yown, yfar, yplus, yminus, ycon, vfar, vplus, vminus, wsum, wown, wfar, wplus, wminus, fin, xres, utile, select, gate_col, meta, meta_src,
               load_sem, tile_sem, send_sem, recv_sem):
    rows, d_model = resid.shape
    half = d_model // 2
    quarter = half // ny
    width = w_gate.shape[2]
    chunk = rows // (2 * PIECES)
    sub = rows // SUBS
    y = lax.axis_index('tp')
    ep = lax.axis_index('ep')
    core = lax.rem(ep, 2)
    x = ep // 2

    def ep_at(dx, other=False):
        return lax.rem(x + dx + nx, nx) * 2 + ((1 - core) if other else core)

    def dev_x(dx, other=False):
        return {'ep': ep_at(dx, other)}

    def dev_y(dy, other=False):
        return {'tp': lax.rem(y + dy + ny, ny), 'ep': ep_at(0, other)}

    partner = dev_x(0, True)

    first_load = pltpu.make_async_copy(resid, utile.at[0], load_sem.at[15])
    first_load.start()
    barrier = pltpu.get_barrier_semaphore()
    peers = [dev_x(dx, o) for dx in range(nx) for o in (False, True) if (dx, o) != (0, False)]
    peers += [dev_y(dy, o) for dy in (1, -1) for o in (False, True)]
    for peer in peers:
        pl.semaphore_signal(barrier, inc=1, device_id=peer, device_id_type=MESH)
    pl.semaphore_wait(barrier, len(peers))

    copies = []

    def remote(src, dst, device):
        at = len(copies)
        copy = pltpu.make_async_remote_copy(src_ref=src, dst_ref=dst, send_sem=send_sem.at[at], recv_sem=recv_sem.at[at], device_id=device, device_id_type=MESH)
        copies.append(copy)
        copy.start()
        return copy

    sent = []

    def finish_send(copy):
        copy.wait_send()
        sent.append(copy)

    locals_ = []

    def local(src, dst):
        copy = pltpu.make_async_copy(src, dst, load_sem.at[len(locals_)])
        locals_.append(copy)
        copy.start()
        return copy

    my_half = pl.multiple_of(core * half, half)
    other_half = pl.multiple_of((1 - core) * half, half)
    my_quarter = pl.multiple_of(my_half + y * quarter, quarter)
    other_quarter = pl.multiple_of(other_half + y * quarter, quarter)

    parity = lax.rem(y, 2)

    def piece(q, mine=True):
        side = parity if mine else 1 - parity
        return pl.ds(pl.multiple_of(side * (rows // 2) + q * chunk, chunk), chunk)

    first_load.wait()
    loads = {}
    for e in range(2):
        loads[e] = (local(w_gate.at[e], w1.at[e]), local(w_up.at[e], v1.at[e]))

    gain = scale[...].astype(F32)[None, :]

    def normalize(i, carry):
        at = pl.ds(pl.multiple_of(i * 16, 16), 16)
        values = utile[0, at, :].astype(F32)
        centered = values - jnp.mean(values, axis=-1, keepdims=True)
        variance = jnp.mean(centered * centered, axis=-1, keepdims=True)
        utile[0, at, :] = (centered * lax.rsqrt(variance + NORM_EPS) * gain).astype(BF16)
        return carry

    lax.fori_loop(0, rows // 16, normalize, 0)

    def meta_for(dx):
        return meta_src.at[lax.rem(x + dx + nx, nx)]

    ax = {}

    def near_send(slot, q):
        ax[slot, q] = remote(utile.at[0, piece(q)], ug.at[slot, 0, piece(q)], dev_x(1 if slot == 1 else -1))

    meta_copies, entry, w2_copies, res_copies = {}, {}, [], []

    def own_routes():
        entry['own'] = remote(utile.at[0], utile.at[1], partner)
        w2_copies.extend(local(w_down.at[e, :, pl.ds(my_half, half)], w2.at[e]) for e in range(2))
        positions, gate_rows = route(utile[0], router_t[...], choice_t[...], capacity)
        per_chip = positions.shape[0] // nx
        for k in range(nx):
            meta_src[k, :per_chip] = positions[k * per_chip:(k + 1) * per_chip]
            meta_src[k, per_chip:] = gate_rows[k * per_chip:(k + 1) * per_chip]
        meta[0] = meta_src[x]
        meta_copies[0, 1] = remote(meta_for(0), meta.at[1], partner)
        w2_copies.extend(remote(w_down.at[e, :, pl.ds(other_half, half)], w2.at[2 + e], partner) for e in range(2))
        res_copies.append(local(resid.at[:, pl.ds(my_quarter, quarter)], xres.at[0]))
        res_copies.append(remote(resid.at[:, pl.ds(other_quarter, quarter)], xres.at[1], partner))

    def send_meta():
        for slot, dx in ((1, 1), (2, -1), (3, 2)):
            for lane in range(2):
                meta_copies[slot, lane] = remote(meta_for(dx), meta.at[slot * 2 + lane], dev_x(dx, lane == 1))

    ay, pushed = {}, {1: [], 2: [], 3: []}

    def push(slot, q, mine):
        at = piece(q, mine)
        pushed[slot].append(remote(ug.at[slot, 0, at], ug.at[slot, 1, at], partner))

    def y_forward(slot, q):
        up = slot == 1 or (slot == 3 and q % 2 == 0)
        ay[slot, q] = remote(ug.at[slot, 0, piece(q)], ug.at[slot, 0, piece(q)], dev_y(1 if up else -1))

    def on_piece(slot, q):
        ax[slot, q].wait_recv()
        if slot == 2 - (q + 1) % 2:
            ax[3, q] = remote(ug.at[slot, 0, piece(q)], ug.at[3, 0, piece(q)], dev_x(1 if slot == 1 else -1))
        y_forward(slot, q)
        push(slot, q, True)

    def on_side(slot, q):
        ay[slot, q].wait_recv()
        push(slot, q, False)

    def slot_onehot(pos_row):
        return lax.broadcasted_iota(jnp.int32, (capacity, rows), 0).astype(F32) == pos_row

    tile = min(1024, d_model)
    tiles = d_model // tile

    def fetch(slot, t, lane):
        cols = pl.ds(t * tile, tile) if isinstance(t, int) else pl.ds(pl.multiple_of(t * tile, tile), tile)
        return pltpu.make_async_copy(ug.at[slot, lane, :, cols], utile.at[lane, :, cols], tile_sem.at[lane * tiles + t])

    def prefetch(slot):
        if 'own' in entry:
            finish_send(entry.pop('own'))
            for q in range(PIECES):
                finish_send(ax[1, q])
                finish_send(ax[2, q])
        for copy in pushed[slot]:
            copy.wait_recv()
        for t in range(tiles):
            for lane in range(2):
                fetch(slot, t, lane).start()

    def meta_rows(slot, lane, e):
        row = 2 * core + e if e < 2 else 2 * (1 - core) + e - 2
        return meta[slot * 2 + lane, pl.ds(row, 1), :], meta[slot * 2 + lane, pl.ds(4 + row, 1), :]

    def gates(slot):
        for lane in range(2):
            taken = jnp.zeros((1, rows), F32)
            picks, weights = ([], []), [jnp.zeros((1, rows), F32), jnp.zeros((1, rows), F32)]
            for e in range(4):
                pos_row, gate_row = meta_rows(slot, lane, e)
                hit = slot_onehot(pos_row)
                for k in range(2):
                    here = taken == float(k)
                    picks[k].append(jnp.where(hit, jnp.where(here, 1.0, 0.0), 0.0))
                    weights[k] = weights[k] + jnp.where(here, jnp.where(pos_row >= 0.0, gate_row, 0.0), 0.0)
                taken = taken + jnp.where(pos_row >= 0.0, 1.0, 0.0)
            for k in range(2):
                select[lane, k] = jnp.concatenate(picks[k], axis=0).T.astype(BF16)
            columns = jnp.concatenate([*weights, jnp.zeros((6, rows), F32)], axis=0).T
            for k in range(2):
                gate_col[lane, k] = jnp.broadcast_to(columns[:, k:k + 1], gate_col.shape[2:])

    def gather(slot):
        picks = []
        for lane in range(2):
            if (slot, lane) != (0, 0):
                meta_copies[slot, lane].wait_recv()
            parts = [slot_onehot(meta_rows(slot, lane, e)[0]).astype(F32).astype(BF16) for e in range(2)]
            picks.append(jnp.concatenate(parts, axis=0))
        if slot == 0:
            entry['own'].wait_recv()

        def body(t, carry):
            cols = pl.ds(pl.multiple_of(t * tile, tile), tile)
            for lane in range(2):
                if slot:
                    fetch(slot, t, lane).wait()
                got = jnp.dot(picks[lane], utile[lane, :, cols], preferred_element_type=F32).astype(BF16)
                for e in range(2):
                    xg[e, lane * capacity:(lane + 1) * capacity, cols] = got[e * capacity:(e + 1) * capacity]
            return carry

        lax.fori_loop(0, tiles, body, 0)

    ftile = min(256, width)

    def gate_up(e, slot):
        if slot == 0:
            for copy in loads[e]:
                copy.wait()

        def body(t, carry):
            cols = pl.ds(pl.multiple_of(t * ftile, ftile), ftile)
            gate_act = jnp.dot(xg[e], w1[e, :, cols], preferred_element_type=F32)
            up_act = jnp.dot(xg[e], v1[e, :, cols], preferred_element_type=F32)
            hid[e, :, cols] = (jax.nn.silu(gate_act) * up_act).astype(BF16)
            return carry

        lax.fori_loop(0, width // ftile, body, 0)

    xcols = yfar.shape[2]
    ycols = quarter - xcols

    shared = {}

    def share_hidden(slot):
        shared[slot] = remote(hid, hpart.at[slot], partner)

    def down(slot):
        if slot == 0:
            for copy in w2_copies:
                copy.wait_recv() if copy.is_remote else copy.wait()
        shared[slot].wait_recv()

        def body(t, carry):
            cols = pl.ds(pl.multiple_of(t * quarter, quarter), quarter)
            outs = []
            for e in range(4):
                lhs = hid[e] if e < 2 else hpart[slot, e - 2]
                outs.append(jnp.dot(lhs, w2[e, :, cols], preferred_element_type=F32).astype(BF16))
            for lane in range(2):
                stack = []
                for e in range(4):
                    at = lane if e < 2 else 1 - lane
                    stack.append(outs[e][at * capacity:(at + 1) * capacity])
                stacked = jnp.concatenate(stack, axis=0)
                total = jnp.dot(select[lane, 0], stacked, preferred_element_type=F32) * gate_col[lane, 0][:, :1]
                total += jnp.dot(select[lane, 1], stacked, preferred_element_type=F32) * gate_col[lane, 1][:, :1]
                total = total.astype(BF16)
                sums[slot, lane, :, pl.ds(pl.multiple_of(t * xcols, 128), xcols)] = total[:, :xcols]
                ycon[slot, lane, :, pl.ds(pl.multiple_of(t * ycols, 128), ycols)] = total[:, xcols:]
            return carry

        lax.fori_loop(0, ny, body, 0)
        finish_send(shared[slot])

    rs = {}

    def add_into(ref, other):
        ref[...] = (ref[...].astype(F32) + other[...].astype(F32)).astype(BF16)

    def rs_start(tag, src, landing, dev):
        far, plus, minus = landing
        rs[tag] = {'f0': remote(src(2, 0), far.at[0], dev(1)), 'f1': remote(src(2, 1), far.at[1], dev(-1)),
                   'p1': remote(src(1, 1), plus.at[1], dev(1)), 'm0': remote(src(-1, 0), minus.at[0], dev(-1))}

    def rs_mid(tag, src, landing, dev):
        far, plus, minus = landing
        rs[tag]['f0'].wait_recv()
        add_into(src(1, 0), far.at[0])
        rs[tag]['p0'] = remote(src(1, 0), plus.at[0], dev(1))
        rs[tag]['f1'].wait_recv()
        add_into(src(-1, 1), far.at[1])
        rs[tag]['m1'] = remote(src(-1, 1), minus.at[1], dev(-1))

    def rs_end(tag):
        for name in ('m0', 'p1', 'p0', 'm1'):
            rs[tag][name].wait_recv()

    def y_args(slot):
        def src(dy, lane):
            return ycon.at[slot, lane, :, pl.ds(pl.multiple_of(lax.rem(y + dy + ny, ny) * ycols, 128), ycols)]
        return src, (vfar.at[slot], vplus.at[slot], vminus.at[slot]), dev_y

    def y_start(slot):
        rs_start(slot, *y_args(slot))

    def y_mid(slot):
        rs_mid(slot, *y_args(slot))

    def y_end(slot):
        rs_end(slot)
        src = y_args(slot)[0]
        for lane in range(2):
            total = src(0, lane)[...].astype(F32) + vplus[slot, lane].astype(F32) + vminus[slot, lane].astype(F32)
            if slot == 0:
                wown[lane] = total
            else:
                wsum[slot - 1, lane] = total.astype(BF16)

    def w_src(dx, lane):
        return wsum.at[{-1: 0, 1: 1, 2: 2}[dx], lane]

    def w_far():
        rs['w'] = {'f0': remote(w_src(2, 0), wfar.at[0], dev_x(1)), 'f1': remote(w_src(2, 1), wfar.at[1], dev_x(-1))}

    wx = {}

    def w_send(name):
        lane = int(name[1])
        dx = 1 if name[0] == 'p' else -1
        if name in ('p0', 'm1'):
            rs['w']['f%d' % lane].wait_recv()
            add_into(w_src(dx, lane), wfar.at[lane])
        landing = wplus if dx == 1 else wminus
        wx[name] = remote(w_src(dx, lane), landing.at[lane], dev_x(dx))

    def sub_rows(j):
        return pl.ds(j * sub, sub)

    sx = {}

    def send_sum(name, slot, lane, j, landing, dx):
        sx[name, j] = remote(sums.at[slot, lane, sub_rows(j)], landing.at[lane, sub_rows(j)], dev_x(dx))

    def x_send(name, j):
        lane = int(name[1])
        if name[0] == 'f':
            send_sum(name, 3, lane, j, rfar, 1 if lane == 0 else -1)
            return
        slot, landing, dx = (2, rplus, 1) if name[0] == 'p' else (1, rminus, -1)
        if name in ('p0', 'm1'):
            sx['f%d' % lane, j].wait_recv()
            add_into(sums.at[slot, lane, sub_rows(j)], rfar.at[lane, sub_rows(j)])
        send_sum(name, slot, lane, j, landing, dx)

    def q_cols(dy):
        return pl.ds(pl.multiple_of(lax.rem(y + dy + ny, ny) * xcols, 128), xcols)

    def send_y(name, lane, j, dcol, landing, dy):
        sx[name, j] = remote(sums.at[0, lane, sub_rows(j), q_cols(dcol)], landing.at[lane, sub_rows(j)], dev_y(dy))

    def stage_own(j):
        for name in ('m0', 'p1', 'p0', 'm1'):
            sx[name, j].wait_recv()
        at = sub_rows(j)
        for lane in range(2):
            cols = q_cols(0)
            yown[lane, at, :] = sums[0, lane, at, cols].astype(F32) + rplus[lane, at, cols].astype(F32) + rminus[lane, at, cols].astype(F32)
        for lane in range(2):
            sums[0, lane, at, :] = (sums[0, lane, at, :].astype(F32) + rplus[lane, at, :].astype(F32) + rminus[lane, at, :].astype(F32)).astype(BF16)
        send_y('yf0', 0, j, 2, yfar, 1)
        send_y('yf1', 1, j, 2, yfar, -1)
        send_y('yp1', 1, j, 1, yplus, 1)
        send_y('ym0', 0, j, -1, yminus, -1)

    def stage_yfar(j):
        sx['yf0', j].wait_recv()
        sx['yf1', j].wait_recv()
        at = sub_rows(j)
        cols = q_cols(1)
        sums[0, 0, at, cols] = (sums[0, 0, at, cols].astype(F32) + yfar[0, at, :].astype(F32)).astype(BF16)
        send_y('yp0', 0, j, 1, yplus, 1)
        cols = q_cols(-1)
        sums[0, 1, at, cols] = (sums[0, 1, at, cols].astype(F32) + yfar[1, at, :].astype(F32)).astype(BF16)
        send_y('ym1', 1, j, -1, yminus, -1)

    done = {}
    pending = [res_copies]

    def residual_ready():
        for copy in pending.pop() if pending else ():
            copy.wait_recv() if copy.is_remote else copy.wait()

    def share_rows(key, at, first, cols):
        def place(start):
            return out.at[at, pl.ds(pl.multiple_of(start + first, 128), cols)]

        src = fin.at[:, at, pl.ds(first, cols)]
        for lane in range(2):
            done['up', lane, key] = remote(src.at[lane], place(my_quarter), dev_y(1, lane == 1))
            done['down', lane, key] = remote(src.at[lane], place(my_quarter), dev_y(-1, lane == 1))
        done['own', key] = local(src.at[0], place(my_quarter))
        done['pair', key] = remote(src.at[1], place(my_quarter), partner)

    def relay_rows(key, at, first, cols):
        def place(start):
            return out.at[at, pl.ds(pl.multiple_of(start + first, 128), cols)]

        done['up', 0, key].wait_recv()
        start = my_half + lax.rem(y - 1 + ny, ny) * quarter
        done['up2', key] = remote(place(start), place(start), dev_y(1))
        done['down', 1, key].wait_recv()
        start = other_half + lax.rem(y + 1, ny) * quarter
        done['down2', key] = remote(place(start), place(start), dev_y(-1))

    def stage_final(j):
        for name in ('ym0', 'yp1', 'yp0', 'ym1'):
            sx[name, j].wait_recv()
        residual_ready()
        at = sub_rows(j)
        for lane in range(2):
            total = yown[lane, at, :] + yplus[lane, at, :].astype(F32) + yminus[lane, at, :].astype(F32)
            fin[lane, at, :xcols] = (xres[lane, at, :xcols].astype(F32) + total).astype(BF16)
        share_rows(j, at, 0, xcols)

    def stage_relay(j):
        relay_rows(j, sub_rows(j), 0, xcols)

    def w_share():
        for name in ('m0', 'p1', 'p0', 'm1'):
            wx[name].wait_recv()
        residual_ready()
        for lane in range(2):
            total = wown[lane] + wplus[lane].astype(F32) + wminus[lane].astype(F32)
            fin[lane, :, xcols:] = (xres[lane, :, xcols:].astype(F32) + total).astype(BF16)
        share_rows('w', pl.ds(0, rows), xcols, ycols)

    def w_relay():
        relay_rows('w', pl.ds(0, rows), xcols, ycols)

    actions = {'E2': own_routes, 'ns': near_send, 'meta': send_meta, 'A': on_piece, 'S': on_side, 'PF': prefetch, 'G': gather,
               'U0': functools.partial(gate_up, 0), 'U1': functools.partial(gate_up, 1), 'H': share_hidden, 'T': gates, 'D': down,
               'YS': y_start, 'YM': y_mid, 'YE': y_end, 'wf': w_far, 'WS': w_share, 'WR': w_relay,
               'O': stage_own, 'V': stage_yfar, 'N': stage_final, 'R': stage_relay}
    for name in ('f0', 'f1', 'm0', 'm1', 'p0', 'p1'):
        actions[name] = functools.partial(x_send, name)
        actions['w' + name] = functools.partial(w_send, name)
    for name, *args in ORDER:
        actions[name](*args)
    for key in (*range(SUBS), 'w'):
        done['up', 1, key].wait_recv()
        done['down', 0, key].wait_recv()
        done['pair', key].wait_recv()
        done['up2', key].wait_recv()
        done['down2', key].wait_recv()
        done['own', key].wait()
    for copy in copies:
        if not any(copy is other for other in sent):
            copy.wait_send()


def solution(mesh):
    row_spec = P(('dp', 'ep'), None)
    ny, nx = mesh.shape['tp'], mesh.shape['ep'] // 2

    def device_step(resid_in, norm_scale, w_router, w_gate, w_up, w_down, choice):
        rows, d_model = resid_in.shape
        experts = w_router.shape[1]
        width = w_gate.shape[2]
        capacity = (2 * rows * choice.shape[1] + experts - 1) // experts
        half, slots = d_model // 2, 2 * capacity
        quarter = half // ny
        ycols = quarter // LATE_X_SHARE
        xcols = quarter - ycols

        hbm, vmem = pl.BlockSpec(memory_space=pl.ANY), pl.BlockSpec(memory_space=pltpu.VMEM)
        out, _ = pl.pallas_call(
            functools.partial(moe_kernel, capacity, ny, nx),
            out_shape=(jax.ShapeDtypeStruct((rows, d_model), BF16), jax.ShapeDtypeStruct((4, 2, rows, d_model), BF16)),
            in_specs=[hbm, vmem, vmem, vmem, hbm, hbm, hbm],
            out_specs=(hbm, hbm),
            scratch_shapes=[
                pltpu.VMEM((2, d_model, width), BF16),
                pltpu.VMEM((2, d_model, width), BF16),
                pltpu.VMEM((4, width, half), BF16),
                pltpu.VMEM((2, slots, d_model), BF16),
                pltpu.VMEM((2, slots, width), BF16),
                pltpu.VMEM((4, 2, slots, width), BF16),
                pltpu.VMEM((4, 2, rows, ny * xcols), BF16),
                pltpu.VMEM((2, rows, ny * xcols), BF16),
                pltpu.VMEM((2, rows, ny * xcols), BF16),
                pltpu.VMEM((2, rows, ny * xcols), BF16),
                pltpu.VMEM((2, rows, xcols), F32),
                pltpu.VMEM((2, rows, xcols), BF16),
                pltpu.VMEM((2, rows, xcols), BF16),
                pltpu.VMEM((2, rows, xcols), BF16),
                pltpu.VMEM((4, 2, rows, ny * ycols), BF16),
                pltpu.VMEM((4, 2, rows, ycols), BF16),
                pltpu.VMEM((4, 2, rows, ycols), BF16),
                pltpu.VMEM((4, 2, rows, ycols), BF16),
                pltpu.VMEM((3, 2, rows, ycols), BF16),
                pltpu.VMEM((2, rows, ycols), F32),
                pltpu.VMEM((2, rows, ycols), BF16),
                pltpu.VMEM((2, rows, ycols), BF16),
                pltpu.VMEM((2, rows, ycols), BF16),
                pltpu.VMEM((2, rows, quarter), BF16),
                pltpu.VMEM((2, rows, quarter), BF16),
                pltpu.VMEM((2, rows, d_model), BF16),
                pltpu.VMEM((2, 2, rows, 4 * capacity), BF16),
                pltpu.VMEM((2, 2, rows, 128), F32),
                pltpu.VMEM((2 * nx, 2 * experts // nx, rows), F32),
                pltpu.VMEM((nx, 2 * experts // nx, rows), F32),
                pltpu.SemaphoreType.DMA((16,)),
                pltpu.SemaphoreType.DMA((2 * (d_model // min(1024, d_model)),)),
                pltpu.SemaphoreType.DMA((256,)),
                pltpu.SemaphoreType.DMA((256,)),
            ],
            compiler_params=pltpu.CompilerParams(collective_id=0, has_side_effects=True, vmem_limit_bytes=67043328),
            name='moe_ring',
        )(resid_in, norm_scale, w_router.T, choice.T, w_gate, w_up, w_down)
        return jnp.where(choice[:, :1] >= 0, out, jnp.zeros((), BF16))

    return jax.shard_map(device_step, mesh=mesh, in_specs=(row_spec, P(None), P(None, None), P('ep', None, 'tp'), P('ep', None, 'tp'), P('ep', 'tp', None), row_spec), out_specs=row_spec, check_vma=False)
```

```python
import functools

import jax
import jax.numpy as jnp
from jax import lax
from jax.experimental import pallas as pl
from jax.experimental.pallas import tpu as pltpu
from jax.sharding import PartitionSpec as P

NORM_EPS = 1e-5
MESH = pl.DeviceIdType.MESH
BF16 = jnp.bfloat16
F32 = jnp.float32
SUBS = 4
PIECES = 4
LATE_X_SHARE = 2
ORDER = (
    ('ns', 1, 0), ('ns', 2, 3), ('ns', 2, 1), ('ns', 1, 2), ('E2',), ('A', 1, 0), ('A', 2, 3), ('A', 1, 2), ('A', 2, 1),
    ('G', 0), ('ns', 2, 0), ('ns', 2, 2), ('U0', 0), ('S', 2, 3), ('A', 3, 0), ('ns', 1, 3), ('A', 3, 3), ('U1', 0),
    ('H', 0), ('A', 3, 2), ('A', 3, 1), ('ns', 1, 1), ('S', 3, 3), ('S', 3, 0), ('T', 0), ('D', 0), ('A', 1, 3),
    ('meta',), ('A', 2, 0), ('S', 3, 2), ('S', 3, 1), ('PF', 3), ('S', 2, 1), ('S', 1, 2), ('S', 1, 0), ('A', 1, 1),
    ('A', 2, 2), ('G', 3), ('U0', 3), ('YS', 0), ('S', 1, 3), ('U1', 3), ('H', 3), ('S', 1, 1), ('T', 3), ('PF', 1),
    ('S', 2, 2), ('D', 3), ('f0', 2), ('f1', 0), ('f1', 2), ('f1', 3), ('YS', 3), ('S', 2, 0), ('G', 1), ('PF', 2),
    ('T', 1), ('f1', 1), ('U0', 1), ('YM', 0), ('U1', 1), ('f0', 0), ('f0', 1), ('YM', 3), ('H', 1), ('G', 2),
    ('f0', 3), ('D', 1), ('YS', 1), ('m0', 3), ('U0', 2), ('U1', 2), ('H', 2), ('YE', 3), ('wf',), ('m0', 0), ('T', 2),
    ('D', 2), ('p1', 3), ('m1', 3), ('m0', 1), ('YM', 1), ('p0', 3), ('p1', 0), ('m1', 0), ('p0', 0), ('YE', 0),
    ('p1', 1), ('YS', 2), ('YE', 1), ('O', 3), ('YM', 2), ('m0', 2), ('p0', 1), ('m1', 1), ('p0', 2), ('V', 3),
    ('m1', 2), ('O', 0), ('N', 3), ('V', 0), ('p1', 2), ('O', 1), ('N', 0), ('YE', 2), ('wp0',), ('wp1',), ('R', 3),
    ('wm0',), ('wm1',), ('V', 1), ('R', 0), ('O', 2), ('N', 1), ('V', 2), ('WS',), ('N', 2), ('R', 1), ('WR',),
    ('R', 2),
)


def route(normed, router_t, choice_t, capacity):
    logits = lax.dot_general(router_t, normed, (((1,), (1,)), ((), ())), preferred_element_type=F32)
    weights = jnp.exp(logits - jnp.max(logits, axis=0, keepdims=True))
    probs = weights / jnp.sum(weights, axis=0, keepdims=True)
    expert_ids = lax.broadcasted_iota(jnp.int32, logits.shape, 0)
    chosen = [expert_ids == choice_t[k:k + 1] for k in range(2)]
    picked = [jnp.sum(jnp.where(hit, probs, 0.0), axis=0, keepdims=True) for hit in chosen]
    total = picked[0] + picked[1]
    gate = jnp.where(chosen[0], picked[0] / total, jnp.where(chosen[1], picked[1] / total, 0.0))
    any_chosen = jnp.where(chosen[0], 1.0, jnp.where(chosen[1], 1.0, 0.0))
    rows = normed.shape[0]
    earlier = lax.broadcasted_iota(jnp.int32, (rows, rows), 0) < lax.broadcasted_iota(jnp.int32, (rows, rows), 1)
    earlier = jnp.where(earlier, 1.0, 0.0).astype(BF16)
    position = jnp.dot(any_chosen.astype(BF16), earlier, preferred_element_type=F32)
    kept = (any_chosen > 0.0) & (position < capacity)
    return jnp.where(kept, position, -1.0), jnp.where(kept, gate, 0.0)


def moe_kernel(capacity, ny, nx, resid, scale, router_t, choice_t, w_gate, w_up, w_down, out, ug,
               w1, v1, w2, xg, hid, hpart, sums, rfar, rplus, rminus, yown, yfar, yplus, yminus, ycon, vfar, vplus, vminus, wsum, wown, wfar, wplus, wminus, xres, utile, select, gate_col, meta, meta_src,
               load_sem, tile_sem, send_sem, recv_sem):
    rows, d_model = resid.shape
    half = d_model // 2
    quarter = half // ny
    width = w_gate.shape[2]
    chunk = rows // (2 * PIECES)
    sub = rows // SUBS
    y = lax.axis_index('tp')
    ep = lax.axis_index('ep')
    core = lax.rem(ep, 2)
    x = ep // 2

    def ep_at(dx, other=False):
        return lax.rem(x + dx + nx, nx) * 2 + ((1 - core) if other else core)

    def dev_x(dx, other=False):
        return {'ep': ep_at(dx, other)}

    def dev_y(dy, other=False):
        return {'tp': lax.rem(y + dy + ny, ny), 'ep': ep_at(0, other)}

    partner = dev_x(0, True)

    first_load = pltpu.make_async_copy(resid, utile.at[0], load_sem.at[15])
    first_load.start()
    barrier = pltpu.get_barrier_semaphore()
    peers = [dev_x(dx, o) for dx in range(nx) for o in (False, True) if (dx, o) != (0, False)]
    peers += [dev_y(dy, o) for dy in (1, -1) for o in (False, True)]
    for peer in peers:
        pl.semaphore_signal(barrier, inc=1, device_id=peer, device_id_type=MESH)
    pl.semaphore_wait(barrier, len(peers))

    copies = []

    def remote(src, dst, device):
        at = len(copies)
        copy = pltpu.make_async_remote_copy(src_ref=src, dst_ref=dst, send_sem=send_sem.at[at], recv_sem=recv_sem.at[at], device_id=device, device_id_type=MESH)
        copies.append(copy)
        copy.start()
        return copy

    sent = []

    def finish_send(copy):
        copy.wait_send()
        sent.append(copy)

    locals_ = []

    def local(src, dst):
        copy = pltpu.make_async_copy(src, dst, load_sem.at[len(locals_)])
        locals_.append(copy)
        copy.start()
        return copy

    my_half = pl.multiple_of(core * half, half)
    other_half = pl.multiple_of((1 - core) * half, half)
    my_quarter = pl.multiple_of(my_half + y * quarter, quarter)
    other_quarter = pl.multiple_of(other_half + y * quarter, quarter)

    parity = lax.rem(y, 2)

    def piece(q, mine=True):
        side = parity if mine else 1 - parity
        return pl.ds(pl.multiple_of(side * (rows // 2) + q * chunk, chunk), chunk)

    first_load.wait()
    loads = {}
    for e in range(2):
        loads[e] = (local(w_gate.at[e], w1.at[e]), local(w_up.at[e], v1.at[e]))

    gain = scale[...].astype(F32)[None, :]

    def normalize(i, start):
        at = pl.ds(pl.multiple_of(start + i * 16, 16), 16)
        values = utile[0, at, :].astype(F32)
        centered = values - jnp.mean(values, axis=-1, keepdims=True)
        variance = jnp.mean(centered * centered, axis=-1, keepdims=True)
        utile[0, at, :] = (centered * lax.rsqrt(variance + NORM_EPS) * gain).astype(BF16)
        return start

    normalized = set()

    def norm_piece(q):
        if q not in normalized:
            normalized.add(q)
            lax.fori_loop(0, chunk // 16, normalize, parity * (rows // 2) + q * chunk)


    def meta_for(dx):
        return meta_src.at[lax.rem(x + dx + nx, nx)]

    ax = {}

    def near_send(slot, q):
        norm_piece(q)
        ax[slot, q] = remote(utile.at[0, piece(q)], ug.at[slot, 0, piece(q)], dev_x(1 if slot == 1 else -1))

    meta_copies, entry, w2_copies, res_copies = {}, {}, [], []

    def own_routes():
        for q in range(PIECES):
            norm_piece(q)
        lax.fori_loop(0, rows // 32, normalize, (1 - parity) * (rows // 2))
        entry['own'] = remote(utile.at[0], utile.at[1], partner)
        w2_copies.extend(local(w_down.at[e, :, pl.ds(my_half, half)], w2.at[e]) for e in range(2))
        positions, gate_rows = route(utile[0], router_t[...], choice_t[...], capacity)
        per_chip = positions.shape[0] // nx
        for k in range(nx):
            meta_src[k, :per_chip] = positions[k * per_chip:(k + 1) * per_chip]
            meta_src[k, per_chip:] = gate_rows[k * per_chip:(k + 1) * per_chip]
        meta[0] = meta_src[x]
        meta_copies[0, 1] = remote(meta_for(0), meta.at[1], partner)
        w2_copies.extend(remote(w_down.at[e, :, pl.ds(other_half, half)], w2.at[2 + e], partner) for e in range(2))
        res_copies.append(local(resid.at[:, pl.ds(my_quarter, quarter)], xres.at[0]))
        res_copies.append(remote(resid.at[:, pl.ds(other_quarter, quarter)], xres.at[1], partner))

    def send_meta():
        for slot, dx in ((1, 1), (2, -1), (3, 2)):
            for lane in range(2):
                meta_copies[slot, lane] = remote(meta_for(dx), meta.at[slot * 2 + lane], dev_x(dx, lane == 1))

    ay, pushed = {}, {1: [], 2: [], 3: []}

    def push(slot, q, mine):
        at = piece(q, mine)
        pushed[slot].append(remote(ug.at[slot, 0, at], ug.at[slot, 1, at], partner))

    def y_forward(slot, q):
        up = slot == 1 or (slot == 3 and q % 2 == 0)
        ay[slot, q] = remote(ug.at[slot, 0, piece(q)], ug.at[slot, 0, piece(q)], dev_y(1 if up else -1))

    def on_piece(slot, q):
        ax[slot, q].wait_recv()
        if slot == 2 - (q + 1) % 2:
            ax[3, q] = remote(ug.at[slot, 0, piece(q)], ug.at[3, 0, piece(q)], dev_x(1 if slot == 1 else -1))
        y_forward(slot, q)
        push(slot, q, True)

    def on_side(slot, q):
        ay[slot, q].wait_recv()
        push(slot, q, False)

    def slot_onehot(pos_row):
        return lax.broadcasted_iota(jnp.int32, (capacity, rows), 0).astype(F32) == pos_row

    tile = min(1024, d_model)
    tiles = d_model // tile

    def fetch(slot, t, lane):
        cols = pl.ds(t * tile, tile) if isinstance(t, int) else pl.ds(pl.multiple_of(t * tile, tile), tile)
        return pltpu.make_async_copy(ug.at[slot, lane, :, cols], utile.at[lane, :, cols], tile_sem.at[lane * tiles + t])

    def prefetch(slot):
        if 'own' in entry:
            finish_send(entry.pop('own'))
            for q in range(PIECES):
                finish_send(ax[1, q])
                finish_send(ax[2, q])
        for copy in pushed[slot]:
            copy.wait_recv()
        for t in range(tiles):
            for lane in range(2):
                fetch(slot, t, lane).start()

    def meta_rows(slot, lane, e):
        row = 2 * core + e if e < 2 else 2 * (1 - core) + e - 2
        return meta[slot * 2 + lane, pl.ds(row, 1), :], meta[slot * 2 + lane, pl.ds(4 + row, 1), :]

    def gates(slot):
        for lane in range(2):
            taken = jnp.zeros((1, rows), F32)
            picks, weights = ([], []), [jnp.zeros((1, rows), F32), jnp.zeros((1, rows), F32)]
            for e in range(4):
                pos_row, gate_row = meta_rows(slot, lane, e)
                hit = slot_onehot(pos_row)
                for k in range(2):
                    here = taken == float(k)
                    picks[k].append(jnp.where(hit, jnp.where(here, 1.0, 0.0), 0.0))
                    weights[k] = weights[k] + jnp.where(here, jnp.where(pos_row >= 0.0, gate_row, 0.0), 0.0)
                taken = taken + jnp.where(pos_row >= 0.0, 1.0, 0.0)
            for k in range(2):
                select[lane, k] = jnp.concatenate(picks[k], axis=0).T.astype(BF16)
            gate_col[lane] = jnp.concatenate([*weights, jnp.zeros((6, rows), F32)], axis=0).T

    def gather(slot):
        picks = []
        for lane in range(2):
            if (slot, lane) != (0, 0):
                meta_copies[slot, lane].wait_recv()
            parts = [slot_onehot(meta_rows(slot, lane, e)[0]).astype(F32).astype(BF16) for e in range(2)]
            picks.append(jnp.concatenate(parts, axis=0))
        if slot == 0:
            entry['own'].wait_recv()

        def body(t, carry):
            cols = pl.ds(pl.multiple_of(t * tile, tile), tile)
            for lane in range(2):
                if slot:
                    fetch(slot, t, lane).wait()
                got = jnp.dot(picks[lane], utile[lane, :, cols], preferred_element_type=F32).astype(BF16)
                for e in range(2):
                    xg[e, lane * capacity:(lane + 1) * capacity, cols] = got[e * capacity:(e + 1) * capacity]
            return carry

        lax.fori_loop(0, tiles, body, 0)

    ftile = min(256, width)

    def gate_up(e, slot):
        if slot == 0:
            for copy in loads[e]:
                copy.wait()

        def body(t, carry):
            cols = pl.ds(pl.multiple_of(t * ftile, ftile), ftile)
            gate_act = jnp.dot(xg[e], w1[e, :, cols], preferred_element_type=F32)
            up_act = jnp.dot(xg[e], v1[e, :, cols], preferred_element_type=F32)
            hid[e, :, cols] = (jax.nn.silu(gate_act) * up_act).astype(BF16)
            return carry

        lax.fori_loop(0, width // ftile, body, 0)

    xcols = yfar.shape[2]
    ycols = quarter - xcols

    shared = {}

    def share_hidden(slot):
        shared[slot] = remote(hid, hpart.at[slot], partner)

    def down(slot):
        if slot == 0:
            for copy in w2_copies:
                copy.wait_recv() if copy.is_remote else copy.wait()
        shared[slot].wait_recv()

        def body(t, carry):
            cols = pl.ds(pl.multiple_of(t * quarter, quarter), quarter)
            outs = []
            for e in range(4):
                lhs = hid[e] if e < 2 else hpart[slot, e - 2]
                outs.append(jnp.dot(lhs, w2[e, :, cols], preferred_element_type=F32).astype(BF16))
            for lane in range(2):
                stack = []
                for e in range(4):
                    at = lane if e < 2 else 1 - lane
                    stack.append(outs[e][at * capacity:(at + 1) * capacity])
                stacked = jnp.concatenate(stack, axis=0)
                total = jnp.dot(select[lane, 0], stacked, preferred_element_type=F32) * gate_col[lane, :, 0:1]
                total += jnp.dot(select[lane, 1], stacked, preferred_element_type=F32) * gate_col[lane, :, 1:2]
                total = total.astype(BF16)
                sums[slot, lane, :, pl.ds(pl.multiple_of(t * xcols, 128), xcols)] = total[:, :xcols]
                ycon[slot, lane, :, pl.ds(pl.multiple_of(t * ycols, 128), ycols)] = total[:, xcols:]
            return carry

        lax.fori_loop(0, ny, body, 0)
        finish_send(shared[slot])

    rs = {}

    def add_into(ref, other):
        ref[...] = (ref[...].astype(F32) + other[...].astype(F32)).astype(BF16)

    def rs_start(tag, src, landing, dev):
        far, plus, minus = landing
        rs[tag] = {'f0': remote(src(2, 0), far.at[0], dev(1)), 'f1': remote(src(2, 1), far.at[1], dev(-1)),
                   'p1': remote(src(1, 1), plus.at[1], dev(1)), 'm0': remote(src(-1, 0), minus.at[0], dev(-1))}

    def rs_mid(tag, src, landing, dev):
        far, plus, minus = landing
        rs[tag]['f0'].wait_recv()
        add_into(src(1, 0), far.at[0])
        rs[tag]['p0'] = remote(src(1, 0), plus.at[0], dev(1))
        rs[tag]['f1'].wait_recv()
        add_into(src(-1, 1), far.at[1])
        rs[tag]['m1'] = remote(src(-1, 1), minus.at[1], dev(-1))

    def rs_end(tag):
        for name in ('m0', 'p1', 'p0', 'm1'):
            rs[tag][name].wait_recv()

    def y_args(slot):
        def src(dy, lane):
            return ycon.at[slot, lane, :, pl.ds(pl.multiple_of(lax.rem(y + dy + ny, ny) * ycols, 128), ycols)]
        return src, (vfar.at[slot], vplus.at[slot], vminus.at[slot]), dev_y

    def y_start(slot):
        rs_start(slot, *y_args(slot))

    def y_mid(slot):
        rs_mid(slot, *y_args(slot))

    def y_end(slot):
        rs_end(slot)
        src = y_args(slot)[0]
        for lane in range(2):
            total = src(0, lane)[...].astype(F32) + vplus[slot, lane].astype(F32) + vminus[slot, lane].astype(F32)
            if slot == 0:
                wown[lane] = total
            else:
                wsum[slot - 1, lane] = total.astype(BF16)

    def w_src(dx, lane):
        return wsum.at[{-1: 0, 1: 1, 2: 2}[dx], lane]

    def w_far():
        rs['w'] = {'f0': remote(w_src(2, 0), wfar.at[0], dev_x(1)), 'f1': remote(w_src(2, 1), wfar.at[1], dev_x(-1))}

    wx = {}

    def w_send(name):
        lane = int(name[1])
        dx = 1 if name[0] == 'p' else -1
        if name in ('p0', 'm1'):
            rs['w']['f%d' % lane].wait_recv()
            add_into(w_src(dx, lane), wfar.at[lane])
        landing = wplus if dx == 1 else wminus
        wx[name] = remote(w_src(dx, lane), landing.at[lane], dev_x(dx))

    def sub_rows(j):
        return pl.ds(j * sub, sub)

    sx = {}

    def send_sum(name, slot, lane, j, landing, dx):
        sx[name, j] = remote(sums.at[slot, lane, sub_rows(j)], landing.at[lane, sub_rows(j)], dev_x(dx))

    def x_send(name, j):
        lane = int(name[1])
        if name[0] == 'f':
            send_sum(name, 3, lane, j, rfar, 1 if lane == 0 else -1)
            return
        slot, landing, dx = (2, rplus, 1) if name[0] == 'p' else (1, rminus, -1)
        if name in ('p0', 'm1'):
            sx['f%d' % lane, j].wait_recv()
            add_into(sums.at[slot, lane, sub_rows(j)], rfar.at[lane, sub_rows(j)])
        send_sum(name, slot, lane, j, landing, dx)

    def q_cols(dy):
        return pl.ds(pl.multiple_of(lax.rem(y + dy + ny, ny) * xcols, 128), xcols)

    def send_y(name, lane, j, dcol, landing, dy):
        sx[name, j] = remote(sums.at[0, lane, sub_rows(j), q_cols(dcol)], landing.at[lane, sub_rows(j)], dev_y(dy))

    def stage_own(j):
        for name in ('m0', 'p1', 'p0', 'm1'):
            sx[name, j].wait_recv()
        at = sub_rows(j)
        for lane in range(2):
            cols = q_cols(0)
            yown[lane, at, :] = sums[0, lane, at, cols].astype(F32) + rplus[lane, at, cols].astype(F32) + rminus[lane, at, cols].astype(F32)
        for lane in range(2):
            sums[0, lane, at, :] = (sums[0, lane, at, :].astype(F32) + rplus[lane, at, :].astype(F32) + rminus[lane, at, :].astype(F32)).astype(BF16)
        send_y('yf0', 0, j, 2, yfar, 1)
        send_y('yf1', 1, j, 2, yfar, -1)
        send_y('yp1', 1, j, 1, yplus, 1)
        send_y('ym0', 0, j, -1, yminus, -1)

    def stage_yfar(j):
        sx['yf0', j].wait_recv()
        sx['yf1', j].wait_recv()
        at = sub_rows(j)
        cols = q_cols(1)
        sums[0, 0, at, cols] = (sums[0, 0, at, cols].astype(F32) + yfar[0, at, :].astype(F32)).astype(BF16)
        send_y('yp0', 0, j, 1, yplus, 1)
        cols = q_cols(-1)
        sums[0, 1, at, cols] = (sums[0, 1, at, cols].astype(F32) + yfar[1, at, :].astype(F32)).astype(BF16)
        send_y('ym1', 1, j, -1, yminus, -1)

    done = {}
    pending = [res_copies]

    def residual_ready():
        for copy in pending.pop() if pending else ():
            copy.wait_recv() if copy.is_remote else copy.wait()

    def share_rows(key, at, first, cols):
        def place(start):
            return out.at[at, pl.ds(pl.multiple_of(start + first, 128), cols)]

        src = xres.at[:, at, pl.ds(first, cols)]
        for lane in range(2):
            done['up', lane, key] = remote(src.at[lane], place(my_quarter), dev_y(1, lane == 1))
            done['down', lane, key] = remote(src.at[lane], place(my_quarter), dev_y(-1, lane == 1))
        done['own', key] = local(src.at[0], place(my_quarter))
        done['pair', key] = remote(src.at[1], place(my_quarter), partner)

    def relay_rows(key, at, first, cols):
        def place(start):
            return out.at[at, pl.ds(pl.multiple_of(start + first, 128), cols)]

        done['up', 0, key].wait_recv()
        start = my_half + lax.rem(y - 1 + ny, ny) * quarter
        done['up2', key] = remote(place(start), place(start), dev_y(1))
        done['down', 1, key].wait_recv()
        start = other_half + lax.rem(y + 1, ny) * quarter
        done['down2', key] = remote(place(start), place(start), dev_y(-1))

    def stage_final(j):
        for name in ('ym0', 'yp1', 'yp0', 'ym1'):
            sx[name, j].wait_recv()
        residual_ready()
        at = sub_rows(j)
        for lane in range(2):
            total = yown[lane, at, :] + yplus[lane, at, :].astype(F32) + yminus[lane, at, :].astype(F32)
            xres[lane, at, :xcols] = (xres[lane, at, :xcols].astype(F32) + total).astype(BF16)
        share_rows(j, at, 0, xcols)

    def stage_relay(j):
        relay_rows(j, sub_rows(j), 0, xcols)

    def w_share():
        for name in ('m0', 'p1', 'p0', 'm1'):
            wx[name].wait_recv()
        residual_ready()
        for lane in range(2):
            total = wown[lane] + wplus[lane].astype(F32) + wminus[lane].astype(F32)
            xres[lane, :, xcols:] = (xres[lane, :, xcols:].astype(F32) + total).astype(BF16)
        share_rows('w', pl.ds(0, rows), xcols, ycols)

    def w_relay():
        relay_rows('w', pl.ds(0, rows), xcols, ycols)

    actions = {'E2': own_routes, 'ns': near_send, 'meta': send_meta, 'A': on_piece, 'S': on_side, 'PF': prefetch, 'G': gather,
               'U0': functools.partial(gate_up, 0), 'U1': functools.partial(gate_up, 1), 'H': share_hidden, 'T': gates, 'D': down,
               'YS': y_start, 'YM': y_mid, 'YE': y_end, 'wf': w_far, 'WS': w_share, 'WR': w_relay,
               'O': stage_own, 'V': stage_yfar, 'N': stage_final, 'R': stage_relay}
    for name in ('f0', 'f1', 'm0', 'm1', 'p0', 'p1'):
        actions[name] = functools.partial(x_send, name)
        actions['w' + name] = functools.partial(w_send, name)
    for name, *args in ORDER:
        actions[name](*args)
    for key in (*range(SUBS), 'w'):
        done['up', 1, key].wait_recv()
        done['down', 0, key].wait_recv()
        done['pair', key].wait_recv()
        done['up2', key].wait_recv()
        done['down2', key].wait_recv()
        done['own', key].wait()
    for copy in copies:
        if not any(copy is other for other in sent):
            copy.wait_send()


def solution(mesh):
    row_spec = P(('dp', 'ep'), None)
    ny, nx = mesh.shape['tp'], mesh.shape['ep'] // 2

    def device_step(resid_in, norm_scale, w_router, w_gate, w_up, w_down, choice):
        rows, d_model = resid_in.shape
        experts = w_router.shape[1]
        width = w_gate.shape[2]
        capacity = (2 * rows * choice.shape[1] + experts - 1) // experts
        half, slots = d_model // 2, 2 * capacity
        quarter = half // ny
        ycols = quarter // LATE_X_SHARE
        xcols = quarter - ycols

        hbm, vmem = pl.BlockSpec(memory_space=pl.ANY), pl.BlockSpec(memory_space=pltpu.VMEM)
        out, _ = pl.pallas_call(
            functools.partial(moe_kernel, capacity, ny, nx),
            out_shape=(jax.ShapeDtypeStruct((rows, d_model), BF16), jax.ShapeDtypeStruct((4, 2, rows, d_model), BF16)),
            in_specs=[hbm, vmem, vmem, vmem, hbm, hbm, hbm],
            out_specs=(hbm, hbm),
            scratch_shapes=[
                pltpu.VMEM((2, d_model, width), BF16),
                pltpu.VMEM((2, d_model, width), BF16),
                pltpu.VMEM((4, width, half), BF16),
                pltpu.VMEM((2, slots, d_model), BF16),
                pltpu.VMEM((2, slots, width), BF16),
                pltpu.VMEM((4, 2, slots, width), BF16),
                pltpu.VMEM((4, 2, rows, ny * xcols), BF16),
                pltpu.VMEM((2, rows, ny * xcols), BF16),
                pltpu.VMEM((2, rows, ny * xcols), BF16),
                pltpu.VMEM((2, rows, ny * xcols), BF16),
                pltpu.VMEM((2, rows, xcols), F32),
                pltpu.VMEM((2, rows, xcols), BF16),
                pltpu.VMEM((2, rows, xcols), BF16),
                pltpu.VMEM((2, rows, xcols), BF16),
                pltpu.VMEM((4, 2, rows, ny * ycols), BF16),
                pltpu.VMEM((4, 2, rows, ycols), BF16),
                pltpu.VMEM((4, 2, rows, ycols), BF16),
                pltpu.VMEM((4, 2, rows, ycols), BF16),
                pltpu.VMEM((3, 2, rows, ycols), BF16),
                pltpu.VMEM((2, rows, ycols), F32),
                pltpu.VMEM((2, rows, ycols), BF16),
                pltpu.VMEM((2, rows, ycols), BF16),
                pltpu.VMEM((2, rows, ycols), BF16),
                pltpu.VMEM((2, rows, quarter), BF16),
                pltpu.VMEM((2, rows, d_model), BF16),
                pltpu.VMEM((2, 2, rows, 4 * capacity), BF16),
                pltpu.VMEM((2, rows, 8), F32),
                pltpu.VMEM((2 * nx, 2 * experts // nx, rows), F32),
                pltpu.VMEM((nx, 2 * experts // nx, rows), F32),
                pltpu.SemaphoreType.DMA((16,)),
                pltpu.SemaphoreType.DMA((2 * (d_model // min(1024, d_model)),)),
                pltpu.SemaphoreType.DMA((256,)),
                pltpu.SemaphoreType.DMA((256,)),
            ],
            compiler_params=pltpu.CompilerParams(collective_id=0, has_side_effects=True, vmem_limit_bytes=67043328),
            name='moe_ring',
        )(resid_in, norm_scale, w_router.T, choice.T, w_gate, w_up, w_down)
        return out

    return jax.shard_map(device_step, mesh=mesh, in_specs=(row_spec, P(None), P(None, None), P('ep', None, 'tp'), P('ep', None, 'tp'), P('ep', 'tp', None), row_spec), out_specs=row_spec, check_vma=False)
```

```python
import functools

import jax
import jax.numpy as jnp
from jax import lax
from jax.experimental import pallas as pl
from jax.experimental.pallas import tpu as pltpu
from jax.sharding import PartitionSpec as P

NORM_EPS = 1e-5
MESH = pl.DeviceIdType.MESH
BF16 = jnp.bfloat16
F32 = jnp.float32
SUBS = 4
PIECES = 4
LATE_X_SHARE = 2
ORDER = (
    ('ns', 1, 0), ('ns', 2, 3), ('ns', 1, 2), ('ns', 2, 1), ('A', 1, 0), ('A', 2, 3), ('E2',), ('A', 1, 2), ('A', 2, 1),
    ('ns', 1, 3), ('S', 2, 3), ('ns', 2, 2), ('G', 0), ('A', 3, 0), ('A', 3, 3), ('U0', 0), ('U1', 0), ('H', 0),
    ('T', 0), ('A', 3, 2), ('A', 3, 1), ('S', 3, 3), ('ns', 1, 1), ('S', 3, 0), ('ns', 2, 0), ('D', 0), ('A', 1, 3),
    ('S', 3, 2), ('S', 3, 1), ('PF', 3), ('A', 2, 2), ('meta',), ('S', 2, 1), ('A', 1, 1), ('G', 3), ('A', 2, 0),
    ('S', 1, 0), ('YS', 0), ('U0', 3), ('S', 1, 3), ('S', 1, 2), ('U1', 3), ('H', 3), ('S', 1, 1), ('T', 3), ('PF', 1),
    ('D', 3), ('f1', 0), ('f1', 3), ('YS', 3), ('S', 2, 2), ('f0', 2), ('f0', 3), ('S', 2, 0), ('f1', 1), ('G', 1),
    ('PF', 2), ('U0', 1), ('U1', 1), ('H', 1), ('G', 2), ('YM', 3), ('f0', 0), ('T', 1), ('D', 1), ('YS', 1), ('m0', 1),
    ('f0', 1), ('m0', 0), ('U0', 2), ('m0', 3), ('U1', 2), ('H', 2), ('YE', 3), ('wf',), ('T', 2), ('YM', 0), ('D', 2),
    ('p1', 3), ('YS', 2), ('p0', 3), ('m1', 3), ('YE', 0), ('YM', 1), ('p0', 1), ('p1', 1), ('m1', 1), ('p1', 0),
    ('O', 3), ('p0', 0), ('m1', 0), ('f1', 2), ('YM', 2), ('V', 3), ('O', 1), ('N', 3), ('p1', 2), ('YE', 1), ('m1', 2),
    ('p0', 2), ('V', 1), ('O', 0), ('m0', 2), ('YE', 2), ('wp1',), ('wm1',), ('wp0',), ('N', 1), ('V', 0), ('R', 3),
    ('R', 1), ('wm0',), ('N', 0), ('O', 2), ('R', 0), ('V', 2), ('WS',), ('N', 2), ('WR',), ('R', 2),
)


def route(normed, router_t, choice_t, capacity):
    logits = lax.dot_general(router_t, normed, (((1,), (1,)), ((), ())), preferred_element_type=F32)
    weights = jnp.exp(logits - jnp.max(logits, axis=0, keepdims=True))
    probs = weights / jnp.sum(weights, axis=0, keepdims=True)
    expert_ids = lax.broadcasted_iota(jnp.int32, logits.shape, 0)
    chosen = [expert_ids == choice_t[k:k + 1] for k in range(2)]
    picked = [jnp.sum(jnp.where(hit, probs, 0.0), axis=0, keepdims=True) for hit in chosen]
    total = picked[0] + picked[1]
    gate = jnp.where(chosen[0], picked[0] / total, jnp.where(chosen[1], picked[1] / total, 0.0))
    any_chosen = jnp.where(chosen[0], 1.0, jnp.where(chosen[1], 1.0, 0.0))
    rows = normed.shape[0]
    earlier = lax.broadcasted_iota(jnp.int32, (rows, rows), 0) < lax.broadcasted_iota(jnp.int32, (rows, rows), 1)
    earlier = jnp.where(earlier, 1.0, 0.0).astype(BF16)
    position = jnp.dot(any_chosen.astype(BF16), earlier, preferred_element_type=F32)
    kept = (any_chosen > 0.0) & (position < capacity)
    return jnp.where(kept, position, -1.0), jnp.where(kept, gate, 0.0)


def moe_kernel(capacity, ny, nx, resid, scale, router_t, choice_t, w_gate, w_up, w_down, out, ug,
               w1, v1, w2, xg, hid, hpart, sums, rfar, rplus, rminus, yown, yfar, yplus, yminus, ycon, vfar, vplus, vminus, wsum, wown, wfar, wplus, wminus, xres, utile, select, gate_col, meta, meta_src,
               load_sem, tile_sem, send_sem, recv_sem):
    rows, d_model = resid.shape
    half = d_model // 2
    quarter = half // ny
    width = w_gate.shape[2]
    chunk = rows // (2 * PIECES)
    sub = rows // SUBS
    y = lax.axis_index('tp')
    ep = lax.axis_index('ep')
    core = lax.rem(ep, 2)
    x = ep // 2

    def ep_at(dx, other=False):
        return lax.rem(x + dx + nx, nx) * 2 + ((1 - core) if other else core)

    def dev_x(dx, other=False):
        return {'ep': ep_at(dx, other)}

    def dev_y(dy, other=False):
        return {'tp': lax.rem(y + dy + ny, ny), 'ep': ep_at(0, other)}

    partner = dev_x(0, True)

    first_load = pltpu.make_async_copy(resid, utile.at[0], load_sem.at[15])
    first_load.start()
    barrier = pltpu.get_barrier_semaphore()
    peers = [dev_x(dx, o) for dx in range(nx) for o in (False, True) if (dx, o) != (0, False)]
    peers += [dev_y(dy, o) for dy in (1, -1) for o in (False, True)]
    for peer in peers:
        pl.semaphore_signal(barrier, inc=1, device_id=peer, device_id_type=MESH)
    pl.semaphore_wait(barrier, len(peers))

    copies = []

    def remote(src, dst, device):
        at = len(copies)
        copy = pltpu.make_async_remote_copy(src_ref=src, dst_ref=dst, send_sem=send_sem.at[at], recv_sem=recv_sem.at[at], device_id=device, device_id_type=MESH)
        copies.append(copy)
        copy.start()
        return copy

    sent = []

    def finish_send(copy):
        copy.wait_send()
        sent.append(copy)

    locals_ = []

    def local(src, dst):
        copy = pltpu.make_async_copy(src, dst, load_sem.at[len(locals_)])
        locals_.append(copy)
        copy.start()
        return copy

    my_half = pl.multiple_of(core * half, half)
    other_half = pl.multiple_of((1 - core) * half, half)
    my_quarter = pl.multiple_of(my_half + y * quarter, quarter)
    other_quarter = pl.multiple_of(other_half + y * quarter, quarter)

    parity = lax.rem(y, 2)

    def piece(q, mine=True):
        side = parity if mine else 1 - parity
        return pl.ds(pl.multiple_of(side * (rows // 2) + q * chunk, chunk), chunk)

    first_load.wait()
    loads = {}
    for e in range(2):
        loads[e] = (local(w_gate.at[e], w1.at[e]), local(w_up.at[e], v1.at[e]))

    gain = scale[...].astype(F32)[None, :]

    def normalize(i, start):
        at = pl.ds(pl.multiple_of(start + i * 16, 16), 16)
        values = utile[0, at, :].astype(F32)
        centered = values - jnp.mean(values, axis=-1, keepdims=True)
        variance = jnp.mean(centered * centered, axis=-1, keepdims=True)
        utile[0, at, :] = (centered * lax.rsqrt(variance + NORM_EPS) * gain).astype(BF16)
        return start

    normalized = set()

    def norm_piece(q):
        if q not in normalized:
            normalized.add(q)
            lax.fori_loop(0, chunk // 16, normalize, parity * (rows // 2) + q * chunk)


    def meta_for(dx):
        return meta_src.at[lax.rem(x + dx + nx, nx)]

    ax = {}

    def near_send(slot, q):
        norm_piece(q)
        ax[slot, q] = remote(utile.at[0, piece(q)], ug.at[slot, 0, piece(q)], dev_x(1 if slot == 1 else -1))

    meta_copies, entry, w2_copies, res_copies = {}, {}, [], []

    def own_routes():
        for q in range(PIECES):
            norm_piece(q)
        lax.fori_loop(0, rows // 32, normalize, (1 - parity) * (rows // 2))
        entry['own'] = remote(utile.at[0], utile.at[1], partner)
        w2_copies.extend(local(w_down.at[e, :, pl.ds(my_half, half)], w2.at[e]) for e in range(2))
        positions, gate_rows = route(utile[0], router_t[...], choice_t[...], capacity)
        per_chip = positions.shape[0] // nx
        for k in range(nx):
            meta_src[k, :per_chip] = positions[k * per_chip:(k + 1) * per_chip]
            meta_src[k, per_chip:] = gate_rows[k * per_chip:(k + 1) * per_chip]
        meta[0] = meta_src[x]
        meta_copies[0, 1] = remote(meta_for(0), meta.at[1], partner)
        w2_copies.extend(remote(w_down.at[e, :, pl.ds(other_half, half)], w2.at[2 + e], partner) for e in range(2))
        res_copies.append(local(resid.at[:, pl.ds(my_quarter, quarter)], xres.at[0]))
        res_copies.append(remote(resid.at[:, pl.ds(other_quarter, quarter)], xres.at[1], partner))

    def send_meta():
        for slot, dx in ((1, 1), (2, -1), (3, 2)):
            for lane in range(2):
                meta_copies[slot, lane] = remote(meta_for(dx), meta.at[slot * 2 + lane], dev_x(dx, lane == 1))

    ay, pushed = {}, {1: [], 2: [], 3: []}

    def push(slot, q, mine):
        at = piece(q, mine)
        pushed[slot].append(remote(ug.at[slot, 0, at], ug.at[slot, 1, at], partner))

    def y_forward(slot, q):
        up = slot == 1 or (slot == 3 and q % 2 == 0)
        ay[slot, q] = remote(ug.at[slot, 0, piece(q)], ug.at[slot, 0, piece(q)], dev_y(1 if up else -1))

    def on_piece(slot, q):
        ax[slot, q].wait_recv()
        if slot == 2 - (q + 1) % 2:
            ax[3, q] = remote(ug.at[slot, 0, piece(q)], ug.at[3, 0, piece(q)], dev_x(1 if slot == 1 else -1))
        y_forward(slot, q)
        push(slot, q, True)

    def on_side(slot, q):
        ay[slot, q].wait_recv()
        push(slot, q, False)

    def slot_onehot(pos_row):
        return lax.broadcasted_iota(jnp.int32, (capacity, rows), 0).astype(F32) == pos_row

    tile = min(1024, d_model)
    tiles = d_model // tile

    def fetch(slot, t, lane):
        cols = pl.ds(t * tile, tile) if isinstance(t, int) else pl.ds(pl.multiple_of(t * tile, tile), tile)
        return pltpu.make_async_copy(ug.at[slot, lane, :, cols], utile.at[lane, :, cols], tile_sem.at[lane * tiles + t])

    def prefetch(slot):
        if 'own' in entry:
            finish_send(entry.pop('own'))
            for q in range(PIECES):
                finish_send(ax[1, q])
                finish_send(ax[2, q])
        for copy in pushed[slot]:
            copy.wait_recv()
        for t in range(tiles):
            for lane in range(2):
                fetch(slot, t, lane).start()

    def meta_rows(slot, lane, e):
        row = 2 * core + e if e < 2 else 2 * (1 - core) + e - 2
        return meta[slot * 2 + lane, pl.ds(row, 1), :], meta[slot * 2 + lane, pl.ds(4 + row, 1), :]

    def gates(slot):
        for lane in range(2):
            taken = jnp.zeros((1, rows), F32)
            picks, weights = ([], []), [jnp.zeros((1, rows), F32), jnp.zeros((1, rows), F32)]
            for e in range(4):
                pos_row, gate_row = meta_rows(slot, lane, e)
                hit = slot_onehot(pos_row)
                for k in range(2):
                    here = taken == float(k)
                    picks[k].append(jnp.where(hit, jnp.where(here, 1.0, 0.0), 0.0))
                    weights[k] = weights[k] + jnp.where(here, jnp.where(pos_row >= 0.0, gate_row, 0.0), 0.0)
                taken = taken + jnp.where(pos_row >= 0.0, 1.0, 0.0)
            for k in range(2):
                select[lane, k] = jnp.concatenate(picks[k], axis=0).T.astype(BF16)
            gate_col[lane] = jnp.concatenate([*weights, jnp.zeros((6, rows), F32)], axis=0).T

    def gather(slot):
        picks = []
        for lane in range(2):
            if (slot, lane) != (0, 0):
                meta_copies[slot, lane].wait_recv()
            parts = [slot_onehot(meta_rows(slot, lane, e)[0]).astype(F32).astype(BF16) for e in range(2)]
            picks.append(jnp.concatenate(parts, axis=0))
        if slot == 0:
            entry['own'].wait_recv()

        def body(t, carry):
            cols = pl.ds(pl.multiple_of(t * tile, tile), tile)
            for lane in range(2):
                if slot:
                    fetch(slot, t, lane).wait()
                got = jnp.dot(picks[lane], utile[lane, :, cols], preferred_element_type=F32).astype(BF16)
                for e in range(2):
                    xg[e, lane * capacity:(lane + 1) * capacity, cols] = got[e * capacity:(e + 1) * capacity]
            return carry

        lax.fori_loop(0, tiles, body, 0)

    ftile = min(256, width)

    def gate_up(e, slot):
        if slot == 0:
            for copy in loads[e]:
                copy.wait()

        def body(t, carry):
            cols = pl.ds(pl.multiple_of(t * ftile, ftile), ftile)
            gate_act = jnp.dot(xg[e], w1[e, :, cols], preferred_element_type=F32)
            up_act = jnp.dot(xg[e], v1[e, :, cols], preferred_element_type=F32)
            hid[e, :, cols] = (jax.nn.silu(gate_act) * up_act).astype(BF16)
            return carry

        lax.fori_loop(0, width // ftile, body, 0)

    xcols = yfar.shape[2]
    ycols = quarter - xcols

    shared = {}

    def share_hidden(slot):
        shared[slot] = remote(hid, hpart.at[slot], partner)

    def down(slot):
        if slot == 0:
            for copy in w2_copies:
                copy.wait_recv() if copy.is_remote else copy.wait()
        shared[slot].wait_recv()

        def body(t, carry):
            cols = pl.ds(pl.multiple_of(t * quarter, quarter), quarter)
            outs = []
            for e in range(4):
                lhs = hid[e] if e < 2 else hpart[slot, e - 2]
                outs.append(jnp.dot(lhs, w2[e, :, cols], preferred_element_type=F32).astype(BF16))
            for lane in range(2):
                stack = []
                for e in range(4):
                    at = lane if e < 2 else 1 - lane
                    stack.append(outs[e][at * capacity:(at + 1) * capacity])
                stacked = jnp.concatenate(stack, axis=0)
                total = jnp.dot(select[lane, 0], stacked, preferred_element_type=F32) * gate_col[lane, :, 0:1]
                total += jnp.dot(select[lane, 1], stacked, preferred_element_type=F32) * gate_col[lane, :, 1:2]
                total = total.astype(BF16)
                sums[slot, lane, :, pl.ds(pl.multiple_of(t * xcols, 128), xcols)] = total[:, :xcols]
                ycon[slot, lane, :, pl.ds(pl.multiple_of(t * ycols, 128), ycols)] = total[:, xcols:]
            return carry

        lax.fori_loop(0, ny, body, 0)
        finish_send(shared[slot])

    rs = {}

    def add_into(ref, other):
        ref[...] = (ref[...].astype(F32) + other[...].astype(F32)).astype(BF16)

    def rs_start(tag, src, landing, dev):
        far, plus, minus = landing
        rs[tag] = {'f0': remote(src(2, 0), far.at[0], dev(1)), 'f1': remote(src(2, 1), far.at[1], dev(-1)),
                   'p1': remote(src(1, 1), plus.at[1], dev(1)), 'm0': remote(src(-1, 0), minus.at[0], dev(-1))}

    def rs_mid(tag, src, landing, dev):
        far, plus, minus = landing
        rs[tag]['f0'].wait_recv()
        add_into(src(1, 0), far.at[0])
        rs[tag]['p0'] = remote(src(1, 0), plus.at[0], dev(1))
        rs[tag]['f1'].wait_recv()
        add_into(src(-1, 1), far.at[1])
        rs[tag]['m1'] = remote(src(-1, 1), minus.at[1], dev(-1))

    def rs_end(tag):
        for name in ('m0', 'p1', 'p0', 'm1'):
            rs[tag][name].wait_recv()

    def y_args(slot):
        def src(dy, lane):
            return ycon.at[slot, lane, :, pl.ds(pl.multiple_of(lax.rem(y + dy + ny, ny) * ycols, 128), ycols)]
        return src, (vfar.at[slot], vplus.at[slot], vminus.at[slot]), dev_y

    def y_start(slot):
        rs_start(slot, *y_args(slot))

    def y_mid(slot):
        rs_mid(slot, *y_args(slot))

    def y_end(slot):
        rs_end(slot)
        src = y_args(slot)[0]
        for lane in range(2):
            total = src(0, lane)[...].astype(F32) + vplus[slot, lane].astype(F32) + vminus[slot, lane].astype(F32)
            if slot == 0:
                wown[lane] = total
            else:
                wsum[slot - 1, lane] = total.astype(BF16)

    def w_src(dx, lane):
        return wsum.at[{-1: 0, 1: 1, 2: 2}[dx], lane]

    def w_far():
        rs['w'] = {'f0': remote(w_src(2, 0), wfar.at[0], dev_x(1)), 'f1': remote(w_src(2, 1), wfar.at[1], dev_x(-1))}

    wx = {}

    def w_send(name):
        lane = int(name[1])
        dx = 1 if name[0] == 'p' else -1
        if name in ('p0', 'm1'):
            rs['w']['f%d' % lane].wait_recv()
            add_into(w_src(dx, lane), wfar.at[lane])
        landing = wplus if dx == 1 else wminus
        wx[name] = remote(w_src(dx, lane), landing.at[lane], dev_x(dx))

    def sub_rows(j):
        return pl.ds(j * sub, sub)

    sx = {}

    def send_sum(name, slot, lane, j, landing, dx):
        sx[name, j] = remote(sums.at[slot, lane, sub_rows(j)], landing.at[lane, sub_rows(j)], dev_x(dx))

    def x_send(name, j):
        lane = int(name[1])
        if name[0] == 'f':
            send_sum(name, 3, lane, j, rfar, 1 if lane == 0 else -1)
            return
        slot, landing, dx = (2, rplus, 1) if name[0] == 'p' else (1, rminus, -1)
        if name in ('p0', 'm1'):
            sx['f%d' % lane, j].wait_recv()
            add_into(sums.at[slot, lane, sub_rows(j)], rfar.at[lane, sub_rows(j)])
        send_sum(name, slot, lane, j, landing, dx)

    def q_cols(dy):
        return pl.ds(pl.multiple_of(lax.rem(y + dy + ny, ny) * xcols, 128), xcols)

    def send_y(name, lane, j, dcol, landing, dy):
        sx[name, j] = remote(sums.at[0, lane, sub_rows(j), q_cols(dcol)], landing.at[lane, sub_rows(j)], dev_y(dy))

    def stage_own(j):
        for name in ('m0', 'p1', 'p0', 'm1'):
            sx[name, j].wait_recv()
        at = sub_rows(j)
        for lane in range(2):
            cols = q_cols(0)
            yown[lane, at, :] = sums[0, lane, at, cols].astype(F32) + rplus[lane, at, cols].astype(F32) + rminus[lane, at, cols].astype(F32)
        for lane in range(2):
            sums[0, lane, at, :] = (sums[0, lane, at, :].astype(F32) + rplus[lane, at, :].astype(F32) + rminus[lane, at, :].astype(F32)).astype(BF16)
        send_y('yf0', 0, j, 2, yfar, 1)
        send_y('yf1', 1, j, 2, yfar, -1)
        send_y('yp1', 1, j, 1, yplus, 1)
        send_y('ym0', 0, j, -1, yminus, -1)

    def stage_yfar(j):
        sx['yf0', j].wait_recv()
        sx['yf1', j].wait_recv()
        at = sub_rows(j)
        cols = q_cols(1)
        sums[0, 0, at, cols] = (sums[0, 0, at, cols].astype(F32) + yfar[0, at, :].astype(F32)).astype(BF16)
        send_y('yp0', 0, j, 1, yplus, 1)
        cols = q_cols(-1)
        sums[0, 1, at, cols] = (sums[0, 1, at, cols].astype(F32) + yfar[1, at, :].astype(F32)).astype(BF16)
        send_y('ym1', 1, j, -1, yminus, -1)

    done = {}
    pending = [res_copies]

    def residual_ready():
        for copy in pending.pop() if pending else ():
            copy.wait_recv() if copy.is_remote else copy.wait()

    def share_rows(key, at, first, cols):
        def place(start):
            return out.at[at, pl.ds(pl.multiple_of(start + first, 128), cols)]

        src = xres.at[:, at, pl.ds(first, cols)]
        for lane in range(2):
            done['up', lane, key] = remote(src.at[lane], place(my_quarter), dev_y(1, lane == 1))
            done['down', lane, key] = remote(src.at[lane], place(my_quarter), dev_y(-1, lane == 1))
        done['own', key] = local(src.at[0], place(my_quarter))
        done['pair', key] = remote(src.at[1], place(my_quarter), partner)

    def relay_rows(key, at, first, cols):
        def place(start):
            return out.at[at, pl.ds(pl.multiple_of(start + first, 128), cols)]

        done['up', 0, key].wait_recv()
        start = my_half + lax.rem(y - 1 + ny, ny) * quarter
        done['up2', key] = remote(place(start), place(start), dev_y(1))
        done['down', 1, key].wait_recv()
        start = other_half + lax.rem(y + 1, ny) * quarter
        done['down2', key] = remote(place(start), place(start), dev_y(-1))

    def stage_final(j):
        for name in ('ym0', 'yp1', 'yp0', 'ym1'):
            sx[name, j].wait_recv()
        residual_ready()
        at = sub_rows(j)
        for lane in range(2):
            total = yown[lane, at, :] + yplus[lane, at, :].astype(F32) + yminus[lane, at, :].astype(F32)
            xres[lane, at, :xcols] = (xres[lane, at, :xcols].astype(F32) + total).astype(BF16)
        share_rows(j, at, 0, xcols)

    def stage_relay(j):
        relay_rows(j, sub_rows(j), 0, xcols)

    def w_share():
        for name in ('m0', 'p1', 'p0', 'm1'):
            wx[name].wait_recv()
        residual_ready()
        for lane in range(2):
            total = wown[lane] + wplus[lane].astype(F32) + wminus[lane].astype(F32)
            xres[lane, :, xcols:] = (xres[lane, :, xcols:].astype(F32) + total).astype(BF16)
        share_rows('w', pl.ds(0, rows), xcols, ycols)

    def w_relay():
        relay_rows('w', pl.ds(0, rows), xcols, ycols)

    actions = {'E2': own_routes, 'ns': near_send, 'meta': send_meta, 'A': on_piece, 'S': on_side, 'PF': prefetch, 'G': gather,
               'U0': functools.partial(gate_up, 0), 'U1': functools.partial(gate_up, 1), 'H': share_hidden, 'T': gates, 'D': down,
               'YS': y_start, 'YM': y_mid, 'YE': y_end, 'wf': w_far, 'WS': w_share, 'WR': w_relay,
               'O': stage_own, 'V': stage_yfar, 'N': stage_final, 'R': stage_relay}
    for name in ('f0', 'f1', 'm0', 'm1', 'p0', 'p1'):
        actions[name] = functools.partial(x_send, name)
        actions['w' + name] = functools.partial(w_send, name)
    for name, *args in ORDER:
        actions[name](*args)
    for key in (*range(SUBS), 'w'):
        done['up', 1, key].wait_recv()
        done['down', 0, key].wait_recv()
        done['pair', key].wait_recv()
        done['up2', key].wait_recv()
        done['down2', key].wait_recv()
        done['own', key].wait()
    for copy in copies:
        if not any(copy is other for other in sent):
            copy.wait_send()


def solution(mesh):
    row_spec = P(('dp', 'ep'), None)
    ny, nx = mesh.shape['tp'], mesh.shape['ep'] // 2

    def device_step(resid_in, norm_scale, w_router, w_gate, w_up, w_down, choice):
        rows, d_model = resid_in.shape
        experts = w_router.shape[1]
        width = w_gate.shape[2]
        capacity = (2 * rows * choice.shape[1] + experts - 1) // experts
        half, slots = d_model // 2, 2 * capacity
        quarter = half // ny
        ycols = quarter // LATE_X_SHARE
        xcols = quarter - ycols

        hbm, vmem = pl.BlockSpec(memory_space=pl.ANY), pl.BlockSpec(memory_space=pltpu.VMEM)
        out, _ = pl.pallas_call(
            functools.partial(moe_kernel, capacity, ny, nx),
            out_shape=(jax.ShapeDtypeStruct((rows, d_model), BF16), jax.ShapeDtypeStruct((4, 2, rows, d_model), BF16)),
            in_specs=[hbm, vmem, vmem, vmem, hbm, hbm, hbm],
            out_specs=(hbm, hbm),
            scratch_shapes=[
                pltpu.VMEM((2, d_model, width), BF16),
                pltpu.VMEM((2, d_model, width), BF16),
                pltpu.VMEM((4, width, half), BF16),
                pltpu.VMEM((2, slots, d_model), BF16),
                pltpu.VMEM((2, slots, width), BF16),
                pltpu.VMEM((4, 2, slots, width), BF16),
                pltpu.VMEM((4, 2, rows, ny * xcols), BF16),
                pltpu.VMEM((2, rows, ny * xcols), BF16),
                pltpu.VMEM((2, rows, ny * xcols), BF16),
                pltpu.VMEM((2, rows, ny * xcols), BF16),
                pltpu.VMEM((2, rows, xcols), F32),
                pltpu.VMEM((2, rows, xcols), BF16),
                pltpu.VMEM((2, rows, xcols), BF16),
                pltpu.VMEM((2, rows, xcols), BF16),
                pltpu.VMEM((4, 2, rows, ny * ycols), BF16),
                pltpu.VMEM((4, 2, rows, ycols), BF16),
                pltpu.VMEM((4, 2, rows, ycols), BF16),
                pltpu.VMEM((4, 2, rows, ycols), BF16),
                pltpu.VMEM((3, 2, rows, ycols), BF16),
                pltpu.VMEM((2, rows, ycols), F32),
                pltpu.VMEM((2, rows, ycols), BF16),
                pltpu.VMEM((2, rows, ycols), BF16),
                pltpu.VMEM((2, rows, ycols), BF16),
                pltpu.VMEM((2, rows, quarter), BF16),
                pltpu.VMEM((2, rows, d_model), BF16),
                pltpu.VMEM((2, 2, rows, 4 * capacity), BF16),
                pltpu.VMEM((2, rows, 8), F32),
                pltpu.VMEM((2 * nx, 2 * experts // nx, rows), F32),
                pltpu.VMEM((nx, 2 * experts // nx, rows), F32),
                pltpu.SemaphoreType.DMA((16,)),
                pltpu.SemaphoreType.DMA((2 * (d_model // min(1024, d_model)),)),
                pltpu.SemaphoreType.DMA((256,)),
                pltpu.SemaphoreType.DMA((256,)),
            ],
            compiler_params=pltpu.CompilerParams(collective_id=0, has_side_effects=True, vmem_limit_bytes=67043328),
            name='moe_ring',
        )(resid_in, norm_scale, w_router.T, choice.T, w_gate, w_up, w_down)
        return out

    return jax.shard_map(device_step, mesh=mesh, in_specs=(row_spec, P(None), P(None, None), P('ep', None, 'tp'), P('ep', None, 'tp'), P('ep', 'tp', None), row_spec), out_specs=row_spec, check_vma=False)
```
